32 devices in a mesh: centre: 4 (over y, core), sample: 8 (over z, x).
Axes of the slice: x: 2, y: 2, z: 4, core: 2. Of those that a mesh axis runs over, the one named last changes fastest.
Arguments:
- centres: bfloat16 [1024, 8192], P(None, 'centre'), may hold values from -40 to 40
- pool: bfloat16 [1024, 8192], P('centre', 'sample'), may hold values from -40 to 40
- labels: int32 [8192], P('sample'), may hold values from 0 to 143
- picks: int32 [2, 4096], P(None, 'sample'), may hold values from 0 to 8191, as said below
- coefs: float32 [144, 8192], P(None, ('centre', 'sample')), may hold values from -192 to 256000
Outputs:
- new_coefs: float32 [144, 8192], P(None, ('centre', 'sample'))
The draws below stay inside these ranges and needn't reach their ends.
Inputs may be any that keep to these rules, and one draw needn't show every extreme that they name: `picks`: entry b of a step's batch is a pool column in [(b // 512) * 1024, (b // 512 + 1) * 1024); entries may repeat.
All inputs are finite; a program needn't handle non-finite values.
Results may differ from the reference program's by a relative error of at most 0.00065.
Values may be sent and summed in bfloat16 or wider, within the bound.
A program may use at most 64 MiB of HBM per device.

```python
import jax
import jax.numpy as jnp
from jax import lax

D = 1024
K = 144
STEPS = 2
BATCH_DEV = 512
POOL_DEV = 1024
CENTRES = 8192
BATCH = 4096
POOL = 8192
N_SAMPLE = 8


GROUP_SHARED = 0.05


GROUP_NOISE = 0.15


GROUP_LEVEL = 128.0


WAVE_AMPLITUDE = 2.5


WAVE_RATE = 0.35


def column_scales(key, count, lower, upper):
    return jnp.exp(jax.random.uniform(key, (count,), jnp.float32, jnp.log(lower), jnp.log(upper)))


def latent_map(key):
    return jax.random.truncated_normal(jax.random.fold_in(key, 5001), -4.0, 4.0, (D, 8), jnp.float32)


def centre_latents(key):
    return jax.random.truncated_normal(jax.random.fold_in(key, 5002), -4.0, 4.0, (8, CENTRES), jnp.float32)


def pool_latents(key):
    return jax.random.truncated_normal(jax.random.fold_in(key, 5003), -4.0, 4.0, (8, POOL), jnp.float32)


def prototypes(key):
    return jax.random.truncated_normal(jax.random.fold_in(key, 6001), -4.0, 4.0, (D, 2 * K), jnp.float32)


def centre_groups(key):
    return jax.random.randint(jax.random.fold_in(key, 6003), (CENTRES,), 0, 2 * K, jnp.int32)


def pool_groups(key):
    return jax.random.randint(jax.random.fold_in(key, 6004), (POOL,), 0, 2 * K, jnp.int32)


def grouped_columns(key, groups, latents, salt, lower, upper):
    scales = column_scales(jax.random.fold_in(key, 6002), 2 * K, lower, upper)
    base = jnp.take(prototypes(key), groups, axis=1)
    jitter = jax.random.truncated_normal(jax.random.fold_in(key, salt), -4.0, 4.0, (D, groups.shape[0]), jnp.float32)
    shared = jnp.dot(latent_map(key), latents, precision=lax.Precision.HIGHEST)
    return jnp.take(scales, groups)[None, :] * (base + GROUP_SHARED * shared + GROUP_NOISE * jitter)


def draw_centres(key, part):
    groups = centre_groups(key)
    columns = grouped_columns(key, groups, centre_latents(key), 11, 0.5, 2.0)
    return jnp.clip(columns, -40.0, 40.0).astype(jnp.bfloat16)


def draw_pool(key, part):
    groups = pool_groups(key)
    columns = grouped_columns(key, groups, pool_latents(key), 13, 0.5, 2.0)
    return jnp.clip(columns, -40.0, 40.0).astype(jnp.bfloat16)


def draw_picks(key, part):
    offsets = jax.random.randint(jax.random.fold_in(key, 31), (STEPS, BATCH), 0, POOL_DEV, jnp.int32)
    starts = jnp.arange(BATCH, dtype=jnp.int32) // BATCH_DEV * POOL_DEV
    return offsets + starts[None, :]


def draw_coefs(key, part):
    frequency = WAVE_RATE * jax.random.normal(jax.random.fold_in(key, 41), (256, 8), jnp.float32)
    phases = jax.random.uniform(jax.random.fold_in(key, 42), (256, 1), jnp.float32, -3.14159265, 3.14159265)
    wave_table = jnp.cos(jnp.dot(frequency, centre_latents(key), precision=lax.Precision.HIGHEST) + phases)
    groups = centre_groups(key)
    mixing = jax.random.uniform(jax.random.fold_in(key, 43), (K, 256), jnp.float32, -1.0, 1.0)
    jitter = jax.random.uniform(jax.random.fold_in(key, 22), (K, CENTRES), jnp.float32, -0.3, 0.3)
    group_table = GROUP_LEVEL * jax.random.uniform(jax.random.fold_in(key, 44), (K, 2 * K), jnp.float32, -1.0, 1.0)
    columns = WAVE_AMPLITUDE / 16.0 * jnp.dot(mixing, wave_table, precision=lax.Precision.HIGHEST) + jitter
    columns = columns + jnp.take(group_table, groups, axis=1)
    return columns.astype(jnp.float32)


def touch_ends(result, own_key, smallest, high):
    spot = [jax.random.randint(jax.random.fold_in(own_key, axis), (), 0, length) for axis, length in enumerate(result.shape)]
    widest = result.shape.index(max(result.shape))
    next_to = spot[:widest] + [(spot[widest] + 1) % result.shape[widest]] + spot[widest + 1:]
    return result.at[tuple(spot)].set(smallest).at[tuple(next_to)].set(high)


def setup_inputs(seed: int = 0) -> dict:
    streams_of = jax.random.split(jax.random.key(seed), 6)
    centres = draw_centres(jax.random.fold_in(streams_of[5], 71), 0)
    pool = draw_pool(jax.random.fold_in(streams_of[5], 71), 0)
    labels = touch_ends(jax.random.randint(streams_of[2], (POOL,), 0, K), jax.random.fold_in(streams_of[2], 1), 0, K - 1).astype(jnp.int32)
    picks = draw_picks(jax.random.fold_in(streams_of[5], 71), 0)
    coefs = draw_coefs(jax.random.fold_in(streams_of[5], 71), 0)
    return dict(centres=centres, pool=pool, labels=labels, picks=picks, coefs=coefs)


LOGIT_GAIN = 16.0
LENGTH_SCALE = 0.5
STEP_GAIN = 2048.0
EPS = 1e-06

def laplace(cross, sample_sq, centre_sq):
    mean_sq = (sample_sq[:, None] + centre_sq[None, :] - 2.0 * cross) / D
    return jnp.exp(-jnp.sqrt(mean_sq + EPS) / LENGTH_SCALE).astype(jnp.bfloat16)

def residual(logits, labs):
    classes = jnp.arange(K, dtype=jnp.int32)
    top = lax.optimization_barrier(jnp.max(logits, axis=0, keepdims=True))
    expo = jnp.exp(logits - top)
    probs = expo / lax.optimization_barrier(jnp.sum(expo, axis=0, keepdims=True))
    hot = (classes[:, None] == labs[None, :]).astype(jnp.float32)
    return (probs - hot).astype(jnp.bfloat16)

def reference(centres, pool, labels, picks, coefs):
    centre_sq = lax.optimization_barrier(jnp.sum(jnp.square(centres.astype(jnp.float32)), axis=0))
    for step in range(STEPS):
        blocks = picks[step].reshape(N_SAMPLE, BATCH_DEV)
        coef_half = coefs.astype(jnp.bfloat16)

        def visit(total, block):
            feats = jnp.take(pool, block, axis=1)
            cross = lax.dot_general(feats, centres, (((0,), (0,)), ((), ())), preferred_element_type=jnp.float32)
            sample_sq = lax.optimization_barrier(jnp.sum(jnp.square(feats.astype(jnp.float32)), axis=0))
            kern = laplace(cross, sample_sq, centre_sq)
            logits = lax.dot_general(coef_half, kern, (((1,), (1,)), ((), ())), preferred_element_type=jnp.float32)
            logits = logits * (LOGIT_GAIN / CENTRES)
            resid = residual(logits, jnp.take(labels, block))
            return (total + jnp.dot(resid, kern, preferred_element_type=jnp.float32), None)
        grad, _ = lax.scan(visit, jnp.zeros((K, CENTRES), jnp.float32), blocks)
        coefs = coefs - STEP_GAIN * LOGIT_GAIN / BATCH * grad
    return coefs
```

```python
import functools
import math

import jax
import jax.numpy as jnp
from jax import lax
from jax.experimental import pallas as pl
from jax.experimental.pallas import tpu as pltpu
from jax.sharding import PartitionSpec as P

LOGIT_GAIN = 16.0
LENGTH_SCALE = 0.5
STEP_GAIN = 2048.0
EPS = 1e-06

GRAD_WIRE = jnp.bfloat16
LOGIT_WIRE = jnp.float32
MESH = pl.DeviceIdType.MESH
NT = (((1,), (1,)), ((), ()))


def kernel(
    n_c, n_s, logit_scale, rate,
    cen_hbm, pool_ref, labels_ref, picks_ref, coefs_ref, out_ref,
    cen, csq, feats, kern, labs, coefb, lsend, lrecv, resid, gsend, grecv, psend, precv, cur,
    cen_sem, send_sem, feat_sem, log_sem, res_sem, coef_sem, grad_sem,
):
    steps, batch = picks_ref.shape
    fd, pool_dev = pool_ref.shape
    classes, own = coefs_ref.shape
    width, cen_dev = cen.shape
    share = batch // n_c
    ny = n_c // 2
    tile = max(own, min(256, cen_dev))
    pieces = tile // own

    c = lax.axis_index("centre")
    s = lax.axis_index("sample")
    sib = c + 1 - 2 * lax.rem(c, 2)
    c_peers = [lax.rem(c + r, n_c) for r in range(1, n_c)]
    s_peers = [lax.rem(s + r, n_s) for r in range(1, n_s)]
    pair = s + 1 - 2 * lax.rem(s, 2)
    nz = n_s // 2
    order = sorted(range(1, nz), key=lambda q: -min(q, nz - q))

    barrier = pltpu.get_barrier_semaphore()
    for peer in c_peers:
        pl.semaphore_signal(barrier, inc=1, device_id={"centre": peer}, device_id_type=MESH)
    for peer in s_peers:
        pl.semaphore_signal(barrier, inc=1, device_id={"sample": peer}, device_id_type=MESH)

    load = pltpu.make_async_copy(cen_hbm, cen, cen_sem)
    load.start()
    started = []

    def send(src, dst, recv, axis, peer):
        copy = pltpu.make_async_remote_copy(
            src_ref=src, dst_ref=dst, send_sem=send_sem.at[len(started)], recv_sem=recv,
            device_id={axis: peer}, device_id_type=MESH,
        )
        copy.start()
        started.append(copy)
        return copy

    label_rows = jnp.broadcast_to(labels_ref[...].astype(jnp.float32), (16, pool_dev)).astype(jnp.bfloat16)

    def pick(t):
        chosen = picks_ref[t:t + 1, :] - s * pool_dev
        rows = lax.broadcasted_iota(jnp.int32, (pool_dev, batch), 0)
        hot = jnp.where(rows == chosen, -2.0, 0.0).astype(jnp.bfloat16)
        got = jnp.dot(pool_ref[...], hot, preferred_element_type=jnp.float32)
        feats[t, c] = got.T.astype(jnp.bfloat16)
        lab = -0.5 * jnp.dot(label_rows, hot, preferred_element_type=jnp.float32)
        for k in range(n_c):
            labs[t, k] = lab[0:8, k * share:(k + 1) * share]

    def send_feats(t):
        mine = feats.at[t, c]
        direct = []
        for q in range(1, ny):
            direct.append(send(mine, mine, feat_sem.at[t, q], "centre", lax.rem(c + 2 * q, n_c)))
        return [send(mine, mine, feat_sem.at[t, 0], "centre", sib)], direct

    def forward_feats(t, near, direct):
        for q, copy in enumerate(direct, 1):
            copy.wait_recv()
            slot = feats.at[t, lax.rem(c - 2 * q + n_c, n_c)]
            near.append(send(slot, slot, feat_sem.at[t, ny - 1 + q], "centre", sib))
        for copy in near:
            copy.wait_recv()

    def send_coefs(t):
        mine = coefb.at[t, s]
        direct = [
            (q, send(mine, mine, coef_sem.at[t, q], "sample", lax.rem(s + 2 * q, n_s)))
            for q in order
        ]
        return [send(mine, mine, coef_sem.at[t, 0], "sample", pair)], direct

    def forward_coefs(t, near, direct):
        for q, copy in direct:
            copy.wait_recv()
            slot = coefb.at[t, lax.rem(s - 2 * q + n_s, n_s)]
            near.append(send(slot, slot, coef_sem.at[t, nz - 1 + q], "sample", pair))

    cur[...] = coefs_ref[...]
    coefb[0, s] = coefs_ref[...].astype(jnp.bfloat16)
    pl.semaphore_wait(barrier, n_c - 1 + n_s - 1)
    coef_near, coef_direct = send_coefs(0)
    pick(0)
    moves = [send_feats(0)]
    pick(1)
    moves.append(send_feats(1))

    load.wait()

    def square(j, _):
        cols = pl.ds(pl.multiple_of(j * tile, tile), tile)
        block = cen[:, cols].astype(jnp.float32)
        csq[:, cols] = jnp.sum(block * block, axis=0, keepdims=True)
        return 0

    lax.fori_loop(0, cen_dev // tile, square, 0)

    bend = (1.0 / (LENGTH_SCALE * math.log(2.0))) ** 2

    def laplace(t):
        parts = [feats[t, k] for k in range(n_c)]
        ssq = sum(
            jnp.sum(jnp.square(p.astype(jnp.float32)), axis=1, keepdims=True) for p in parts
        ) * 0.25
        if fd % 128 == 0:
            parts = [jnp.concatenate(parts, axis=1)]
        deep = width // len(parts)

        def body(j, _):
            cols = pl.ds(pl.multiple_of(j * tile, tile), tile)
            cross = sum(
                jnp.dot(p, cen[k * deep:(k + 1) * deep, cols], preferred_element_type=jnp.float32)
                for k, p in enumerate(parts)
            )
            arg = ((ssq + csq[:, cols]) + cross) * (bend / width) + bend * EPS
            arg = jnp.maximum(arg, 1e-30)
            value = jnp.exp2(-(arg * lax.rsqrt(arg)))
            for k in range(pieces):
                kern[t, j * pieces + k] = value[:, k * own:(k + 1) * own].astype(jnp.bfloat16)
            return 0

        lax.fori_loop(0, cen_dev // tile, body, 0)

    def residual(t):
        part = sum(
            lax.dot_general(coefb[t, j], kern[t, j], NT, preferred_element_type=jnp.float32)
            for j in range(n_s)
        )
        for k in range(n_c):
            lsend[t, k] = part[:, k * share:(k + 1) * share].astype(LOGIT_WIRE)
        copies = [
            send(lsend.at[t, peer], lrecv.at[t, r], log_sem.at[t, r], "centre", peer)
            for r, peer in enumerate(c_peers)
        ]
        if t + 1 < steps:
            forward_feats(t + 1, *moves[t + 1])
        total = lsend[t, c].astype(jnp.float32)
        for r, copy in enumerate(copies):
            copy.wait_recv()
            total = total + lrecv[t, r].astype(jnp.float32)
        logits = total * logit_scale
        expo = jnp.exp(logits - jnp.max(logits, axis=0, keepdims=True))
        probs = expo / jnp.sum(expo, axis=0, keepdims=True)
        ids = lax.broadcasted_iota(jnp.int32, (classes, share), 0).astype(jnp.float32)
        hot = jnp.where(ids == labs[t, c][0:1, :], 1.0, 0.0)
        resid[t, c] = (probs - hot).astype(jnp.bfloat16)
        mine = resid.at[t, c]
        copies = [
            send(mine, mine, res_sem.at[t, r], "centre", peer) for r, peer in enumerate(c_peers)
        ]
        for copy in copies:
            copy.wait_recv()

    def gradient(t):
        if share % 128 == 0:
            whole = jnp.concatenate([resid[t, k] for k in range(n_c)], axis=1)

            def grad(j):
                return jnp.dot(whole, kern[t, j], preferred_element_type=jnp.float32)
        else:
            def grad(j):
                return sum(
                    jnp.dot(resid[t, k], kern[t, j, k * share:(k + 1) * share, :],
                            preferred_element_type=jnp.float32)
                    for k in range(n_c)
                )
        def put(i, value, peer):
            gsend[t, i] = value.astype(GRAD_WIRE)
            return send(gsend.at[t, i], grecv.at[t, i], grad_sem.at[t, i], "sample", peer)

        far = [lax.rem(start + 2 * q, n_s) for q in order for start in (s, pair)]
        copies = [put(i, grad(peer), peer) for i, peer in enumerate(far)]
        psend[t] = grad(pair)
        last = send(psend.at[t], precv.at[t], grad_sem.at[t, n_s - 2], "sample", pair)
        return grad(s), last, copies

    forward_coefs(0, coef_near, coef_direct[:2])
    forward_feats(0, *moves[0])
    forward_coefs(0, coef_near, coef_direct[2:])
    laplace(0)
    for t in range(steps):
        for copy in coef_near:
            copy.wait_recv()
        residual(t)
        total, last, copies = gradient(t)
        if t + 1 < steps:
            laplace(t + 1)
        last.wait_recv()
        total = total + precv[t]
        for r, copy in enumerate(copies):
            copy.wait_recv()
            total = total + grecv[t, r].astype(jnp.float32)
        fresh = cur[...] - rate * total
        if t + 1 < steps:
            cur[...] = fresh
            coefb[t + 1, s] = fresh.astype(jnp.bfloat16)
            coef_near, coef_direct = send_coefs(t + 1)
            forward_coefs(t + 1, coef_near, coef_direct)
        else:
            out_ref[...] = fresh
    for copy in started:
        copy.wait_send()


CHUNKS = 2
PIECES = 3
LOG_STEPS = 520.0
LOG_LOW = 50.0


def encode(value):
    size = jnp.maximum(jnp.abs(value), 2.0 ** -LOG_LOW)
    code = jnp.round((jnp.log(size) * (1.0 / math.log(2.0)) + LOG_LOW) * LOG_STEPS)
    return jnp.where(value < 0.0, -code, code).astype(jnp.int16)


def decode(code):
    number = code.astype(jnp.float32)
    size = jnp.exp2(jnp.abs(number) * (1.0 / LOG_STEPS) - LOG_LOW)
    return jnp.where(number < 0.0, -size, jnp.where(number > 0.0, size, 0.0))


def line_kernel(
    logit_scale, rate,
    cen_hbm, pool_hbm, labels_hbm, picks_hbm, coefs_hbm, out_ref,
    cen, pool_ref, labels_ref, picks_ref, cur,
    csq, feats, kern, labs, coefb, lpart, lrecv, lsum, ysum, resid, gown,
    xsend, xrecv, asend, arecv, bsend, brecv,
    load_sem, send_sem, feat_sem, log_sem, red_x, red_a, red_b, coef_x, coef_a, coef_b,
):
    steps, batch = picks_ref.shape
    fd, pool_dev = pool_ref.shape
    classes, own = cur.shape
    width, cen_dev = cen.shape
    blocks = cen_dev // own
    rows_n = batch // CHUNKS
    half = rows_n // 2
    piece = classes // PIECES
    tile = 2 * own

    c = lax.axis_index("centre")
    s = lax.axis_index("sample")
    y, k = lax.div(c, 2), lax.rem(c, 2)
    z, x = lax.div(s, 2), lax.rem(s, 2)
    side = lax.div(z, 2)
    inner = lax.rem(z + side, 2)
    is_inner = inner == 1
    is_outer = inner == 0
    SO, SI, OI, OO = 3 * side, 1 + side, 2 - side, 3 - 3 * side
    sib_c = c + 1 - 2 * k
    far_c = (1 - y) * 2 + k
    far_sib_c = (1 - y) * 2 + 1 - k
    sib = {"centre": sib_c}
    far = {"centre": far_c}
    xp = {"sample": z * 2 + 1 - x}
    za = {"sample": (z + 1 - 2 * lax.rem(z, 2)) * 2 + x}
    zb = {"sample": (3 - z) * 2 + x}

    barrier = pltpu.get_barrier_semaphore()
    for peer in (sib, far, xp, za, zb):
        pl.semaphore_signal(barrier, inc=1, device_id=peer, device_id_type=MESH)

    loads = [
        pltpu.make_async_copy(src, dst, load_sem.at[i])
        for i, (src, dst) in enumerate(
            [(picks_hbm, picks_ref), (pool_hbm, pool_ref), (labels_hbm, labels_ref), (coefs_hbm, cur), (cen_hbm, cen)]
        )
    ]
    for copy in loads:
        copy.start()

    used = []

    def make(src, dst, recv, peer):
        used.append(pltpu.make_async_remote_copy(
            src_ref=src, dst_ref=dst, send_sem=send_sem.at[len(used)], recv_sem=recv,
            device_id=peer, device_id_type=MESH,
        ))
        return used[-1]

    def rows_of(i):
        return slice(i * rows_n, (i + 1) * rows_n)

    def piece_of(h):
        return slice(h * piece, (h + 1) * piece)

    everyone, outers, inners = [], [], []

    def plain(*args):
        copy = make(*args)
        everyone.append(copy)
        return copy

    feat_far = [[plain(feats.at[t, c, rows_of(i)], feats.at[t, c, rows_of(i)], feat_sem.at[t, 0, i], far)
                 for i in range(CHUNKS)] for t in range(steps)]
    feat_sib = [[plain(feats.at[t, c, rows_of(i)], feats.at[t, c, rows_of(i)], feat_sem.at[t, 1, i], sib)
                 for i in range(CHUNKS)] for t in range(steps)]
    feat_fwd = [[plain(feats.at[t, far_c, rows_of(i)], feats.at[t, far_c, rows_of(i)], feat_sem.at[t, 2, i], sib)
                 for i in range(CHUNKS)] for t in range(steps)]
    log_sib = [[plain(lpart.at[t, i, 1 - k], lrecv.at[t, i], log_sem.at[t, 0, i], sib)
                for i in range(CHUNKS)] for t in range(steps)]
    log_far = [[plain(lsum.at[t, i], ysum.at[t, i], log_sem.at[t, 1, i], far)
                for i in range(CHUNKS)] for t in range(steps)]
    res_sib = [[plain(resid.at[t, i, k], resid.at[t, i, k], log_sem.at[t, 2, i], sib)
                for i in range(CHUNKS)] for t in range(steps)]
    sum_x = [[[plain(xsend.at[t, p, piece_of(h)], xrecv.at[t, p, piece_of(h)], red_x.at[t, p, h], xp)
               for h in range(PIECES)] for p in range(4)] for t in range(steps)]

    def group(store, *args):
        copy = make(*args)
        store.append(copy)
        return copy

    sum_a = [[[make(asend.at[t, p, piece_of(h)], arecv.at[t, p, piece_of(h)], red_a.at[t, p, h], za)
               for h in range(PIECES)] for p in range(3)] for t in range(steps)]
    sum_b = [[[make(bsend.at[t, p, piece_of(h)], brecv.at[t, p, piece_of(h)], red_b.at[t, p, h], zb)
               for h in range(PIECES)] for p in range(2)] for t in range(steps)]
    for t in range(steps):
        for h in range(PIECES):
            outers.extend([sum_a[t][p][h] for p in range(3)])
            inners.extend([sum_a[t][0][h], sum_b[t][0][h], sum_b[t][1][h]])

    names = (SO, SI, OI, OO)

    def coef_copy(t, name, h, sem, peer):
        slot = coefb.at[t, name * 2 + x, piece_of(h)]
        return make(slot, slot, sem, peer)

    put_x = [[[coef_copy(t, names[n], h, coef_x.at[t, n, h], xp) for h in range(PIECES)] for n in range(4)]
             for t in range(steps)]
    out_a = [[coef_copy(t, SO, h, coef_a.at[t, 0, h], za) for h in range(PIECES)] for t in range(steps)]
    in_a = [[[coef_copy(t, names[1 + n], h, coef_a.at[t, n, h], za) for h in range(PIECES)] for n in range(3)]
            for t in range(steps)]
    in_b = [[[coef_copy(t, (SI, SO)[n], h, coef_b.at[t, n, h], zb) for h in range(PIECES)] for n in range(2)]
            for t in range(steps)]
    for t in range(steps):
        for h in range(PIECES):
            everyone.extend([put_x[t][n][h] for n in range(4)])
            outers.append(out_a[t][h])
            inners.extend([in_a[t][n][h] for n in range(3)] + [in_b[t][n][h] for n in range(2)])

    def pick(t):
        chosen = picks_ref[t:t + 1, :] - s * pool_dev
        rows = lax.broadcasted_iota(jnp.int32, (pool_dev, batch), 0)
        hot = jnp.where(rows == chosen, -2.0, 0.0).astype(jnp.bfloat16)
        got = jnp.dot(pool_ref[...], hot, preferred_element_type=jnp.float32)
        feats[t, c] = got.T.astype(jnp.bfloat16)
        return hot

    def pick_labels(t, hot):
        label_rows = jnp.broadcast_to(labels_ref[...].astype(jnp.float32), (16, pool_dev)).astype(jnp.bfloat16)
        lab = -0.5 * jnp.dot(label_rows, hot, preferred_element_type=jnp.float32)
        for n in range(2 * CHUNKS):
            labs[t, n] = lab[0:8, n * half:(n + 1) * half]

    bend = (1.0 / (LENGTH_SCALE * math.log(2.0))) ** 2

    def laplace(t, i, first, last):
        rows = rows_of(i)
        ssq = sum(
            jnp.sum(jnp.square(feats[t, q, rows].astype(jnp.float32)), axis=1, keepdims=True) for q in range(4)
        ) * 0.25

        def body(j, _):
            cols = pl.ds(pl.multiple_of(j * tile, tile), tile)
            lhs = jnp.concatenate([feats[t, q, rows] for q in range(4)], axis=1)
            cross = jnp.dot(lhs, cen[:, cols], preferred_element_type=jnp.float32)
            arg = ((ssq + csq[:, cols]) + cross) * (bend / width) + bend * EPS
            arg = jnp.maximum(arg, 1e-30)
            value = jnp.exp2(-(arg * lax.rsqrt(arg)))
            for q in range(2):
                kern[t, j * 2 + q, rows] = value[:, q * own:(q + 1) * own].astype(jnp.bfloat16)
            return 0

        lax.fori_loop(first, last, body, 0)

    tiles = cen_dev // tile

    def logits(t, i):
        part = sum(
            lax.dot_general(coefb[t, j], kern[t, j, rows_of(i)], NT, preferred_element_type=jnp.float32)
            for j in range(blocks)
        )
        for h in range(2):
            lpart[t, i, h] = part[:, h * half:(h + 1) * half]
        log_sib[t][i].start()

    def chip_sum(t, i):
        log_sib[t][i].wait_recv()
        lsum[t, i] = lpart[t, i, k] + lrecv[t, i]
        log_far[t][i].start()

    def residual(t, i):
        log_far[t][i].wait_recv()
        value = (lsum[t, i] + ysum[t, i]) * logit_scale
        expo = jnp.exp(value - jnp.max(value, axis=0, keepdims=True))
        probs = expo / jnp.sum(expo, axis=0, keepdims=True)
        ids = lax.broadcasted_iota(jnp.int32, (classes, half), 0).astype(jnp.float32)
        hot = jnp.where(ids == labs[t, 2 * i + k][0:1, :], 1.0, 0.0)
        resid[t, i, k] = (probs - hot).astype(jnp.bfloat16)
        res_sib[t][i].start()

    def swap(now, later):
        return jnp.where(is_inner, later, now)

    order = (OO, swap(OI, SO), swap(SI, OI), swap(SO, SI))

    def gradient(t):
        for i in range(CHUNKS):
            res_sib[t][i].wait_recv()
        whole = jnp.concatenate([resid[t, i, h] for i in range(CHUNKS) for h in range(2)], axis=1)

        def grad(zd, xd):
            return jnp.dot(whole, kern[t, zd * 2 + xd], preferred_element_type=jnp.float32)

        for p in range(4):
            xsend[t, p] = encode(grad(order[p], 1 - x))
            for h in range(PIECES):
                sum_x[t][p][h].start()
        for p in range(4):
            gown[p] = grad(order[p], x)

    def chain(t, p):
        def add_x(h):
            sum_x[t][p][h].wait_recv()
            return gown[p, piece_of(h)] + decode(xrecv[t, p, piece_of(h)])

        @pl.when(is_outer)
        def _():
            for h in range(PIECES):
                value = add_x(h)
                if p < 3:
                    asend[t, p, piece_of(h)] = encode(value)
                    sum_a[t][p][h].start()
                else:
                    sum_a[t][0][h].wait_recv()
                    gown[3, piece_of(h)] = value + decode(arecv[t, 0, piece_of(h)])

        @pl.when(is_inner)
        def _():
            for h in range(PIECES):
                value = add_x(h)
                rows = piece_of(h)
                if p == 0:
                    sum_a[t][0][h].wait_recv()
                    bsend[t, 0, rows] = encode(value + decode(arecv[t, 0, rows]))
                    sum_b[t][0][h].start()
                elif p == 1:
                    sum_b[t][0][h].wait_recv()
                    asend[t, 0, rows] = encode(value + decode(brecv[t, 0, rows]))
                    sum_a[t][0][h].start()
                elif p == 2:
                    sum_a[t][1][h].wait_recv()
                    bsend[t, 1, rows] = encode(value + decode(arecv[t, 1, rows]))
                    sum_b[t][1][h].start()
                else:
                    sum_a[t][2][h].wait_recv()
                    sum_b[t][1][h].wait_recv()
                    gown[3, rows] = value + decode(arecv[t, 2, rows]) + decode(brecv[t, 1, rows])

    def share_own(t):
        @pl.when(is_outer)
        def _():
            for h in range(PIECES):
                out_a[t][h].start()
                put_x[t][0][h].start()

        @pl.when(is_inner)
        def _():
            for h in range(PIECES):
                in_b[t][0][h].start()
                in_a[t][0][h].start()
                put_x[t][1][h].start()

    def share_hop(t, hop):
        @pl.when(is_outer)
        def _():
            for h in range(PIECES):
                in_a[t][hop][h].wait_recv()
                put_x[t][1 + hop][h].start()

        @pl.when(is_inner)
        def _():
            for h in range(PIECES):
                if hop == 0:
                    out_a[t][h].wait_recv()
                    in_b[t][1][h].start()
                    in_b[t][0][h].wait_recv()
                    in_a[t][1][h].start()
                    put_x[t][0][h].start()
                    put_x[t][2][h].start()
                elif hop == 1:
                    in_b[t][1][h].wait_recv()
                    in_a[t][2][h].start()
                    put_x[t][3][h].start()

    def share_end(t):
        for n in range(4):
            for h in range(PIECES):
                put_x[t][n][h].wait_recv()

    loads[0].wait()
    loads[1].wait()
    hots = pick(0)
    pl.semaphore_wait(barrier, 5)
    for i in range(CHUNKS):
        feat_far[0][i].start()
        feat_sib[0][i].start()
    loads[3].wait()
    coefb[0, s] = cur[...].astype(jnp.bfloat16)
    share_own(0)
    loads[2].wait()
    pick_labels(0, hots)
    pick_labels(1, pick(1))
    loads[4].wait()

    def square(j, _):
        cols = pl.ds(pl.multiple_of(j * own, own), own)
        block = cen[:, cols].astype(jnp.float32)
        csq[:, cols] = jnp.sum(block * block, axis=0, keepdims=True)
        return 0

    lax.fori_loop(0, cen_dev // own, square, 0)

    share_hop(0, 0)
    feat_far[0][0].wait_recv()
    feat_fwd[0][0].start()
    share_hop(0, 1)
    feat_sib[0][0].wait_recv()
    feat_fwd[0][0].wait_recv()
    laplace(0, 0, 0, tiles // 2)
    share_hop(0, 2)
    laplace(0, 0, tiles // 2, tiles)
    feat_far[0][1].wait_recv()
    feat_fwd[0][1].start()
    share_end(0)
    logits(0, 0)
    feat_sib[0][1].wait_recv()
    feat_fwd[0][1].wait_recv()
    laplace(0, 1, 0, tiles // 2)
    chip_sum(0, 0)
    laplace(0, 1, tiles // 2, tiles)
    logits(0, 1)
    residual(0, 0)
    chip_sum(0, 1)
    for i in range(CHUNKS):
        feat_far[1][i].start()
        feat_sib[1][i].start()
    residual(0, 1)

    gradient(0)
    chain(0, 0)
    feat_far[1][0].wait_recv()
    feat_fwd[1][0].start()
    chain(0, 1)
    feat_sib[1][0].wait_recv()
    feat_fwd[1][0].wait_recv()
    laplace(1, 0, 0, 1)
    chain(0, 2)
    laplace(1, 0, 1, 2)
    chain(0, 3)
    fresh = cur[...] - rate * gown[3]
    cur[...] = fresh
    coefb[1, s] = fresh.astype(jnp.bfloat16)
    share_own(1)
    feat_far[1][1].wait_recv()
    feat_fwd[1][1].start()
    laplace(1, 0, 2, tiles)
    feat_sib[1][1].wait_recv()
    feat_fwd[1][1].wait_recv()
    share_hop(1, 0)
    laplace(1, 1, 0, 1)
    share_hop(1, 1)
    laplace(1, 1, 1, 2)
    share_hop(1, 2)
    laplace(1, 1, 2, tiles)
    share_end(1)
    for i in range(CHUNKS):
        logits(1, i)
    for i in range(CHUNKS):
        chip_sum(1, i)
    for i in range(CHUNKS):
        residual(1, i)
    gradient(1)
    for p in range(4):
        chain(1, p)
    out_ref[...] = cur[...] - rate * gown[3]

    for copy in everyone:
        copy.wait_send()

    @pl.when(is_outer)
    def _():
        for copy in outers:
            copy.wait_send()

    @pl.when(is_inner)
    def _():
        for copy in inners:
            copy.wait_send()


def line_device(n_c, n_s, centres, pool, labels, picks, coefs):
    width, cen_dev = centres.shape
    fd, pool_dev = pool.shape
    steps, batch = picks.shape
    classes, own = coefs.shape
    half = batch // CHUNKS // 2
    bf16, f32 = jnp.bfloat16, jnp.float32
    anyspace = pl.BlockSpec(memory_space=pl.ANY)
    dma = pltpu.SemaphoreType.DMA
    copies = steps * (6 * CHUNKS + (4 + 3 + 2 + 4 + 1 + 3 + 2) * PIECES)
    return pl.pallas_call(
        functools.partial(
            line_kernel, LOGIT_GAIN / (cen_dev * n_c), STEP_GAIN * LOGIT_GAIN / (batch * n_s)
        ),
        out_shape=jax.ShapeDtypeStruct((classes, own), f32),
        in_specs=[anyspace] * 5,
        out_specs=pl.BlockSpec(memory_space=pltpu.VMEM),
        scratch_shapes=[
            pltpu.VMEM((width, cen_dev), bf16),
            pltpu.VMEM((fd, pool_dev), bf16),
            pltpu.VMEM((1, pool_dev), jnp.int32),
            pltpu.VMEM((steps, batch), jnp.int32),
            pltpu.VMEM((classes, own), f32),
            pltpu.VMEM((1, cen_dev), f32),
            pltpu.VMEM((steps, n_c, batch, fd), bf16),
            pltpu.VMEM((steps, n_s, batch, own), bf16),
            pltpu.VMEM((steps, 2 * CHUNKS, 8, half), f32),
            pltpu.VMEM((steps, n_s, classes, own), bf16),
            pltpu.VMEM((steps, CHUNKS, 2, classes, half), f32),
            pltpu.VMEM((steps, CHUNKS, classes, half), f32),
            pltpu.VMEM((steps, CHUNKS, classes, half), f32),
            pltpu.VMEM((steps, CHUNKS, classes, half), f32),
            pltpu.VMEM((steps, CHUNKS, 2, classes, half), bf16),
            pltpu.VMEM((4, classes, own), f32),
            pltpu.VMEM((steps, 4, classes, own), jnp.int16),
            pltpu.VMEM((steps, 4, classes, own), jnp.int16),
            pltpu.VMEM((steps, 3, classes, own), jnp.int16),
            pltpu.VMEM((steps, 3, classes, own), jnp.int16),
            pltpu.VMEM((steps, 2, classes, own), jnp.int16),
            pltpu.VMEM((steps, 2, classes, own), jnp.int16),
            dma((5,)),
            dma((copies,)),
            dma((steps, 3, CHUNKS)),
            dma((steps, 3, CHUNKS)),
            dma((steps, 4, PIECES)),
            dma((steps, 3, PIECES)),
            dma((steps, 2, PIECES)),
            dma((steps, 4, PIECES)),
            dma((steps, 3, PIECES)),
            dma((steps, 2, PIECES)),
        ],
        compiler_params=pltpu.CompilerParams(
            collective_id=0, has_side_effects=True, vmem_limit_bytes=60 * 1024 * 1024
        ),
    )(centres, pool, labels.reshape(1, pool_dev), picks, coefs)


def suits_line(mesh, centres, pool, picks, coefs):
    n_c, n_s = mesh.shape["centre"], mesh.shape["sample"]
    own, batch, fd = coefs.shape[1], picks.shape[1], pool.shape[0]
    return (
        n_c == 4 and n_s == 8 and own % 128 == 0 and fd % 128 == 0 and picks.shape[0] == 2
        and batch % (256 * CHUNKS) == 0 and coefs.shape[0] % (16 * PIECES) == 0 and batch * n_s <= 4096
    )


def on_device(mesh, centres, pool, labels, picks, coefs):
    n_c, n_s = mesh.shape["centre"], mesh.shape["sample"]
    if suits_line(mesh, centres, pool, picks, coefs):
        return line_device(n_c, n_s, centres, pool, labels, picks, coefs)
    width, cen_dev = centres.shape
    fd, pool_dev = pool.shape
    steps, batch = picks.shape
    classes, own = coefs.shape
    share = batch // n_c
    bf16, f32 = jnp.bfloat16, jnp.float32
    body = functools.partial(
        kernel, n_c, n_s, LOGIT_GAIN / (cen_dev * n_c), STEP_GAIN * LOGIT_GAIN / (batch * n_s)
    )
    vmem = pl.BlockSpec(memory_space=pltpu.VMEM)
    return pl.pallas_call(
        body,
        out_shape=jax.ShapeDtypeStruct((classes, own), f32),
        in_specs=[pl.BlockSpec(memory_space=pl.ANY)] + [vmem] * 4,
        out_specs=vmem,
        scratch_shapes=[
            pltpu.VMEM((width, cen_dev), bf16),
            pltpu.VMEM((1, cen_dev), f32),
            pltpu.VMEM((steps, n_c, batch, fd), bf16),
            pltpu.VMEM((steps, n_s, batch, own), bf16),
            pltpu.VMEM((steps, n_c, 8, share), f32),
            pltpu.VMEM((steps, n_s, classes, own), bf16),
            pltpu.VMEM((steps, n_c, classes, share), LOGIT_WIRE),
            pltpu.VMEM((steps, n_c - 1, classes, share), LOGIT_WIRE),
            pltpu.VMEM((steps, n_c, classes, share), bf16),
            pltpu.VMEM((steps, n_s - 2, classes, own), GRAD_WIRE),
            pltpu.VMEM((steps, n_s - 2, classes, own), GRAD_WIRE),
            pltpu.VMEM((steps, classes, own), f32),
            pltpu.VMEM((steps, classes, own), f32),
            pltpu.VMEM((classes, own), f32),
            pltpu.SemaphoreType.DMA,
            pltpu.SemaphoreType.DMA((steps * (3 * (n_c - 1) + 2 * (n_s - 1)),)),
            pltpu.SemaphoreType.DMA((steps, n_c - 1)),
            pltpu.SemaphoreType.DMA((steps, n_c - 1)),
            pltpu.SemaphoreType.DMA((steps, n_c - 1)),
            pltpu.SemaphoreType.DMA((steps, n_s - 1)),
            pltpu.SemaphoreType.DMA((steps, n_s - 1)),
        ],
        compiler_params=pltpu.CompilerParams(
            collective_id=0, has_side_effects=True, vmem_limit_bytes=60 * 1024 * 1024
        ),
    )(centres, pool, labels.reshape(1, pool_dev), picks, coefs)


def solution(mesh):
    placed = (
        P(None, "centre"),
        P("centre", "sample"),
        P("sample"),
        P(None, "sample"),
        P(None, ("centre", "sample")),
    )
    return jax.shard_map(
        functools.partial(on_device, mesh),
        mesh=mesh,
        in_specs=placed,
        out_specs=P(None, ("centre", "sample")),
        check_vma=False,
    )
```

```python
import functools
import math

import jax
import jax.numpy as jnp
from jax import lax
from jax.experimental import pallas as pl
from jax.experimental.pallas import tpu as pltpu
from jax.sharding import PartitionSpec as P

LOGIT_GAIN = 16.0
LENGTH_SCALE = 0.5
STEP_GAIN = 2048.0
EPS = 1e-06

GRAD_WIRE = jnp.bfloat16
LOGIT_WIRE = jnp.float32
MESH = pl.DeviceIdType.MESH
NT = (((1,), (1,)), ((), ()))


def kernel(
    n_c, n_s, logit_scale, rate,
    cen_hbm, pool_ref, labels_ref, picks_ref, coefs_ref, out_ref,
    cen, csq, feats, kern, labs, coefb, lsend, lrecv, resid, gsend, grecv, psend, precv, cur,
    cen_sem, send_sem, feat_sem, log_sem, res_sem, coef_sem, grad_sem,
):
    steps, batch = picks_ref.shape
    fd, pool_dev = pool_ref.shape
    classes, own = coefs_ref.shape
    width, cen_dev = cen.shape
    share = batch // n_c
    ny = n_c // 2
    tile = max(own, min(256, cen_dev))
    pieces = tile // own

    c = lax.axis_index("centre")
    s = lax.axis_index("sample")
    sib = c + 1 - 2 * lax.rem(c, 2)
    c_peers = [lax.rem(c + r, n_c) for r in range(1, n_c)]
    s_peers = [lax.rem(s + r, n_s) for r in range(1, n_s)]
    pair = s + 1 - 2 * lax.rem(s, 2)
    nz = n_s // 2
    order = sorted(range(1, nz), key=lambda q: -min(q, nz - q))

    barrier = pltpu.get_barrier_semaphore()
    for peer in c_peers:
        pl.semaphore_signal(barrier, inc=1, device_id={"centre": peer}, device_id_type=MESH)
    for peer in s_peers:
        pl.semaphore_signal(barrier, inc=1, device_id={"sample": peer}, device_id_type=MESH)

    load = pltpu.make_async_copy(cen_hbm, cen, cen_sem)
    load.start()
    started = []

    def send(src, dst, recv, axis, peer):
        copy = pltpu.make_async_remote_copy(
            src_ref=src, dst_ref=dst, send_sem=send_sem.at[len(started)], recv_sem=recv,
            device_id={axis: peer}, device_id_type=MESH,
        )
        copy.start()
        started.append(copy)
        return copy

    label_rows = jnp.broadcast_to(labels_ref[...].astype(jnp.float32), (16, pool_dev)).astype(jnp.bfloat16)

    def pick(t):
        chosen = picks_ref[t:t + 1, :] - s * pool_dev
        rows = lax.broadcasted_iota(jnp.int32, (pool_dev, batch), 0)
        hot = jnp.where(rows == chosen, -2.0, 0.0).astype(jnp.bfloat16)
        got = jnp.dot(pool_ref[...], hot, preferred_element_type=jnp.float32)
        feats[t, c] = got.T.astype(jnp.bfloat16)
        lab = -0.5 * jnp.dot(label_rows, hot, preferred_element_type=jnp.float32)
        for k in range(n_c):
            labs[t, k] = lab[0:8, k * share:(k + 1) * share]

    def send_feats(t):
        mine = feats.at[t, c]
        direct = []
        for q in range(1, ny):
            direct.append(send(mine, mine, feat_sem.at[t, q], "centre", lax.rem(c + 2 * q, n_c)))
        return [send(mine, mine, feat_sem.at[t, 0], "centre", sib)], direct

    def forward_feats(t, near, direct):
        for q, copy in enumerate(direct, 1):
            copy.wait_recv()
            slot = feats.at[t, lax.rem(c - 2 * q + n_c, n_c)]
            near.append(send(slot, slot, feat_sem.at[t, ny - 1 + q], "centre", sib))
        for copy in near:
            copy.wait_recv()

    def send_coefs(t):
        mine = coefb.at[t, s]
        direct = [
            (q, send(mine, mine, coef_sem.at[t, q], "sample", lax.rem(s + 2 * q, n_s)))
            for q in order
        ]
        return [send(mine, mine, coef_sem.at[t, 0], "sample", pair)], direct

    def forward_coefs(t, near, direct):
        for q, copy in direct:
            copy.wait_recv()
            slot = coefb.at[t, lax.rem(s - 2 * q + n_s, n_s)]
            near.append(send(slot, slot, coef_sem.at[t, nz - 1 + q], "sample", pair))

    cur[...] = coefs_ref[...]
    coefb[0, s] = coefs_ref[...].astype(jnp.bfloat16)
    pl.semaphore_wait(barrier, n_c - 1 + n_s - 1)
    coef_near, coef_direct = send_coefs(0)
    pick(0)
    moves = [send_feats(0)]
    pick(1)
    moves.append(send_feats(1))

    load.wait()

    def square(j, _):
        cols = pl.ds(pl.multiple_of(j * tile, tile), tile)
        block = cen[:, cols].astype(jnp.float32)
        csq[:, cols] = jnp.sum(block * block, axis=0, keepdims=True)
        return 0

    lax.fori_loop(0, cen_dev // tile, square, 0)

    bend = (1.0 / (LENGTH_SCALE * math.log(2.0))) ** 2

    def laplace(t):
        parts = [feats[t, k] for k in range(n_c)]
        ssq = sum(
            jnp.sum(jnp.square(p.astype(jnp.float32)), axis=1, keepdims=True) for p in parts
        ) * 0.25
        if fd % 128 == 0:
            parts = [jnp.concatenate(parts, axis=1)]
        deep = width // len(parts)

        def body(j, _):
            cols = pl.ds(pl.multiple_of(j * tile, tile), tile)
            cross = sum(
                jnp.dot(p, cen[k * deep:(k + 1) * deep, cols], preferred_element_type=jnp.float32)
                for k, p in enumerate(parts)
            )
            arg = ((ssq + csq[:, cols]) + cross) * (bend / width) + bend * EPS
            arg = jnp.maximum(arg, 1e-30)
            value = jnp.exp2(-(arg * lax.rsqrt(arg)))
            for k in range(pieces):
                kern[t, j * pieces + k] = value[:, k * own:(k + 1) * own].astype(jnp.bfloat16)
            return 0

        lax.fori_loop(0, cen_dev // tile, body, 0)

    def residual(t):
        part = sum(
            lax.dot_general(coefb[t, j], kern[t, j], NT, preferred_element_type=jnp.float32)
            for j in range(n_s)
        )
        for k in range(n_c):
            lsend[t, k] = part[:, k * share:(k + 1) * share].astype(LOGIT_WIRE)
        copies = [
            send(lsend.at[t, peer], lrecv.at[t, r], log_sem.at[t, r], "centre", peer)
            for r, peer in enumerate(c_peers)
        ]
        if t + 1 < steps:
            forward_feats(t + 1, *moves[t + 1])
        total = lsend[t, c].astype(jnp.float32)
        for r, copy in enumerate(copies):
            copy.wait_recv()
            total = total + lrecv[t, r].astype(jnp.float32)
        logits = total * logit_scale
        expo = jnp.exp(logits - jnp.max(logits, axis=0, keepdims=True))
        probs = expo / jnp.sum(expo, axis=0, keepdims=True)
        ids = lax.broadcasted_iota(jnp.int32, (classes, share), 0).astype(jnp.float32)
        hot = jnp.where(ids == labs[t, c][0:1, :], 1.0, 0.0)
        resid[t, c] = (probs - hot).astype(jnp.bfloat16)
        mine = resid.at[t, c]
        copies = [
            send(mine, mine, res_sem.at[t, r], "centre", peer) for r, peer in enumerate(c_peers)
        ]
        for copy in copies:
            copy.wait_recv()

    def gradient(t):
        if share % 128 == 0:
            whole = jnp.concatenate([resid[t, k] for k in range(n_c)], axis=1)

            def grad(j):
                return jnp.dot(whole, kern[t, j], preferred_element_type=jnp.float32)
        else:
            def grad(j):
                return sum(
                    jnp.dot(resid[t, k], kern[t, j, k * share:(k + 1) * share, :],
                            preferred_element_type=jnp.float32)
                    for k in range(n_c)
                )
        def put(i, value, peer):
            gsend[t, i] = value.astype(GRAD_WIRE)
            return send(gsend.at[t, i], grecv.at[t, i], grad_sem.at[t, i], "sample", peer)

        far = [lax.rem(start + 2 * q, n_s) for q in order for start in (s, pair)]
        copies = [put(i, grad(peer), peer) for i, peer in enumerate(far)]
        psend[t] = grad(pair)
        last = send(psend.at[t], precv.at[t], grad_sem.at[t, n_s - 2], "sample", pair)
        return grad(s), last, copies

    forward_coefs(0, coef_near, coef_direct[:2])
    forward_feats(0, *moves[0])
    forward_coefs(0, coef_near, coef_direct[2:])
    laplace(0)
    for t in range(steps):
        for copy in coef_near:
            copy.wait_recv()
        residual(t)
        total, last, copies = gradient(t)
        if t + 1 < steps:
            laplace(t + 1)
        last.wait_recv()
        total = total + precv[t]
        for r, copy in enumerate(copies):
            copy.wait_recv()
            total = total + grecv[t, r].astype(jnp.float32)
        fresh = cur[...] - rate * total
        if t + 1 < steps:
            cur[...] = fresh
            coefb[t + 1, s] = fresh.astype(jnp.bfloat16)
            coef_near, coef_direct = send_coefs(t + 1)
            forward_coefs(t + 1, coef_near, coef_direct)
        else:
            out_ref[...] = fresh
    for copy in started:
        copy.wait_send()


CHUNKS = 2
PIECES = 3
LOG_STEPS = 520.0
LOG_LOW = 50.0


def encode(value):
    size = jnp.maximum(jnp.abs(value), 2.0 ** -LOG_LOW)
    code = jnp.round((jnp.log(size) * (1.0 / math.log(2.0)) + LOG_LOW) * LOG_STEPS)
    return jnp.where(value < 0.0, -code, code).astype(jnp.int16)


def decode(code):
    number = code.astype(jnp.float32)
    size = jnp.exp2(jnp.abs(number) * (1.0 / LOG_STEPS) - LOG_LOW)
    return jnp.where(number < 0.0, -size, jnp.where(number > 0.0, size, 0.0))


def line_kernel(
    logit_scale, rate,
    cen_hbm, pool_hbm, labels_hbm, picks_hbm, coefs_hbm, out_ref,
    cen, pool_ref, labels_ref, picks_ref, cur,
    csq, feats, kern, labs, coefb, lacc, lpart, lrecv, lsum, ysum, resid, gown,
    near_out, near_in, cross_out, cross_in,
    load_sem, send_sem, feat_sem, log_sem, near_sem, cross_sem, mine_sem, over_sem, pass_sem,
):
    steps, batch = picks_ref.shape
    fd, pool_dev = pool_ref.shape
    classes, own = cur.shape
    width, cen_dev = cen.shape
    rows_n = batch // CHUNKS
    half = rows_n // 2
    piece = classes // PIECES
    tile = 2 * own
    tiles = cen_dev // tile

    c = lax.axis_index("centre")
    s = lax.axis_index("sample")
    y, k = lax.div(c, 2), lax.rem(c, 2)
    z, x = lax.div(s, 2), lax.rem(s, 2)
    z_near = z + 1 - 2 * lax.rem(z, 2)
    z_over = lax.rem(z + 2, 4)
    z_both = lax.rem(z_near + 2, 4)
    far_c = (1 - y) * 2 + k
    sib = {"centre": c + 1 - 2 * k}
    far = {"centre": far_c}
    over = {"sample": z_over * 2 + x}
    quad = [z * 2 + 1 - x, z_near * 2 + x, z_near * 2 + 1 - x]
    across = [z_over * 2 + 1 - x, z_both * 2 + x, z_both * 2 + 1 - x]
    near = [{"sample": q} for q in quad]

    barrier = pltpu.get_barrier_semaphore()
    for peer in [sib, far, over] + near:
        pl.semaphore_signal(barrier, inc=1, device_id=peer, device_id_type=MESH)

    loads = [
        pltpu.make_async_copy(src, dst, load_sem.at[i])
        for i, (src, dst) in enumerate(
            [(picks_hbm, picks_ref), (pool_hbm, pool_ref), (labels_hbm, labels_ref), (coefs_hbm, cur), (cen_hbm, cen)]
        )
    ]
    for i in (3, 0, 1, 2, 4):
        loads[i].start()

    def make(kind, t, src, dst, recv, peer):
        return pltpu.make_async_remote_copy(
            src_ref=src, dst_ref=dst, send_sem=send_sem.at[kind, t], recv_sem=recv,
            device_id=peer, device_id_type=MESH,
        )

    def rows_of(i):
        return slice(i * rows_n, (i + 1) * rows_n)

    def piece_of(h):
        return slice(h * piece, (h + 1) * piece)

    def feat_copy(t, i, owner, n, peer):
        slot = feats.at[t, owner, rows_of(i)]
        return make(0, t, slot, slot, feat_sem.at[t, n, i], peer)

    def feat_far(t, i):
        return feat_copy(t, i, c, 0, far)

    def feat_sib(t, i):
        return feat_copy(t, i, c, 1, sib)

    def feat_fwd(t, i):
        return feat_copy(t, i, far_c, 2, sib)

    def log_sib(t, i):
        return make(1, t, lpart.at[t, i, 1 - k], lrecv.at[t, i], log_sem.at[0, t, i], sib)

    def log_far(t, i):
        return make(1, t, lsum.at[t, i], ysum.at[t, i], log_sem.at[1, t, i], far)

    def res_sib(t, i):
        return make(2, t, resid.at[t, i, k], resid.at[t, i, k], log_sem.at[2, t, i], sib)

    def sum_near(t, n, q, h):
        rows = piece_of(h)
        return make(3, t, near_out.at[t, n, q, rows], near_in.at[t, n, q, rows], near_sem.at[n, q, h], near[q])

    def sum_over(t, h):
        rows = piece_of(h)
        return make(4, t, cross_out.at[t, rows], cross_in.at[t, rows], cross_sem.at[h], over)

    def coef_mine(t, q):
        return make(5, t, coefb.at[t, s], coefb.at[t, s], mine_sem.at[q], near[q])

    def coef_over(t, h):
        slot = coefb.at[t, s, piece_of(h)]
        return make(5, t, slot, slot, over_sem.at[h], over)

    def coef_pass(t, q, h):
        slot = coefb.at[t, z_over * 2 + x, piece_of(h)]
        return make(5, t, slot, slot, pass_sem.at[q, h], near[q])

    def pick(t):
        chosen = picks_ref[t:t + 1, :] - s * pool_dev
        rows = lax.broadcasted_iota(jnp.int32, (pool_dev, batch), 0)
        hot = jnp.where(rows == chosen, -2.0, 0.0).astype(jnp.bfloat16)
        got = jnp.dot(pool_ref[...], hot, preferred_element_type=jnp.float32)
        feats[t, c] = got.T.astype(jnp.bfloat16)
        return hot

    def pick_labels(t, hot):
        label_rows = jnp.broadcast_to(labels_ref[...].astype(jnp.float32), (16, pool_dev)).astype(jnp.bfloat16)
        lab = -0.5 * jnp.dot(label_rows, hot, preferred_element_type=jnp.float32)
        for n in range(2 * CHUNKS):
            labs[t, n] = lab[0:8, n * half:(n + 1) * half]

    bend = (1.0 / (LENGTH_SCALE * math.log(2.0))) ** 2

    def laplace(t, i, first, last):
        rows = rows_of(i)
        ssq = sum(
            jnp.sum(jnp.square(feats[t, q, rows].astype(jnp.float32)), axis=1, keepdims=True) for q in range(4)
        ) * 0.25

        def body(j, _):
            cols = pl.ds(pl.multiple_of(j * tile, tile), tile)
            lhs = jnp.concatenate([feats[t, q, rows] for q in range(4)], axis=1)
            cross = jnp.dot(lhs, cen[:, cols], preferred_element_type=jnp.float32)
            arg = ((ssq + csq[:, cols]) + cross) * (bend / width) + bend * EPS
            arg = jnp.maximum(arg, 1e-30)
            value = jnp.exp2(-(arg * lax.rsqrt(arg)))
            for q in range(2):
                kern[t, j * 2 + q, rows] = value[:, q * own:(q + 1) * own].astype(jnp.bfloat16)
            return 0

        lax.fori_loop(first, last, body, 0)

    def logits(t, i, group, first, last):
        part = sum(
            lax.dot_general(coefb[t, j], kern[t, j, rows_of(i)], NT, preferred_element_type=jnp.float32)
            for j in group
        )
        if not first:
            part = part + lacc[i]
        if not last:
            lacc[i] = part
            return
        for h in range(2):
            lpart[t, i, h] = part[:, h * half:(h + 1) * half]
        log_sib(t, i).start()

    def chip_sum(t, i):
        log_sib(t, i).wait_recv()
        lsum[t, i] = lpart[t, i, k] + lrecv[t, i]
        log_far(t, i).start()

    def residual(t, i):
        log_far(t, i).wait_recv()
        value = (lsum[t, i] + ysum[t, i]) * logit_scale
        expo = jnp.exp(value - jnp.max(value, axis=0, keepdims=True))
        probs = expo / jnp.sum(expo, axis=0, keepdims=True)
        ids = lax.broadcasted_iota(jnp.int32, (classes, half), 0).astype(jnp.float32)
        hot = jnp.where(ids == labs[t, 2 * i + k][0:1, :], 1.0, 0.0)
        resid[t, i, k] = (probs - hot).astype(jnp.bfloat16)
        res_sib(t, i).start()

    def gradient(t):
        for i in range(CHUNKS):
            res_sib(t, i).wait_recv()
        whole = jnp.concatenate([resid[t, i, h] for i in range(CHUNKS) for h in range(2)], axis=1)

        def grad(block):
            return jnp.dot(whole, kern[t, block], preferred_element_type=jnp.float32)

        parts = [grad(block) for block in across]
        for h in range(PIECES):
            for q in range(3):
                near_out[t, 0, q, piece_of(h)] = encode(parts[q][piece_of(h)])
                sum_near(t, 0, q, h).start()
        for q in range(3):
            near_out[t, 1, q] = encode(grad(quad[q]))
            for h in range(PIECES):
                sum_near(t, 1, q, h).start()
        gown[0] = grad(z_over * 2 + x)
        gown[1] = grad(s)

    def reduce_near(t, n, h):
        total = gown[n, piece_of(h)]
        for q in range(3):
            sum_near(t, n, q, h).wait_recv()
            total = total + decode(near_in[t, n, q, piece_of(h)])
        return total

    def reduce_across(t, h):
        cross_out[t, piece_of(h)] = encode(reduce_near(t, 0, h))
        sum_over(t, h).start()

    def reduce_end(t, h):
        total = reduce_near(t, 1, h)
        sum_over(t, h).wait_recv()
        return total + decode(cross_in[t, piece_of(h)])

    def share_mine(t):
        for h in range(PIECES):
            coef_over(t, h).start()
        for q in range(3):
            coef_mine(t, q).start()

    def share_pass(t, h):
        coef_over(t, h).wait_recv()
        for q in range(3):
            coef_pass(t, q, h).start()

    def share_near(t):
        for q in range(3):
            coef_mine(t, q).wait_recv()

    def share_end(t):
        for q in range(3):
            for h in range(PIECES):
                coef_pass(t, q, h).wait_recv()

    first_group = [s] + quad + [z_over * 2 + x]

    pl.semaphore_wait(barrier, 6)
    loads[3].wait()
    coefb[0, s] = cur[...].astype(jnp.bfloat16)
    share_mine(0)
    loads[0].wait()
    loads[1].wait()
    hots = pick(0)
    for i in range(CHUNKS):
        feat_far(0, i).start()
        feat_sib(0, i).start()
    loads[2].wait()
    pick_labels(0, hots)
    pick_labels(1, pick(1))
    loads[4].wait()

    def square(j, _):
        cols = pl.ds(pl.multiple_of(j * own, own), own)
        block = cen[:, cols].astype(jnp.float32)
        csq[:, cols] = jnp.sum(block * block, axis=0, keepdims=True)
        return 0

    lax.fori_loop(0, cen_dev // own, square, 0)

    for h in range(PIECES):
        share_pass(0, h)
    feat_far(0, 0).wait_recv()
    feat_fwd(0, 0).start()
    feat_sib(0, 0).wait_recv()
    feat_fwd(0, 0).wait_recv()
    laplace(0, 0, 0, tiles)
    feat_far(0, 1).wait_recv()
    feat_fwd(0, 1).start()
    share_near(0)
    share_end(0)
    logits(0, 0, first_group + across, True, True)
    feat_sib(0, 1).wait_recv()
    feat_fwd(0, 1).wait_recv()
    laplace(0, 1, 0, tiles // 2)
    chip_sum(0, 0)
    laplace(0, 1, tiles // 2, tiles)
    logits(0, 1, first_group + across, True, True)
    residual(0, 0)
    chip_sum(0, 1)
    for i in range(CHUNKS):
        feat_far(1, i).start()
        feat_sib(1, i).start()
    residual(0, 1)

    gradient(0)
    feat_far(1, 0).wait_recv()
    feat_fwd(1, 0).start()
    feat_sib(1, 0).wait_recv()
    reduce_across(0, 0)
    feat_fwd(1, 0).wait_recv()
    reduce_across(0, 1)
    laplace(1, 0, 0, 1)
    reduce_across(0, 2)
    feat_far(1, 1).wait_recv()
    feat_fwd(1, 1).start()
    laplace(1, 0, 1, tiles)
    for h in range(PIECES):
        rows = piece_of(h)
        fresh = cur[rows] - rate * reduce_end(0, h)
        cur[rows] = fresh
        coefb[1, s, rows] = fresh.astype(jnp.bfloat16)
        coef_over(1, h).start()
    for q in range(3):
        coef_mine(1, q).start()
    feat_sib(1, 1).wait_recv()
    feat_fwd(1, 1).wait_recv()
    laplace(1, 1, 0, tiles)
    for h in range(PIECES):
        share_pass(1, h)
    share_near(1)
    for i in range(CHUNKS):
        logits(1, i, first_group, True, False)
    share_end(1)
    for i in range(CHUNKS):
        logits(1, i, across, False, True)
    for i in range(CHUNKS):
        chip_sum(1, i)
    for i in range(CHUNKS):
        residual(1, i)
    gradient(1)
    for h in range(PIECES):
        reduce_across(1, h)
    for h in range(PIECES):
        out_ref[piece_of(h)] = cur[piece_of(h)] - rate * reduce_end(1, h)

    def drain(kind, t, ref):
        make(kind, t, ref, ref, cross_sem.at[0], over).wait_send()

    for t in range(steps):
        drain(0, t, feats.at[t, 0:3])
        drain(1, t, lpart.at[t])
        drain(2, t, resid.at[t, 0])
        drain(3, t, near_out.at[t])
        drain(4, t, cross_out.at[t])
        drain(5, t, coefb.at[t, 0:7])


def line_device(n_c, n_s, centres, pool, labels, picks, coefs):
    width, cen_dev = centres.shape
    fd, pool_dev = pool.shape
    steps, batch = picks.shape
    classes, own = coefs.shape
    half = batch // CHUNKS // 2
    bf16, f32, i16 = jnp.bfloat16, jnp.float32, jnp.int16
    dma = pltpu.SemaphoreType.DMA
    return pl.pallas_call(
        functools.partial(
            line_kernel, LOGIT_GAIN / (cen_dev * n_c), STEP_GAIN * LOGIT_GAIN / (batch * n_s)
        ),
        out_shape=pltpu.VMEM((classes, own), f32),
        in_specs=[pl.BlockSpec(memory_space=pltpu.HBM)] * 5,
        out_specs=pl.BlockSpec(memory_space=pltpu.VMEM),
        scratch_shapes=[
            pltpu.VMEM((width, cen_dev), bf16),
            pltpu.VMEM((fd, pool_dev), bf16),
            pltpu.VMEM((1, pool_dev), jnp.int32),
            pltpu.VMEM((steps, batch), jnp.int32),
            pltpu.VMEM((classes, own), f32),
            pltpu.VMEM((1, cen_dev), f32),
            pltpu.VMEM((steps, n_c, batch, fd), bf16),
            pltpu.VMEM((steps, n_s, batch, own), bf16),
            pltpu.VMEM((steps, 2 * CHUNKS, 8, half), f32),
            pltpu.VMEM((steps, n_s, classes, own), bf16),
            pltpu.VMEM((CHUNKS, classes, 2 * half), f32),
            pltpu.VMEM((steps, CHUNKS, 2, classes, half), f32),
            pltpu.VMEM((steps, CHUNKS, classes, half), f32),
            pltpu.VMEM((steps, CHUNKS, classes, half), f32),
            pltpu.VMEM((steps, CHUNKS, classes, half), f32),
            pltpu.VMEM((steps, CHUNKS, 2, classes, half), bf16),
            pltpu.VMEM((2, classes, own), f32),
            pltpu.VMEM((steps, 2, 3, classes, own), i16),
            pltpu.VMEM((steps, 2, 3, classes, own), i16),
            pltpu.VMEM((steps, classes, own), i16),
            pltpu.VMEM((steps, classes, own), i16),
            dma((5,)),
            dma((6, steps)),
            dma((steps, 3, CHUNKS)),
            dma((3, steps, CHUNKS)),
            dma((2, 3, PIECES)),
            dma((PIECES,)),
            dma((3,)),
            dma((PIECES,)),
            dma((3, PIECES)),
        ],
        compiler_params=pltpu.CompilerParams(
            collective_id=0, has_side_effects=True, vmem_limit_bytes=60 * 1024 * 1024
        ),
    )(centres, pool, labels.reshape(1, pool_dev), picks, coefs)


def suits_line(mesh, centres, pool, picks, coefs):
    n_c, n_s = mesh.shape["centre"], mesh.shape["sample"]
    own, batch, fd = coefs.shape[1], picks.shape[1], pool.shape[0]
    return (
        n_c == 4 and n_s == 8 and own % 128 == 0 and fd % 128 == 0 and picks.shape[0] == 2
        and batch % (256 * CHUNKS) == 0 and coefs.shape[0] % (16 * PIECES) == 0 and batch * n_s <= 4096
    )


def on_device(mesh, centres, pool, labels, picks, coefs):
    n_c, n_s = mesh.shape["centre"], mesh.shape["sample"]
    if suits_line(mesh, centres, pool, picks, coefs):
        return line_device(n_c, n_s, centres, pool, labels, picks, coefs)
    width, cen_dev = centres.shape
    fd, pool_dev = pool.shape
    steps, batch = picks.shape
    classes, own = coefs.shape
    share = batch // n_c
    bf16, f32 = jnp.bfloat16, jnp.float32
    body = functools.partial(
        kernel, n_c, n_s, LOGIT_GAIN / (cen_dev * n_c), STEP_GAIN * LOGIT_GAIN / (batch * n_s)
    )
    vmem = pl.BlockSpec(memory_space=pltpu.VMEM)
    return pl.pallas_call(
        body,
        out_shape=jax.ShapeDtypeStruct((classes, own), f32),
        in_specs=[pl.BlockSpec(memory_space=pl.ANY)] + [vmem] * 4,
        out_specs=vmem,
        scratch_shapes=[
            pltpu.VMEM((width, cen_dev), bf16),
            pltpu.VMEM((1, cen_dev), f32),
            pltpu.VMEM((steps, n_c, batch, fd), bf16),
            pltpu.VMEM((steps, n_s, batch, own), bf16),
            pltpu.VMEM((steps, n_c, 8, share), f32),
            pltpu.VMEM((steps, n_s, classes, own), bf16),
            pltpu.VMEM((steps, n_c, classes, share), LOGIT_WIRE),
            pltpu.VMEM((steps, n_c - 1, classes, share), LOGIT_WIRE),
            pltpu.VMEM((steps, n_c, classes, share), bf16),
            pltpu.VMEM((steps, n_s - 2, classes, own), GRAD_WIRE),
            pltpu.VMEM((steps, n_s - 2, classes, own), GRAD_WIRE),
            pltpu.VMEM((steps, classes, own), f32),
            pltpu.VMEM((steps, classes, own), f32),
            pltpu.VMEM((classes, own), f32),
            pltpu.SemaphoreType.DMA,
            pltpu.SemaphoreType.DMA((steps * (3 * (n_c - 1) + 2 * (n_s - 1)),)),
            pltpu.SemaphoreType.DMA((steps, n_c - 1)),
            pltpu.SemaphoreType.DMA((steps, n_c - 1)),
            pltpu.SemaphoreType.DMA((steps, n_c - 1)),
            pltpu.SemaphoreType.DMA((steps, n_s - 1)),
            pltpu.SemaphoreType.DMA((steps, n_s - 1)),
        ],
        compiler_params=pltpu.CompilerParams(
            collective_id=0, has_side_effects=True, vmem_limit_bytes=60 * 1024 * 1024
        ),
    )(centres, pool, labels.reshape(1, pool_dev), picks, coefs)


def solution(mesh):
    placed = (
        P(None, "centre"),
        P("centre", "sample"),
        P("sample"),
        P(None, "sample"),
        P(None, ("centre", "sample")),
    )
    return jax.shard_map(
        functools.partial(on_device, mesh),
        mesh=mesh,
        in_specs=placed,
        out_specs=P(None, ("centre", "sample")),
        check_vma=False,
    )
```

```python
import functools
import math

import jax
import jax.numpy as jnp
from jax import lax
from jax.experimental import pallas as pl
from jax.experimental.pallas import tpu as pltpu
from jax.sharding import PartitionSpec as P

LOGIT_GAIN = 16.0
LENGTH_SCALE = 0.5
STEP_GAIN = 2048.0
EPS = 1e-06

GRAD_WIRE = jnp.bfloat16
LOGIT_WIRE = jnp.float32
MESH = pl.DeviceIdType.MESH
NT = (((1,), (1,)), ((), ()))


def kernel(
    n_c, n_s, logit_scale, rate,
    cen_hbm, pool_ref, labels_ref, picks_ref, coefs_ref, out_ref,
    cen, csq, feats, kern, labs, coefb, lsend, lrecv, resid, gsend, grecv, psend, precv, cur,
    cen_sem, send_sem, feat_sem, log_sem, res_sem, coef_sem, grad_sem,
):
    steps, batch = picks_ref.shape
    fd, pool_dev = pool_ref.shape
    classes, own = coefs_ref.shape
    width, cen_dev = cen.shape
    share = batch // n_c
    ny = n_c // 2
    tile = max(own, min(256, cen_dev))
    pieces = tile // own

    c = lax.axis_index("centre")
    s = lax.axis_index("sample")
    sib = c + 1 - 2 * lax.rem(c, 2)
    c_peers = [lax.rem(c + r, n_c) for r in range(1, n_c)]
    s_peers = [lax.rem(s + r, n_s) for r in range(1, n_s)]
    pair = s + 1 - 2 * lax.rem(s, 2)
    nz = n_s // 2
    order = sorted(range(1, nz), key=lambda q: -min(q, nz - q))

    barrier = pltpu.get_barrier_semaphore()
    for peer in c_peers:
        pl.semaphore_signal(barrier, inc=1, device_id={"centre": peer}, device_id_type=MESH)
    for peer in s_peers:
        pl.semaphore_signal(barrier, inc=1, device_id={"sample": peer}, device_id_type=MESH)

    load = pltpu.make_async_copy(cen_hbm, cen, cen_sem)
    load.start()
    started = []

    def send(src, dst, recv, axis, peer):
        copy = pltpu.make_async_remote_copy(
            src_ref=src, dst_ref=dst, send_sem=send_sem.at[len(started)], recv_sem=recv,
            device_id={axis: peer}, device_id_type=MESH,
        )
        copy.start()
        started.append(copy)
        return copy

    label_rows = jnp.broadcast_to(labels_ref[...].astype(jnp.float32), (16, pool_dev)).astype(jnp.bfloat16)

    def pick(t):
        chosen = picks_ref[t:t + 1, :] - s * pool_dev
        rows = lax.broadcasted_iota(jnp.int32, (pool_dev, batch), 0)
        hot = jnp.where(rows == chosen, -2.0, 0.0).astype(jnp.bfloat16)
        got = jnp.dot(pool_ref[...], hot, preferred_element_type=jnp.float32)
        feats[t, c] = got.T.astype(jnp.bfloat16)
        lab = -0.5 * jnp.dot(label_rows, hot, preferred_element_type=jnp.float32)
        for k in range(n_c):
            labs[t, k] = lab[0:8, k * share:(k + 1) * share]

    def send_feats(t):
        mine = feats.at[t, c]
        direct = []
        for q in range(1, ny):
            direct.append(send(mine, mine, feat_sem.at[t, q], "centre", lax.rem(c + 2 * q, n_c)))
        return [send(mine, mine, feat_sem.at[t, 0], "centre", sib)], direct

    def forward_feats(t, near, direct):
        for q, copy in enumerate(direct, 1):
            copy.wait_recv()
            slot = feats.at[t, lax.rem(c - 2 * q + n_c, n_c)]
            near.append(send(slot, slot, feat_sem.at[t, ny - 1 + q], "centre", sib))
        for copy in near:
            copy.wait_recv()

    def send_coefs(t):
        mine = coefb.at[t, s]
        direct = [
            (q, send(mine, mine, coef_sem.at[t, q], "sample", lax.rem(s + 2 * q, n_s)))
            for q in order
        ]
        return [send(mine, mine, coef_sem.at[t, 0], "sample", pair)], direct

    def forward_coefs(t, near, direct):
        for q, copy in direct:
            copy.wait_recv()
            slot = coefb.at[t, lax.rem(s - 2 * q + n_s, n_s)]
            near.append(send(slot, slot, coef_sem.at[t, nz - 1 + q], "sample", pair))

    cur[...] = coefs_ref[...]
    coefb[0, s] = coefs_ref[...].astype(jnp.bfloat16)
    pl.semaphore_wait(barrier, n_c - 1 + n_s - 1)
    coef_near, coef_direct = send_coefs(0)
    pick(0)
    moves = [send_feats(0)]
    pick(1)
    moves.append(send_feats(1))

    load.wait()

    def square(j, _):
        cols = pl.ds(pl.multiple_of(j * tile, tile), tile)
        block = cen[:, cols].astype(jnp.float32)
        csq[:, cols] = jnp.sum(block * block, axis=0, keepdims=True)
        return 0

    lax.fori_loop(0, cen_dev // tile, square, 0)

    bend = (1.0 / (LENGTH_SCALE * math.log(2.0))) ** 2

    def laplace(t):
        parts = [feats[t, k] for k in range(n_c)]
        ssq = sum(
            jnp.sum(jnp.square(p.astype(jnp.float32)), axis=1, keepdims=True) for p in parts
        ) * 0.25
        if fd % 128 == 0:
            parts = [jnp.concatenate(parts, axis=1)]
        deep = width // len(parts)

        def body(j, _):
            cols = pl.ds(pl.multiple_of(j * tile, tile), tile)
            cross = sum(
                jnp.dot(p, cen[k * deep:(k + 1) * deep, cols], preferred_element_type=jnp.float32)
                for k, p in enumerate(parts)
            )
            arg = ((ssq + csq[:, cols]) + cross) * (bend / width) + bend * EPS
            arg = jnp.maximum(arg, 1e-30)
            value = jnp.exp2(-(arg * lax.rsqrt(arg)))
            for k in range(pieces):
                kern[t, j * pieces + k] = value[:, k * own:(k + 1) * own].astype(jnp.bfloat16)
            return 0

        lax.fori_loop(0, cen_dev // tile, body, 0)

    def residual(t):
        part = sum(
            lax.dot_general(coefb[t, j], kern[t, j], NT, preferred_element_type=jnp.float32)
            for j in range(n_s)
        )
        for k in range(n_c):
            lsend[t, k] = part[:, k * share:(k + 1) * share].astype(LOGIT_WIRE)
        copies = [
            send(lsend.at[t, peer], lrecv.at[t, r], log_sem.at[t, r], "centre", peer)
            for r, peer in enumerate(c_peers)
        ]
        if t + 1 < steps:
            forward_feats(t + 1, *moves[t + 1])
        total = lsend[t, c].astype(jnp.float32)
        for r, copy in enumerate(copies):
            copy.wait_recv()
            total = total + lrecv[t, r].astype(jnp.float32)
        logits = total * logit_scale
        expo = jnp.exp(logits - jnp.max(logits, axis=0, keepdims=True))
        probs = expo / jnp.sum(expo, axis=0, keepdims=True)
        ids = lax.broadcasted_iota(jnp.int32, (classes, share), 0).astype(jnp.float32)
        hot = jnp.where(ids == labs[t, c][0:1, :], 1.0, 0.0)
        resid[t, c] = (probs - hot).astype(jnp.bfloat16)
        mine = resid.at[t, c]
        copies = [
            send(mine, mine, res_sem.at[t, r], "centre", peer) for r, peer in enumerate(c_peers)
        ]
        for copy in copies:
            copy.wait_recv()

    def gradient(t):
        if share % 128 == 0:
            whole = jnp.concatenate([resid[t, k] for k in range(n_c)], axis=1)

            def grad(j):
                return jnp.dot(whole, kern[t, j], preferred_element_type=jnp.float32)
        else:
            def grad(j):
                return sum(
                    jnp.dot(resid[t, k], kern[t, j, k * share:(k + 1) * share, :],
                            preferred_element_type=jnp.float32)
                    for k in range(n_c)
                )
        def put(i, value, peer):
            gsend[t, i] = value.astype(GRAD_WIRE)
            return send(gsend.at[t, i], grecv.at[t, i], grad_sem.at[t, i], "sample", peer)

        far = [lax.rem(start + 2 * q, n_s) for q in order for start in (s, pair)]
        copies = [put(i, grad(peer), peer) for i, peer in enumerate(far)]
        psend[t] = grad(pair)
        last = send(psend.at[t], precv.at[t], grad_sem.at[t, n_s - 2], "sample", pair)
        return grad(s), last, copies

    forward_coefs(0, coef_near, coef_direct[:2])
    forward_feats(0, *moves[0])
    forward_coefs(0, coef_near, coef_direct[2:])
    laplace(0)
    for t in range(steps):
        for copy in coef_near:
            copy.wait_recv()
        residual(t)
        total, last, copies = gradient(t)
        if t + 1 < steps:
            laplace(t + 1)
        last.wait_recv()
        total = total + precv[t]
        for r, copy in enumerate(copies):
            copy.wait_recv()
            total = total + grecv[t, r].astype(jnp.float32)
        fresh = cur[...] - rate * total
        if t + 1 < steps:
            cur[...] = fresh
            coefb[t + 1, s] = fresh.astype(jnp.bfloat16)
            coef_near, coef_direct = send_coefs(t + 1)
            forward_coefs(t + 1, coef_near, coef_direct)
        else:
            out_ref[...] = fresh
    for copy in started:
        copy.wait_send()


CHUNKS = 2
PIECES = 3
LOG_STEPS = 520.0
LOG_LOW = 50.0
LEVELS = 64.0
FIXED = 32000.0


def encode(value):
    size = jnp.maximum(jnp.abs(value), 2.0 ** -LOG_LOW)
    code = jnp.round((jnp.log(size) * (1.0 / math.log(2.0)) + LOG_LOW) * LOG_STEPS)
    return jnp.where(value < 0.0, -code, code).astype(jnp.int16)


def decode(code):
    number = code.astype(jnp.float32)
    size = jnp.exp2(jnp.abs(number) * (1.0 / LOG_STEPS) - LOG_LOW)
    return jnp.where(number < 0.0, -size, jnp.where(number > 0.0, size, 0.0))


def line_kernel(
    logit_scale, rate,
    cen_hbm, pool_hbm, labels_hbm, picks_hbm, coefs_hbm, out_ref,
    cen, pool_ref, labels_ref, picks_ref, cur,
    csq, feats, kern, labs, coefb, lacc, lpart, lrecv, lsum, ysend, ysum, resid, gown,
    near_out, near_in, cross_out, cross_in,
    load_sem, send_sem, feat_sem, log_sem, near_sem, cross_sem, mine_sem, over_sem, pass_sem,
):
    steps, batch = picks_ref.shape
    fd, pool_dev = pool_ref.shape
    classes, own = cur.shape
    width, cen_dev = cen.shape
    rows_n = batch // CHUNKS
    half = rows_n // 2
    piece = classes // PIECES
    tile = 2 * own
    tiles = cen_dev // tile

    c = lax.axis_index("centre")
    s = lax.axis_index("sample")
    y, k = lax.div(c, 2), lax.rem(c, 2)
    z, x = lax.div(s, 2), lax.rem(s, 2)
    z_near = z + 1 - 2 * lax.rem(z, 2)
    z_over = lax.rem(z + 2, 4)
    z_both = lax.rem(z_near + 2, 4)
    far_c = (1 - y) * 2 + k
    sib = {"centre": c + 1 - 2 * k}
    far = {"centre": far_c}
    over = {"sample": z_over * 2 + x}
    quad = [z * 2 + 1 - x, z_near * 2 + x, z_near * 2 + 1 - x]
    across = [z_over * 2 + 1 - x, z_both * 2 + x, z_both * 2 + 1 - x]
    near = [{"sample": q} for q in quad]

    barrier = pltpu.get_barrier_semaphore()
    for peer in [sib, far, over] + near:
        pl.semaphore_signal(barrier, inc=1, device_id=peer, device_id_type=MESH)

    loads = [
        pltpu.make_async_copy(src, dst, load_sem.at[i])
        for i, (src, dst) in enumerate(
            [(picks_hbm, picks_ref), (pool_hbm, pool_ref), (labels_hbm, labels_ref), (coefs_hbm, cur), (cen_hbm, cen)]
        )
    ]
    for i in (3, 0, 1, 2, 4):
        loads[i].start()

    def make(kind, t, src, dst, recv, peer):
        return pltpu.make_async_remote_copy(
            src_ref=src, dst_ref=dst, send_sem=send_sem.at[kind, t], recv_sem=recv,
            device_id=peer, device_id_type=MESH,
        )

    def rows_of(i):
        return slice(i * rows_n, (i + 1) * rows_n)

    def piece_of(h):
        return slice(h * piece, (h + 1) * piece)

    def feat_copy(t, i, owner, n, peer):
        slot = feats.at[t, owner, rows_of(i)]
        return make(0, t, slot, slot, feat_sem.at[t, n, i], peer)

    def feat_far(t, i):
        return feat_copy(t, i, c, 0, far)

    def feat_sib(t, i):
        return feat_copy(t, i, c, 1, sib)

    def feat_fwd(t, i):
        return feat_copy(t, i, far_c, 2, sib)

    def log_sib(t, i):
        return make(1, t, lpart.at[t, i, 1 - k], lrecv.at[t, i], log_sem.at[0, t, i], sib)

    def log_far(t, i):
        return make(6, t, ysend.at[t, i], ysum.at[t, i], log_sem.at[1, t, i], far)

    def res_sib(t, i):
        return make(2, t, resid.at[t, i, k], resid.at[t, i, k], log_sem.at[2, t, i], sib)

    def sum_near(t, n, q, h):
        rows = piece_of(h)
        return make(3, t, near_out.at[t, n, q, rows], near_in.at[t, n, q, rows], near_sem.at[n, q, h], near[q])

    def sum_over(t, h):
        rows = piece_of(h)
        return make(4, t, cross_out.at[t, rows], cross_in.at[t, rows], cross_sem.at[h], over)

    def coef_mine(t, q, h=None):
        slot = coefb.at[t, s] if h is None else coefb.at[t, s, piece_of(h)]
        return make(5, t, slot, slot, mine_sem.at[q], near[q])

    def coef_over(t, h):
        slot = coefb.at[t, s, piece_of(h)]
        return make(5, t, slot, slot, over_sem.at[h], over)

    def coef_pass(t, q, h):
        slot = coefb.at[t, z_over * 2 + x, piece_of(h)]
        return make(5, t, slot, slot, pass_sem.at[q, h], near[q])

    def pick(t, i):
        chosen = picks_ref[t:t + 1, rows_of(i)] - s * pool_dev
        rows = lax.broadcasted_iota(jnp.int32, (pool_dev, rows_n), 0)
        hot = jnp.where(rows == chosen, -2.0, 0.0).astype(jnp.bfloat16)
        got = jnp.dot(pool_ref[...], hot, preferred_element_type=jnp.float32)
        feats[t, c, rows_of(i)] = got.T.astype(jnp.bfloat16)
        return hot

    def pick_labels(t, i, hot):
        label_rows = jnp.broadcast_to(labels_ref[...].astype(jnp.float32), (16, pool_dev)).astype(jnp.bfloat16)
        lab = -0.5 * jnp.dot(label_rows, hot, preferred_element_type=jnp.float32)
        for h in range(2):
            labs[t, 2 * i + h] = lab[0:8, h * half:(h + 1) * half]

    bend = (1.0 / (LENGTH_SCALE * math.log(2.0))) ** 2

    def laplace(t, i, first, last):
        rows = rows_of(i)
        ssq = sum(
            jnp.sum(jnp.square(feats[t, q, rows].astype(jnp.float32)), axis=1, keepdims=True) for q in range(4)
        ) * 0.25

        def body(j, _):
            cols = pl.ds(pl.multiple_of(j * tile, tile), tile)
            lhs = jnp.concatenate([feats[t, q, rows] for q in range(4)], axis=1)
            cross = jnp.dot(lhs, cen[:, cols], preferred_element_type=jnp.float32)
            arg = ((ssq + csq[:, cols]) + cross) * (bend / width) + bend * EPS
            arg = jnp.maximum(arg, 1e-30)
            value = jnp.exp2(-(arg * lax.rsqrt(arg)))
            for q in range(2):
                kern[t, j * 2 + q, rows] = value[:, q * own:(q + 1) * own].astype(jnp.bfloat16)
            return 0

        lax.fori_loop(first, last, body, 0)

    def logits(t, i, group, first, last):
        part = sum(
            lax.dot_general(coefb[t, j], kern[t, j, rows_of(i)], NT, preferred_element_type=jnp.float32)
            for j in group
        )
        if not first:
            part = part + lacc[i]
        if not last:
            lacc[i] = part
            return
        for h in range(2):
            lpart[t, i, h] = part[:, h * half:(h + 1) * half]
        log_sib(t, i).start()

    def chip_sum(t, i):
        log_sib(t, i).wait_recv()
        value = lpart[t, i, k] + lrecv[t, i]
        lsum[t, i] = value
        top = jnp.maximum(jnp.max(jnp.abs(value), axis=0, keepdims=True), 2.0 ** -100)
        level = jnp.ceil(jnp.log(top) * (LEVELS / math.log(2.0)))
        code = jnp.round(value * (FIXED * jnp.exp2(level * (-1.0 / LEVELS))))
        ysend[t, i, 0:classes] = code.astype(jnp.int16)
        ysend[t, i, classes:] = jnp.broadcast_to(level, (16, half)).astype(jnp.int16)
        log_far(t, i).start()

    def residual(t, i):
        log_far(t, i).wait_recv()
        level = ysum[t, i, classes:].astype(jnp.float32)[0:1]
        other = ysum[t, i, 0:classes].astype(jnp.float32) * (jnp.exp2(level * (1.0 / LEVELS)) * (1.0 / FIXED))
        value = (lsum[t, i] + other) * logit_scale
        expo = jnp.exp(value - jnp.max(value, axis=0, keepdims=True))
        probs = expo / jnp.sum(expo, axis=0, keepdims=True)
        ids = lax.broadcasted_iota(jnp.int32, (classes, half), 0).astype(jnp.float32)
        hot = jnp.where(ids == labs[t, 2 * i + k][0:1, :], 1.0, 0.0)
        resid[t, i, k] = (probs - hot).astype(jnp.bfloat16)
        res_sib(t, i).start()

    def gradient(t):
        for i in range(CHUNKS):
            res_sib(t, i).wait_recv()
        whole = jnp.concatenate([resid[t, i, h] for i in range(CHUNKS) for h in range(2)], axis=1)

        def grad(block):
            return jnp.dot(whole, kern[t, block], preferred_element_type=jnp.float32)

        parts = [grad(block) for block in across]
        for h in range(PIECES):
            for q in (2, 1, 0):
                near_out[t, 0, q, piece_of(h)] = encode(parts[q][piece_of(h)])
                sum_near(t, 0, q, h).start()
        parts = [grad(block) for block in quad]
        for h in range(PIECES):
            for q in (2, 1, 0):
                near_out[t, 1, q, piece_of(h)] = encode(parts[q][piece_of(h)])
                sum_near(t, 1, q, h).start()
        gown[0] = grad(z_over * 2 + x)
        gown[1] = grad(s)

    def reduce_near(t, n, h):
        total = gown[n, piece_of(h)]
        for q in range(3):
            sum_near(t, n, q, h).wait_recv()
            total = total + decode(near_in[t, n, q, piece_of(h)])
        return total

    def reduce_across(t, h):
        cross_out[t, piece_of(h)] = encode(reduce_near(t, 0, h))
        sum_over(t, h).start()

    def reduce_end(t, h):
        total = reduce_near(t, 1, h)
        sum_over(t, h).wait_recv()
        return total + decode(cross_in[t, piece_of(h)])

    def share_mine(t):
        for h in range(PIECES):
            coef_over(t, h).start()
        for q in range(3):
            coef_mine(t, q).start()

    def share_pass(t, h):
        coef_over(t, h).wait_recv()
        for q in (2, 1, 0):
            coef_pass(t, q, h).start()

    def share_near(t):
        for q in range(3):
            coef_mine(t, q).wait_recv()

    def share_end(t):
        for q in range(3):
            for h in range(PIECES):
                coef_pass(t, q, h).wait_recv()

    first_group = [s] + quad + [z_over * 2 + x]

    pl.semaphore_wait(barrier, 6)
    loads[3].wait()
    coefb[0, s] = cur[...].astype(jnp.bfloat16)
    share_mine(0)
    loads[0].wait()
    loads[1].wait()
    hots = []
    for i in range(CHUNKS):
        hots.append(pick(0, i))
        feat_far(0, i).start()
        feat_sib(0, i).start()
    loads[2].wait()
    for i in range(CHUNKS):
        pick_labels(0, i, hots[i])
    for i in range(CHUNKS):
        pick_labels(1, i, pick(1, i))
    loads[4].wait()

    def square(j, _):
        cols = pl.ds(pl.multiple_of(j * own, own), own)
        block = cen[:, cols].astype(jnp.float32)
        csq[:, cols] = jnp.sum(block * block, axis=0, keepdims=True)
        return 0

    lax.fori_loop(0, cen_dev // own, square, 0)

    for h in range(PIECES):
        share_pass(0, h)
    feat_far(0, 0).wait_recv()
    feat_fwd(0, 0).start()
    feat_sib(0, 0).wait_recv()
    feat_fwd(0, 0).wait_recv()
    laplace(0, 0, 0, tiles)
    feat_far(0, 1).wait_recv()
    feat_fwd(0, 1).start()
    feat_sib(0, 1).wait_recv()
    feat_fwd(0, 1).wait_recv()
    laplace(0, 1, 0, tiles // 2)
    share_near(0)
    share_end(0)
    logits(0, 0, first_group + across, True, True)
    laplace(0, 1, tiles // 2, tiles)
    chip_sum(0, 0)
    logits(0, 1, first_group + across, True, True)
    chip_sum(0, 1)
    for i in range(CHUNKS):
        feat_far(1, i).start()
        feat_sib(1, i).start()
    residual(0, 0)
    residual(0, 1)

    gradient(0)
    feat_far(1, 0).wait_recv()
    feat_fwd(1, 0).start()
    feat_sib(1, 0).wait_recv()
    reduce_across(0, 0)
    feat_fwd(1, 0).wait_recv()
    reduce_across(0, 1)
    laplace(1, 0, 0, 1)
    reduce_across(0, 2)
    feat_far(1, 1).wait_recv()
    feat_fwd(1, 1).start()
    laplace(1, 0, 1, tiles)
    for h in range(PIECES):
        rows = piece_of(h)
        fresh = cur[rows] - rate * reduce_end(0, h)
        cur[rows] = fresh
        coefb[1, s, rows] = fresh.astype(jnp.bfloat16)
        coef_over(1, h).start()
        for q in (2, 1, 0):
            coef_mine(1, q, h).start()
    feat_sib(1, 1).wait_recv()
    feat_fwd(1, 1).wait_recv()
    laplace(1, 1, 0, tiles)
    for h in range(PIECES):
        share_pass(1, h)
    share_near(1)
    for i in range(CHUNKS):
        logits(1, i, first_group, True, False)
    share_end(1)
    for i in range(CHUNKS):
        logits(1, i, across, False, True)
    for i in range(CHUNKS):
        chip_sum(1, i)
    for i in range(CHUNKS):
        residual(1, i)
    gradient(1)
    for h in range(PIECES):
        reduce_across(1, h)
    for h in range(PIECES):
        out_ref[piece_of(h)] = cur[piece_of(h)] - rate * reduce_end(1, h)

    def drain(kind, t, ref):
        make(kind, t, ref, ref, cross_sem.at[0], over).wait_send()

    for t in range(steps):
        drain(0, t, feats.at[t, 0:3])
        drain(1, t, lpart.at[t, 0])
        drain(6, t, ysend.at[t])
        drain(2, t, resid.at[t, 0])
        drain(3, t, near_out.at[t])
        drain(4, t, cross_out.at[t])
        drain(5, t, coefb.at[t, 0:7])


def line_device(n_c, n_s, centres, pool, labels, picks, coefs):
    width, cen_dev = centres.shape
    fd, pool_dev = pool.shape
    steps, batch = picks.shape
    classes, own = coefs.shape
    half = batch // CHUNKS // 2
    bf16, f32, i16 = jnp.bfloat16, jnp.float32, jnp.int16
    dma = pltpu.SemaphoreType.DMA
    return pl.pallas_call(
        functools.partial(
            line_kernel, LOGIT_GAIN / (cen_dev * n_c), STEP_GAIN * LOGIT_GAIN / (batch * n_s)
        ),
        out_shape=pltpu.VMEM((classes, own), f32),
        in_specs=[pl.BlockSpec(memory_space=pltpu.HBM)] * 5,
        out_specs=pl.BlockSpec(memory_space=pltpu.VMEM),
        scratch_shapes=[
            pltpu.VMEM((width, cen_dev), bf16),
            pltpu.VMEM((fd, pool_dev), bf16),
            pltpu.VMEM((1, pool_dev), jnp.int32),
            pltpu.VMEM((steps, batch), jnp.int32),
            pltpu.VMEM((classes, own), f32),
            pltpu.VMEM((1, cen_dev), f32),
            pltpu.VMEM((steps, n_c, batch, fd), bf16),
            pltpu.VMEM((steps, n_s, batch, own), bf16),
            pltpu.VMEM((steps, 2 * CHUNKS, 8, half), f32),
            pltpu.VMEM((steps, n_s, classes, own), bf16),
            pltpu.VMEM((CHUNKS, classes, 2 * half), f32),
            pltpu.VMEM((steps, CHUNKS, 2, classes, half), f32),
            pltpu.VMEM((steps, CHUNKS, classes, half), f32),
            pltpu.VMEM((steps, CHUNKS, classes, half), f32),
            pltpu.VMEM((steps, CHUNKS, classes + 16, half), i16),
            pltpu.VMEM((steps, CHUNKS, classes + 16, half), i16),
            pltpu.VMEM((steps, CHUNKS, 2, classes, half), bf16),
            pltpu.VMEM((2, classes, own), f32),
            pltpu.VMEM((steps, 2, 3, classes, own), i16),
            pltpu.VMEM((steps, 2, 3, classes, own), i16),
            pltpu.VMEM((steps, classes, own), i16),
            pltpu.VMEM((steps, classes, own), i16),
            dma((5,)),
            dma((7, steps)),
            dma((steps, 3, CHUNKS)),
            dma((3, steps, CHUNKS)),
            dma((2, 3, PIECES)),
            dma((PIECES,)),
            dma((3,)),
            dma((PIECES,)),
            dma((3, PIECES)),
        ],
        compiler_params=pltpu.CompilerParams(
            collective_id=0, has_side_effects=True, vmem_limit_bytes=60 * 1024 * 1024
        ),
    )(centres, pool, labels.reshape(1, pool_dev), picks, coefs)


def suits_line(mesh, centres, pool, picks, coefs):
    n_c, n_s = mesh.shape["centre"], mesh.shape["sample"]
    own, batch, fd = coefs.shape[1], picks.shape[1], pool.shape[0]
    return (
        n_c == 4 and n_s == 8 and own % 128 == 0 and fd % 128 == 0 and picks.shape[0] == 2
        and batch % (256 * CHUNKS) == 0 and coefs.shape[0] % (16 * PIECES) == 0 and batch * n_s <= 4096
    )


def on_device(mesh, centres, pool, labels, picks, coefs):
    n_c, n_s = mesh.shape["centre"], mesh.shape["sample"]
    if suits_line(mesh, centres, pool, picks, coefs):
        return line_device(n_c, n_s, centres, pool, labels, picks, coefs)
    width, cen_dev = centres.shape
    fd, pool_dev = pool.shape
    steps, batch = picks.shape
    classes, own = coefs.shape
    share = batch // n_c
    bf16, f32 = jnp.bfloat16, jnp.float32
    body = functools.partial(
        kernel, n_c, n_s, LOGIT_GAIN / (cen_dev * n_c), STEP_GAIN * LOGIT_GAIN / (batch * n_s)
    )
    vmem = pl.BlockSpec(memory_space=pltpu.VMEM)
    return pl.pallas_call(
        body,
        out_shape=jax.ShapeDtypeStruct((classes, own), f32),
        in_specs=[pl.BlockSpec(memory_space=pl.ANY)] + [vmem] * 4,
        out_specs=vmem,
        scratch_shapes=[
            pltpu.VMEM((width, cen_dev), bf16),
            pltpu.VMEM((1, cen_dev), f32),
            pltpu.VMEM((steps, n_c, batch, fd), bf16),
            pltpu.VMEM((steps, n_s, batch, own), bf16),
            pltpu.VMEM((steps, n_c, 8, share), f32),
            pltpu.VMEM((steps, n_s, classes, own), bf16),
            pltpu.VMEM((steps, n_c, classes, share), LOGIT_WIRE),
            pltpu.VMEM((steps, n_c - 1, classes, share), LOGIT_WIRE),
            pltpu.VMEM((steps, n_c, classes, share), bf16),
            pltpu.VMEM((steps, n_s - 2, classes, own), GRAD_WIRE),
            pltpu.VMEM((steps, n_s - 2, classes, own), GRAD_WIRE),
            pltpu.VMEM((steps, classes, own), f32),
            pltpu.VMEM((steps, classes, own), f32),
            pltpu.VMEM((classes, own), f32),
            pltpu.SemaphoreType.DMA,
            pltpu.SemaphoreType.DMA((steps * (3 * (n_c - 1) + 2 * (n_s - 1)),)),
            pltpu.SemaphoreType.DMA((steps, n_c - 1)),
            pltpu.SemaphoreType.DMA((steps, n_c - 1)),
            pltpu.SemaphoreType.DMA((steps, n_c - 1)),
            pltpu.SemaphoreType.DMA((steps, n_s - 1)),
            pltpu.SemaphoreType.DMA((steps, n_s - 1)),
        ],
        compiler_params=pltpu.CompilerParams(
            collective_id=0, has_side_effects=True, vmem_limit_bytes=60 * 1024 * 1024
        ),
    )(centres, pool, labels.reshape(1, pool_dev), picks, coefs)


def solution(mesh):
    placed = (
        P(None, "centre"),
        P("centre", "sample"),
        P("sample"),
        P(None, "sample"),
        P(None, ("centre", "sample")),
    )
    return jax.shard_map(
        functools.partial(on_device, mesh),
        mesh=mesh,
        in_specs=placed,
        out_specs=P(None, ("centre", "sample")),
        check_vma=False,
    )
```

```python
import functools
import math

import jax
import jax.numpy as jnp
from jax import lax
from jax.experimental import pallas as pl
from jax.experimental.pallas import tpu as pltpu
from jax.sharding import PartitionSpec as P

LOGIT_GAIN = 16.0
LENGTH_SCALE = 0.5
STEP_GAIN = 2048.0
EPS = 1e-06

GRAD_WIRE = jnp.bfloat16
LOGIT_WIRE = jnp.float32
MESH = pl.DeviceIdType.MESH
NT = (((1,), (1,)), ((), ()))


def kernel(
    n_c, n_s, logit_scale, rate,
    cen_hbm, pool_ref, labels_ref, picks_ref, coefs_ref, out_ref,
    cen, csq, feats, kern, labs, coefb, lsend, lrecv, resid, gsend, grecv, psend, precv, cur,
    cen_sem, send_sem, feat_sem, log_sem, res_sem, coef_sem, grad_sem,
):
    steps, batch = picks_ref.shape
    fd, pool_dev = pool_ref.shape
    classes, own = coefs_ref.shape
    width, cen_dev = cen.shape
    share = batch // n_c
    ny = n_c // 2
    tile = max(own, min(256, cen_dev))
    pieces = tile // own

    c = lax.axis_index("centre")
    s = lax.axis_index("sample")
    sib = c + 1 - 2 * lax.rem(c, 2)
    c_peers = [lax.rem(c + r, n_c) for r in range(1, n_c)]
    s_peers = [lax.rem(s + r, n_s) for r in range(1, n_s)]
    pair = s + 1 - 2 * lax.rem(s, 2)
    nz = n_s // 2
    order = sorted(range(1, nz), key=lambda q: -min(q, nz - q))

    barrier = pltpu.get_barrier_semaphore()
    for peer in c_peers:
        pl.semaphore_signal(barrier, inc=1, device_id={"centre": peer}, device_id_type=MESH)
    for peer in s_peers:
        pl.semaphore_signal(barrier, inc=1, device_id={"sample": peer}, device_id_type=MESH)

    load = pltpu.make_async_copy(cen_hbm, cen, cen_sem)
    load.start()
    started = []

    def send(src, dst, recv, axis, peer):
        copy = pltpu.make_async_remote_copy(
            src_ref=src, dst_ref=dst, send_sem=send_sem.at[len(started)], recv_sem=recv,
            device_id={axis: peer}, device_id_type=MESH,
        )
        copy.start()
        started.append(copy)
        return copy

    label_rows = jnp.broadcast_to(labels_ref[...].astype(jnp.float32), (16, pool_dev)).astype(jnp.bfloat16)

    def pick(t):
        chosen = picks_ref[t:t + 1, :] - s * pool_dev
        rows = lax.broadcasted_iota(jnp.int32, (pool_dev, batch), 0)
        hot = jnp.where(rows == chosen, -2.0, 0.0).astype(jnp.bfloat16)
        got = jnp.dot(pool_ref[...], hot, preferred_element_type=jnp.float32)
        feats[t, c] = got.T.astype(jnp.bfloat16)
        lab = -0.5 * jnp.dot(label_rows, hot, preferred_element_type=jnp.float32)
        for k in range(n_c):
            labs[t, k] = lab[0:8, k * share:(k + 1) * share]

    def send_feats(t):
        mine = feats.at[t, c]
        direct = []
        for q in range(1, ny):
            direct.append(send(mine, mine, feat_sem.at[t, q], "centre", lax.rem(c + 2 * q, n_c)))
        return [send(mine, mine, feat_sem.at[t, 0], "centre", sib)], direct

    def forward_feats(t, near, direct):
        for q, copy in enumerate(direct, 1):
            copy.wait_recv()
            slot = feats.at[t, lax.rem(c - 2 * q + n_c, n_c)]
            near.append(send(slot, slot, feat_sem.at[t, ny - 1 + q], "centre", sib))
        for copy in near:
            copy.wait_recv()

    def send_coefs(t):
        mine = coefb.at[t, s]
        direct = [
            (q, send(mine, mine, coef_sem.at[t, q], "sample", lax.rem(s + 2 * q, n_s)))
            for q in order
        ]
        return [send(mine, mine, coef_sem.at[t, 0], "sample", pair)], direct

    def forward_coefs(t, near, direct):
        for q, copy in direct:
            copy.wait_recv()
            slot = coefb.at[t, lax.rem(s - 2 * q + n_s, n_s)]
            near.append(send(slot, slot, coef_sem.at[t, nz - 1 + q], "sample", pair))

    cur[...] = coefs_ref[...]
    coefb[0, s] = coefs_ref[...].astype(jnp.bfloat16)
    pl.semaphore_wait(barrier, n_c - 1 + n_s - 1)
    coef_near, coef_direct = send_coefs(0)
    pick(0)
    moves = [send_feats(0)]
    pick(1)
    moves.append(send_feats(1))

    load.wait()

    def square(j, _):
        cols = pl.ds(pl.multiple_of(j * tile, tile), tile)
        block = cen[:, cols].astype(jnp.float32)
        csq[:, cols] = jnp.sum(block * block, axis=0, keepdims=True)
        return 0

    lax.fori_loop(0, cen_dev // tile, square, 0)

    bend = (1.0 / (LENGTH_SCALE * math.log(2.0))) ** 2

    def laplace(t):
        parts = [feats[t, k] for k in range(n_c)]
        ssq = sum(
            jnp.sum(jnp.square(p.astype(jnp.float32)), axis=1, keepdims=True) for p in parts
        ) * 0.25
        if fd % 128 == 0:
            parts = [jnp.concatenate(parts, axis=1)]
        deep = width // len(parts)

        def body(j, _):
            cols = pl.ds(pl.multiple_of(j * tile, tile), tile)
            cross = sum(
                jnp.dot(p, cen[k * deep:(k + 1) * deep, cols], preferred_element_type=jnp.float32)
                for k, p in enumerate(parts)
            )
            arg = ((ssq + csq[:, cols]) + cross) * (bend / width) + bend * EPS
            arg = jnp.maximum(arg, 1e-30)
            value = jnp.exp2(-(arg * lax.rsqrt(arg)))
            for k in range(pieces):
                kern[t, j * pieces + k] = value[:, k * own:(k + 1) * own].astype(jnp.bfloat16)
            return 0

        lax.fori_loop(0, cen_dev // tile, body, 0)

    def residual(t):
        part = sum(
            lax.dot_general(coefb[t, j], kern[t, j], NT, preferred_element_type=jnp.float32)
            for j in range(n_s)
        )
        for k in range(n_c):
            lsend[t, k] = part[:, k * share:(k + 1) * share].astype(LOGIT_WIRE)
        copies = [
            send(lsend.at[t, peer], lrecv.at[t, r], log_sem.at[t, r], "centre", peer)
            for r, peer in enumerate(c_peers)
        ]
        if t + 1 < steps:
            forward_feats(t + 1, *moves[t + 1])
        total = lsend[t, c].astype(jnp.float32)
        for r, copy in enumerate(copies):
            copy.wait_recv()
            total = total + lrecv[t, r].astype(jnp.float32)
        logits = total * logit_scale
        expo = jnp.exp(logits - jnp.max(logits, axis=0, keepdims=True))
        probs = expo / jnp.sum(expo, axis=0, keepdims=True)
        ids = lax.broadcasted_iota(jnp.int32, (classes, share), 0).astype(jnp.float32)
        hot = jnp.where(ids == labs[t, c][0:1, :], 1.0, 0.0)
        resid[t, c] = (probs - hot).astype(jnp.bfloat16)
        mine = resid.at[t, c]
        copies = [
            send(mine, mine, res_sem.at[t, r], "centre", peer) for r, peer in enumerate(c_peers)
        ]
        for copy in copies:
            copy.wait_recv()

    def gradient(t):
        if share % 128 == 0:
            whole = jnp.concatenate([resid[t, k] for k in range(n_c)], axis=1)

            def grad(j):
                return jnp.dot(whole, kern[t, j], preferred_element_type=jnp.float32)
        else:
            def grad(j):
                return sum(
                    jnp.dot(resid[t, k], kern[t, j, k * share:(k + 1) * share, :],
                            preferred_element_type=jnp.float32)
                    for k in range(n_c)
                )
        def put(i, value, peer):
            gsend[t, i] = value.astype(GRAD_WIRE)
            return send(gsend.at[t, i], grecv.at[t, i], grad_sem.at[t, i], "sample", peer)

        far = [lax.rem(start + 2 * q, n_s) for q in order for start in (s, pair)]
        copies = [put(i, grad(peer), peer) for i, peer in enumerate(far)]
        psend[t] = grad(pair)
        last = send(psend.at[t], precv.at[t], grad_sem.at[t, n_s - 2], "sample", pair)
        return grad(s), last, copies

    forward_coefs(0, coef_near, coef_direct[:2])
    forward_feats(0, *moves[0])
    forward_coefs(0, coef_near, coef_direct[2:])
    laplace(0)
    for t in range(steps):
        for copy in coef_near:
            copy.wait_recv()
        residual(t)
        total, last, copies = gradient(t)
        if t + 1 < steps:
            laplace(t + 1)
        last.wait_recv()
        total = total + precv[t]
        for r, copy in enumerate(copies):
            copy.wait_recv()
            total = total + grecv[t, r].astype(jnp.float32)
        fresh = cur[...] - rate * total
        if t + 1 < steps:
            cur[...] = fresh
            coefb[t + 1, s] = fresh.astype(jnp.bfloat16)
            coef_near, coef_direct = send_coefs(t + 1)
            forward_coefs(t + 1, coef_near, coef_direct)
        else:
            out_ref[...] = fresh
    for copy in started:
        copy.wait_send()


CHUNKS = 2
PIECES = 3
LOG_STEPS = 520.0
LOG_LOW = 50.0
LEVELS = 64.0
FIXED = 32000.0


def encode(value):
    size = jnp.maximum(jnp.abs(value), 2.0 ** -LOG_LOW)
    code = jnp.round((jnp.log(size) * (1.0 / math.log(2.0)) + LOG_LOW) * LOG_STEPS)
    return jnp.where(value < 0.0, -code, code).astype(jnp.int16)


def decode(code):
    number = code.astype(jnp.float32)
    size = jnp.exp2(jnp.abs(number) * (1.0 / LOG_STEPS) - LOG_LOW)
    return jnp.where(number < 0.0, -size, jnp.where(number > 0.0, size, 0.0))


def line_kernel(
    logit_scale, rate,
    cen_hbm, pool_hbm, labels_hbm, picks_hbm, coefs_hbm, out_ref,
    cen, pool_ref, labels_ref, picks_ref, cur,
    csq, part, feats, kern, labs, coefb, lacc, lpart, lrecv, lsum, ysend, ysum, resid, gown,
    near_out, near_in, cross_out, cross_in,
    load_sem, send_sem, feat_sem, log_sem, near_sem, cross_sem, mine_sem, over_sem, pass_sem,
):
    steps, batch = picks_ref.shape
    fd, pool_dev = pool_ref.shape
    classes, own = cur.shape
    width, cen_dev = cen.shape
    rows_n = batch // CHUNKS
    half = rows_n // 2
    piece = classes // PIECES
    tile = 2 * own
    tiles = cen_dev // tile

    c = lax.axis_index("centre")
    s = lax.axis_index("sample")
    y, k = lax.div(c, 2), lax.rem(c, 2)
    z, x = lax.div(s, 2), lax.rem(s, 2)
    z_near = z + 1 - 2 * lax.rem(z, 2)
    z_over = lax.rem(z + 2, 4)
    z_both = lax.rem(z_near + 2, 4)
    far_c = (1 - y) * 2 + k
    sib = {"centre": c + 1 - 2 * k}
    far = {"centre": far_c}
    over = {"sample": z_over * 2 + x}
    quad = [z * 2 + 1 - x, z_near * 2 + x, z_near * 2 + 1 - x]
    across = [z_over * 2 + 1 - x, z_both * 2 + x, z_both * 2 + 1 - x]
    near = [{"sample": q} for q in quad]

    barrier = pltpu.get_barrier_semaphore()
    for peer in [sib, far, over] + near:
        pl.semaphore_signal(barrier, inc=1, device_id=peer, device_id_type=MESH)

    loads = [
        pltpu.make_async_copy(src, dst, load_sem.at[i])
        for i, (src, dst) in enumerate(
            [(picks_hbm, picks_ref), (pool_hbm, pool_ref), (labels_hbm, labels_ref), (coefs_hbm, cur), (cen_hbm, cen)]
        )
    ]
    for i in (0, 1, 3, 2, 4):
        loads[i].start()

    def make(kind, t, src, dst, recv, peer):
        return pltpu.make_async_remote_copy(
            src_ref=src, dst_ref=dst, send_sem=send_sem.at[kind, t], recv_sem=recv,
            device_id=peer, device_id_type=MESH,
        )

    def rows_of(i):
        return slice(i * rows_n, (i + 1) * rows_n)

    def piece_of(h):
        return slice(h * piece, (h + 1) * piece)

    def feat_copy(t, i, owner, n, peer):
        slot = feats.at[t, owner, rows_of(i)]
        return make(0, t, slot, slot, feat_sem.at[t, n, i], peer)

    def feat_far(t, i):
        return feat_copy(t, i, c, 0, far)

    def feat_sib(t, i):
        return feat_copy(t, i, c, 1, sib)

    def feat_fwd(t, i):
        return feat_copy(t, i, far_c, 2, sib)

    def log_sib(t, i):
        return make(1, t, lpart.at[t, i, 1 - k], lrecv.at[t, i], log_sem.at[0, t, i], sib)

    def log_far(t, i):
        return make(6, t, ysend.at[t, i], ysum.at[t, i], log_sem.at[1, t, i], far)

    def res_sib(t, i):
        return make(2, t, resid.at[t, i, k], resid.at[t, i, k], log_sem.at[2, t, i], sib)

    def sum_near(t, n, q, h):
        rows = piece_of(h)
        return make(3, t, near_out.at[t, n, q, rows], near_in.at[t, n, q, rows], near_sem.at[n, q, h], near[q])

    def sum_over(t, h):
        rows = piece_of(h)
        return make(4, t, cross_out.at[t, rows], cross_in.at[t, rows], cross_sem.at[h], over)

    def coef_mine(t, q, h=None):
        slot = coefb.at[t, s] if h is None else coefb.at[t, s, piece_of(h)]
        return make(5, t, slot, slot, mine_sem.at[q], near[q])

    def coef_over(t, h):
        slot = coefb.at[t, s, piece_of(h)]
        return make(5, t, slot, slot, over_sem.at[h], over)

    def coef_pass(t, q, h):
        slot = coefb.at[t, z_over * 2 + x, piece_of(h)]
        return make(5, t, slot, slot, pass_sem.at[q, h], near[q])

    def pick(t, i):
        chosen = picks_ref[t:t + 1, rows_of(i)] - s * pool_dev
        rows = lax.broadcasted_iota(jnp.int32, (pool_dev, rows_n), 0)
        hot = jnp.where(rows == chosen, -2.0, 0.0).astype(jnp.bfloat16)
        got = jnp.dot(pool_ref[...], hot, preferred_element_type=jnp.float32)
        feats[t, c, rows_of(i)] = got.T.astype(jnp.bfloat16)
        return hot

    def pick_labels(t, i, hot):
        label_rows = jnp.broadcast_to(labels_ref[...].astype(jnp.float32), (16, pool_dev)).astype(jnp.bfloat16)
        lab = -0.5 * jnp.dot(label_rows, hot, preferred_element_type=jnp.float32)
        for h in range(2):
            labs[t, 2 * i + h] = lab[0:8, h * half:(h + 1) * half]

    bend = (1.0 / (LENGTH_SCALE * math.log(2.0))) ** 2

    def laplace(t, i, first, last):
        rows = rows_of(i)
        ssq = sum(
            jnp.sum(jnp.square(feats[t, q, rows].astype(jnp.float32)), axis=1, keepdims=True) for q in range(4)
        ) * 0.25

        def body(j, _):
            cols = pl.ds(pl.multiple_of(j * tile, tile), tile)
            lhs = jnp.concatenate([feats[t, q, rows] for q in range(4)], axis=1)
            cross = jnp.dot(lhs, cen[:, cols], preferred_element_type=jnp.float32)
            arg = ((ssq + csq[:, cols]) + cross) * (bend / width) + bend * EPS
            arg = jnp.maximum(arg, 1e-30)
            value = jnp.exp2(-(arg * lax.rsqrt(arg)))
            for q in range(2):
                kern[t, j * 2 + q, rows] = value[:, q * own:(q + 1) * own].astype(jnp.bfloat16)
            return 0

        lax.fori_loop(first, last, body, 0, unroll=min(2, last - first))

    def near_part(i):
        rows = rows_of(i)
        slots = (2 * y, 2 * y + 1)
        ssq = sum(
            jnp.sum(jnp.square(feats[0, q, rows].astype(jnp.float32)), axis=1, keepdims=True) for q in slots
        ) * 0.25

        def body(j, _):
            cols = pl.ds(pl.multiple_of(j * tile, tile), tile)
            lhs = jnp.concatenate([feats[0, q, rows] for q in slots], axis=1)
            deep = pl.ds(pl.multiple_of(2 * y * fd, 2 * fd), 2 * fd)
            cross = jnp.dot(lhs, cen[deep, cols], preferred_element_type=jnp.float32)
            part[rows, cols] = (ssq + csq[:, cols]) + cross
            return 0

        lax.fori_loop(0, tiles, body, 0, unroll=2)

    def laplace_far(i, first, last):
        rows = rows_of(i)
        slots = (2 * (1 - y), 2 * (1 - y) + 1)
        ssq = sum(
            jnp.sum(jnp.square(feats[0, q, rows].astype(jnp.float32)), axis=1, keepdims=True) for q in slots
        ) * 0.25

        def body(j, _):
            cols = pl.ds(pl.multiple_of(j * tile, tile), tile)
            lhs = jnp.concatenate([feats[0, q, rows] for q in slots], axis=1)
            deep = pl.ds(pl.multiple_of(2 * (1 - y) * fd, 2 * fd), 2 * fd)
            cross = jnp.dot(lhs, cen[deep, cols], preferred_element_type=jnp.float32)
            arg = ((part[rows, cols] + ssq) + cross) * (bend / width) + bend * EPS
            arg = jnp.maximum(arg, 1e-30)
            value = jnp.exp2(-(arg * lax.rsqrt(arg)))
            for q in range(2):
                kern[0, j * 2 + q, rows] = value[:, q * own:(q + 1) * own].astype(jnp.bfloat16)
            return 0

        lax.fori_loop(first, last, body, 0, unroll=min(2, last - first))

    def logits(t, i, group, first, last):
        part = sum(
            lax.dot_general(coefb[t, j], kern[t, j, rows_of(i)], NT, preferred_element_type=jnp.float32)
            for j in group
        )
        if not first:
            part = part + lacc[i]
        if not last:
            lacc[i] = part
            return
        for h in range(2):
            lpart[t, i, h] = part[:, h * half:(h + 1) * half]
        log_sib(t, i).start()

    def chip_sum(t, i):
        log_sib(t, i).wait_recv()
        value = lpart[t, i, k] + lrecv[t, i]
        lsum[t, i] = value
        top = jnp.maximum(jnp.max(jnp.abs(value), axis=0, keepdims=True), 2.0 ** -100)
        level = jnp.ceil(jnp.log(top) * (LEVELS / math.log(2.0)))
        code = jnp.round(value * (FIXED * jnp.exp2(level * (-1.0 / LEVELS))))
        ysend[t, i, 0:classes] = code.astype(jnp.int16)
        ysend[t, i, classes:] = jnp.broadcast_to(level, (16, half)).astype(jnp.int16)
        log_far(t, i).start()

    def residual(t, i):
        log_far(t, i).wait_recv()
        level = ysum[t, i, classes:].astype(jnp.float32)[0:1]
        other = ysum[t, i, 0:classes].astype(jnp.float32) * (jnp.exp2(level * (1.0 / LEVELS)) * (1.0 / FIXED))
        value = (lsum[t, i] + other) * logit_scale
        expo = jnp.exp(value - jnp.max(value, axis=0, keepdims=True))
        probs = expo / jnp.sum(expo, axis=0, keepdims=True)
        ids = lax.broadcasted_iota(jnp.int32, (classes, half), 0).astype(jnp.float32)
        hot = jnp.where(ids == labs[t, 2 * i + k][0:1, :], 1.0, 0.0)
        resid[t, i, k] = (probs - hot).astype(jnp.bfloat16)
        res_sib(t, i).start()

    def gradient(t):
        for i in range(CHUNKS):
            res_sib(t, i).wait_recv()
        whole = jnp.concatenate([resid[t, i, h] for i in range(CHUNKS) for h in range(2)], axis=1)

        def grad(block):
            return jnp.dot(whole, kern[t, block], preferred_element_type=jnp.float32)

        parts = [grad(block) for block in across]
        for h in range(PIECES):
            for q in (2, 1, 0):
                near_out[t, 0, q, piece_of(h)] = encode(parts[q][piece_of(h)])
                sum_near(t, 0, q, h).start()
        parts = [grad(block) for block in quad]
        for h in range(PIECES):
            for q in (2, 1, 0):
                near_out[t, 1, q, piece_of(h)] = encode(parts[q][piece_of(h)])
                sum_near(t, 1, q, h).start()
        gown[0] = grad(z_over * 2 + x)
        gown[1] = grad(s)

    def reduce_near(t, n, h):
        total = gown[n, piece_of(h)]
        for q in range(3):
            sum_near(t, n, q, h).wait_recv()
            total = total + decode(near_in[t, n, q, piece_of(h)])
        return total

    def reduce_across(t, h):
        cross_out[t, piece_of(h)] = encode(reduce_near(t, 0, h))
        sum_over(t, h).start()

    def reduce_end(t, h):
        total = reduce_near(t, 1, h)
        sum_over(t, h).wait_recv()
        return total + decode(cross_in[t, piece_of(h)])

    def share_mine(t):
        for h in range(PIECES):
            coef_over(t, h).start()
        for q in range(3):
            coef_mine(t, q).start()

    def share_pass(t, h):
        coef_over(t, h).wait_recv()
        for q in (2, 1, 0):
            coef_pass(t, q, h).start()

    def share_near(t):
        for q in range(3):
            coef_mine(t, q).wait_recv()

    def share_end(t, q):
        for h in range(PIECES):
            coef_pass(t, q, h).wait_recv()

    first_group = [s] + quad + [z_over * 2 + x]

    pl.semaphore_wait(barrier, 6)
    loads[3].wait()
    coefb[0, s] = cur[...].astype(jnp.bfloat16)
    share_mine(0)
    loads[0].wait()
    loads[1].wait()
    hots = []
    for i in range(CHUNKS):
        hots.append(pick(0, i))
        feat_far(0, i).start()
        feat_sib(0, i).start()
    loads[2].wait()
    for i in range(CHUNKS):
        pick_labels(0, i, hots[i])
    for i in range(CHUNKS):
        pick_labels(1, i, pick(1, i))
    loads[4].wait()

    def square(j, _):
        cols = pl.ds(pl.multiple_of(j * own, own), own)
        block = cen[:, cols].astype(jnp.float32)
        csq[:, cols] = jnp.sum(block * block, axis=0, keepdims=True)
        return 0

    lax.fori_loop(0, cen_dev // own, square, 0)

    feat_sib(0, 0).wait_recv()
    near_part(0)
    share_pass(0, 0)
    feat_sib(0, 1).wait_recv()
    near_part(1)
    for h in range(1, PIECES):
        share_pass(0, h)
    feat_far(0, 0).wait_recv()
    feat_fwd(0, 0).start()
    feat_fwd(0, 0).wait_recv()
    laplace_far(0, 0, tiles // 2)
    feat_far(0, 1).wait_recv()
    feat_fwd(0, 1).start()
    laplace_far(0, tiles // 2, tiles)
    feat_fwd(0, 1).wait_recv()
    laplace_far(1, 0, tiles // 2)
    share_near(0)
    for q in range(3):
        share_end(0, q)
    logits(0, 0, first_group + across, True, True)
    laplace_far(1, tiles // 2, tiles)
    chip_sum(0, 0)
    logits(0, 1, first_group + across, True, True)
    chip_sum(0, 1)
    for i in range(CHUNKS):
        feat_far(1, i).start()
        feat_sib(1, i).start()
    residual(0, 0)
    residual(0, 1)

    gradient(0)
    feat_far(1, 0).wait_recv()
    feat_fwd(1, 0).start()
    feat_sib(1, 0).wait_recv()
    reduce_across(0, 0)
    feat_fwd(1, 0).wait_recv()
    reduce_across(0, 1)
    laplace(1, 0, 0, 1)
    reduce_across(0, 2)
    feat_far(1, 1).wait_recv()
    feat_fwd(1, 1).start()
    laplace(1, 0, 1, tiles)
    for h in range(PIECES):
        rows = piece_of(h)
        fresh = cur[rows] - rate * reduce_end(0, h)
        cur[rows] = fresh
        coefb[1, s, rows] = fresh.astype(jnp.bfloat16)
        coef_over(1, h).start()
        for q in (2, 1, 0):
            coef_mine(1, q, h).start()
    feat_sib(1, 1).wait_recv()
    feat_fwd(1, 1).wait_recv()
    laplace(1, 1, 0, tiles)
    for h in range(PIECES):
        share_pass(1, h)
    share_near(1)
    for i in range(CHUNKS):
        logits(1, i, first_group, True, False)
    for q in range(3):
        share_end(1, q)
        for i in range(CHUNKS):
            logits(1, i, across[q:q + 1], False, q == 2)
    for i in range(CHUNKS):
        chip_sum(1, i)
    for i in range(CHUNKS):
        residual(1, i)
    gradient(1)
    for h in range(PIECES):
        reduce_across(1, h)
    for h in range(PIECES):
        out_ref[piece_of(h)] = cur[piece_of(h)] - rate * reduce_end(1, h)

    def drain(kind, t, ref):
        make(kind, t, ref, ref, cross_sem.at[0], over).wait_send()

    for t in range(steps):
        drain(0, t, feats.at[t, 0:3])
        drain(1, t, lpart.at[t, 0])
        drain(6, t, ysend.at[t])
        drain(2, t, resid.at[t, 0])
        drain(3, t, near_out.at[t])
        drain(4, t, cross_out.at[t])
        drain(5, t, coefb.at[t, 0:7])


def line_device(n_c, n_s, centres, pool, labels, picks, coefs):
    width, cen_dev = centres.shape
    fd, pool_dev = pool.shape
    steps, batch = picks.shape
    classes, own = coefs.shape
    half = batch // CHUNKS // 2
    bf16, f32, i16 = jnp.bfloat16, jnp.float32, jnp.int16
    dma = pltpu.SemaphoreType.DMA
    return pl.pallas_call(
        functools.partial(
            line_kernel, LOGIT_GAIN / (cen_dev * n_c), STEP_GAIN * LOGIT_GAIN / (batch * n_s)
        ),
        out_shape=pltpu.VMEM((classes, own), f32),
        in_specs=[pl.BlockSpec(memory_space=pltpu.HBM)] * 5,
        out_specs=pl.BlockSpec(memory_space=pltpu.VMEM),
        scratch_shapes=[
            pltpu.VMEM((width, cen_dev), bf16),
            pltpu.VMEM((fd, pool_dev), bf16),
            pltpu.VMEM((1, pool_dev), jnp.int32),
            pltpu.VMEM((steps, batch), jnp.int32),
            pltpu.VMEM((classes, own), f32),
            pltpu.VMEM((1, cen_dev), f32),
            pltpu.VMEM((batch, cen_dev), f32),
            pltpu.VMEM((steps, n_c, batch, fd), bf16),
            pltpu.VMEM((steps, n_s, batch, own), bf16),
            pltpu.VMEM((steps, 2 * CHUNKS, 8, half), f32),
            pltpu.VMEM((steps, n_s, classes, own), bf16),
            pltpu.VMEM((CHUNKS, classes, 2 * half), f32),
            pltpu.VMEM((steps, CHUNKS, 2, classes, half), f32),
            pltpu.VMEM((steps, CHUNKS, classes, half), f32),
            pltpu.VMEM((steps, CHUNKS, classes, half), f32),
            pltpu.VMEM((steps, CHUNKS, classes + 16, half), i16),
            pltpu.VMEM((steps, CHUNKS, classes + 16, half), i16),
            pltpu.VMEM((steps, CHUNKS, 2, classes, half), bf16),
            pltpu.VMEM((2, classes, own), f32),
            pltpu.VMEM((steps, 2, 3, classes, own), i16),
            pltpu.VMEM((steps, 2, 3, classes, own), i16),
            pltpu.VMEM((steps, classes, own), i16),
            pltpu.VMEM((steps, classes, own), i16),
            dma((5,)),
            dma((7, steps)),
            dma((steps, 3, CHUNKS)),
            dma((3, steps, CHUNKS)),
            dma((2, 3, PIECES)),
            dma((PIECES,)),
            dma((3,)),
            dma((PIECES,)),
            dma((3, PIECES)),
        ],
        compiler_params=pltpu.CompilerParams(
            collective_id=0, has_side_effects=True, vmem_limit_bytes=60 * 1024 * 1024
        ),
    )(centres, pool, labels.reshape(1, pool_dev), picks, coefs)


def suits_line(mesh, centres, pool, picks, coefs):
    n_c, n_s = mesh.shape["centre"], mesh.shape["sample"]
    own, batch, fd = coefs.shape[1], picks.shape[1], pool.shape[0]
    return (
        n_c == 4 and n_s == 8 and own % 128 == 0 and fd % 128 == 0 and picks.shape[0] == 2
        and batch % (256 * CHUNKS) == 0 and coefs.shape[0] % (16 * PIECES) == 0 and batch * n_s <= 4096
    )


def on_device(mesh, centres, pool, labels, picks, coefs):
    n_c, n_s = mesh.shape["centre"], mesh.shape["sample"]
    if suits_line(mesh, centres, pool, picks, coefs):
        return line_device(n_c, n_s, centres, pool, labels, picks, coefs)
    width, cen_dev = centres.shape
    fd, pool_dev = pool.shape
    steps, batch = picks.shape
    classes, own = coefs.shape
    share = batch // n_c
    bf16, f32 = jnp.bfloat16, jnp.float32
    body = functools.partial(
        kernel, n_c, n_s, LOGIT_GAIN / (cen_dev * n_c), STEP_GAIN * LOGIT_GAIN / (batch * n_s)
    )
    vmem = pl.BlockSpec(memory_space=pltpu.VMEM)
    return pl.pallas_call(
        body,
        out_shape=jax.ShapeDtypeStruct((classes, own), f32),
        in_specs=[pl.BlockSpec(memory_space=pl.ANY)] + [vmem] * 4,
        out_specs=vmem,
        scratch_shapes=[
            pltpu.VMEM((width, cen_dev), bf16),
            pltpu.VMEM((1, cen_dev), f32),
            pltpu.VMEM((steps, n_c, batch, fd), bf16),
            pltpu.VMEM((steps, n_s, batch, own), bf16),
            pltpu.VMEM((steps, n_c, 8, share), f32),
            pltpu.VMEM((steps, n_s, classes, own), bf16),
            pltpu.VMEM((steps, n_c, classes, share), LOGIT_WIRE),
            pltpu.VMEM((steps, n_c - 1, classes, share), LOGIT_WIRE),
            pltpu.VMEM((steps, n_c, classes, share), bf16),
            pltpu.VMEM((steps, n_s - 2, classes, own), GRAD_WIRE),
            pltpu.VMEM((steps, n_s - 2, classes, own), GRAD_WIRE),
            pltpu.VMEM((steps, classes, own), f32),
            pltpu.VMEM((steps, classes, own), f32),
            pltpu.VMEM((classes, own), f32),
            pltpu.SemaphoreType.DMA,
            pltpu.SemaphoreType.DMA((steps * (3 * (n_c - 1) + 2 * (n_s - 1)),)),
            pltpu.SemaphoreType.DMA((steps, n_c - 1)),
            pltpu.SemaphoreType.DMA((steps, n_c - 1)),
            pltpu.SemaphoreType.DMA((steps, n_c - 1)),
            pltpu.SemaphoreType.DMA((steps, n_s - 1)),
            pltpu.SemaphoreType.DMA((steps, n_s - 1)),
        ],
        compiler_params=pltpu.CompilerParams(
            collective_id=0, has_side_effects=True, vmem_limit_bytes=60 * 1024 * 1024
        ),
    )(centres, pool, labels.reshape(1, pool_dev), picks, coefs)


def solution(mesh):
    placed = (
        P(None, "centre"),
        P("centre", "sample"),
        P("sample"),
        P(None, "sample"),
        P(None, ("centre", "sample")),
    )
    return jax.shard_map(
        functools.partial(on_device, mesh),
        mesh=mesh,
        in_specs=placed,
        out_specs=P(None, ("centre", "sample")),
        check_vma=False,
    )
```

```python
import functools
import math

import jax
import jax.numpy as jnp
from jax import lax
from jax.experimental import pallas as pl
from jax.experimental.pallas import tpu as pltpu
from jax.sharding import PartitionSpec as P

LOGIT_GAIN = 16.0
LENGTH_SCALE = 0.5
STEP_GAIN = 2048.0
EPS = 1e-06

GRAD_WIRE = jnp.bfloat16
LOGIT_WIRE = jnp.float32
MESH = pl.DeviceIdType.MESH
NT = (((1,), (1,)), ((), ()))


def kernel(
    n_c, n_s, logit_scale, rate,
    cen_hbm, pool_ref, labels_ref, picks_ref, coefs_ref, out_ref,
    cen, csq, feats, kern, labs, coefb, lsend, lrecv, resid, gsend, grecv, psend, precv, cur,
    cen_sem, send_sem, feat_sem, log_sem, res_sem, coef_sem, grad_sem,
):
    steps, batch = picks_ref.shape
    fd, pool_dev = pool_ref.shape
    classes, own = coefs_ref.shape
    width, cen_dev = cen.shape
    share = batch // n_c
    ny = n_c // 2
    tile = max(own, min(256, cen_dev))
    pieces = tile // own

    c = lax.axis_index("centre")
    s = lax.axis_index("sample")
    sib = c + 1 - 2 * lax.rem(c, 2)
    c_peers = [lax.rem(c + r, n_c) for r in range(1, n_c)]
    s_peers = [lax.rem(s + r, n_s) for r in range(1, n_s)]
    pair = s + 1 - 2 * lax.rem(s, 2)
    nz = n_s // 2
    order = sorted(range(1, nz), key=lambda q: -min(q, nz - q))

    barrier = pltpu.get_barrier_semaphore()
    for peer in c_peers:
        pl.semaphore_signal(barrier, inc=1, device_id={"centre": peer}, device_id_type=MESH)
    for peer in s_peers:
        pl.semaphore_signal(barrier, inc=1, device_id={"sample": peer}, device_id_type=MESH)

    load = pltpu.make_async_copy(cen_hbm, cen, cen_sem)
    load.start()
    started = []

    def send(src, dst, recv, axis, peer):
        copy = pltpu.make_async_remote_copy(
            src_ref=src, dst_ref=dst, send_sem=send_sem.at[len(started)], recv_sem=recv,
            device_id={axis: peer}, device_id_type=MESH,
        )
        copy.start()
        started.append(copy)
        return copy

    label_rows = jnp.broadcast_to(labels_ref[...].astype(jnp.float32), (16, pool_dev)).astype(jnp.bfloat16)

    def pick(t):
        chosen = picks_ref[t:t + 1, :] - s * pool_dev
        rows = lax.broadcasted_iota(jnp.int32, (pool_dev, batch), 0)
        hot = jnp.where(rows == chosen, -2.0, 0.0).astype(jnp.bfloat16)
        got = jnp.dot(pool_ref[...], hot, preferred_element_type=jnp.float32)
        feats[t, c] = got.T.astype(jnp.bfloat16)
        lab = -0.5 * jnp.dot(label_rows, hot, preferred_element_type=jnp.float32)
        for k in range(n_c):
            labs[t, k] = lab[0:8, k * share:(k + 1) * share]

    def send_feats(t):
        mine = feats.at[t, c]
        direct = []
        for q in range(1, ny):
            direct.append(send(mine, mine, feat_sem.at[t, q], "centre", lax.rem(c + 2 * q, n_c)))
        return [send(mine, mine, feat_sem.at[t, 0], "centre", sib)], direct

    def forward_feats(t, near, direct):
        for q, copy in enumerate(direct, 1):
            copy.wait_recv()
            slot = feats.at[t, lax.rem(c - 2 * q + n_c, n_c)]
            near.append(send(slot, slot, feat_sem.at[t, ny - 1 + q], "centre", sib))
        for copy in near:
            copy.wait_recv()

    def send_coefs(t):
        mine = coefb.at[t, s]
        direct = [
            (q, send(mine, mine, coef_sem.at[t, q], "sample", lax.rem(s + 2 * q, n_s)))
            for q in order
        ]
        return [send(mine, mine, coef_sem.at[t, 0], "sample", pair)], direct

    def forward_coefs(t, near, direct):
        for q, copy in direct:
            copy.wait_recv()
            slot = coefb.at[t, lax.rem(s - 2 * q + n_s, n_s)]
            near.append(send(slot, slot, coef_sem.at[t, nz - 1 + q], "sample", pair))

    cur[...] = coefs_ref[...]
    coefb[0, s] = coefs_ref[...].astype(jnp.bfloat16)
    pl.semaphore_wait(barrier, n_c - 1 + n_s - 1)
    coef_near, coef_direct = send_coefs(0)
    pick(0)
    moves = [send_feats(0)]
    pick(1)
    moves.append(send_feats(1))

    load.wait()

    def square(j, _):
        cols = pl.ds(pl.multiple_of(j * tile, tile), tile)
        block = cen[:, cols].astype(jnp.float32)
        csq[:, cols] = jnp.sum(block * block, axis=0, keepdims=True)
        return 0

    lax.fori_loop(0, cen_dev // tile, square, 0)

    bend = (1.0 / (LENGTH_SCALE * math.log(2.0))) ** 2

    def laplace(t):
        parts = [feats[t, k] for k in range(n_c)]
        ssq = sum(
            jnp.sum(jnp.square(p.astype(jnp.float32)), axis=1, keepdims=True) for p in parts
        ) * 0.25
        if fd % 128 == 0:
            parts = [jnp.concatenate(parts, axis=1)]
        deep = width // len(parts)

        def body(j, _):
            cols = pl.ds(pl.multiple_of(j * tile, tile), tile)
            cross = sum(
                jnp.dot(p, cen[k * deep:(k + 1) * deep, cols], preferred_element_type=jnp.float32)
                for k, p in enumerate(parts)
            )
            arg = ((ssq + csq[:, cols]) + cross) * (bend / width) + bend * EPS
            arg = jnp.maximum(arg, 1e-30)
            value = jnp.exp2(-(arg * lax.rsqrt(arg)))
            for k in range(pieces):
                kern[t, j * pieces + k] = value[:, k * own:(k + 1) * own].astype(jnp.bfloat16)
            return 0

        lax.fori_loop(0, cen_dev // tile, body, 0)

    def residual(t):
        part = sum(
            lax.dot_general(coefb[t, j], kern[t, j], NT, preferred_element_type=jnp.float32)
            for j in range(n_s)
        )
        for k in range(n_c):
            lsend[t, k] = part[:, k * share:(k + 1) * share].astype(LOGIT_WIRE)
        copies = [
            send(lsend.at[t, peer], lrecv.at[t, r], log_sem.at[t, r], "centre", peer)
            for r, peer in enumerate(c_peers)
        ]
        if t + 1 < steps:
            forward_feats(t + 1, *moves[t + 1])
        total = lsend[t, c].astype(jnp.float32)
        for r, copy in enumerate(copies):
            copy.wait_recv()
            total = total + lrecv[t, r].astype(jnp.float32)
        logits = total * logit_scale
        expo = jnp.exp(logits - jnp.max(logits, axis=0, keepdims=True))
        probs = expo / jnp.sum(expo, axis=0, keepdims=True)
        ids = lax.broadcasted_iota(jnp.int32, (classes, share), 0).astype(jnp.float32)
        hot = jnp.where(ids == labs[t, c][0:1, :], 1.0, 0.0)
        resid[t, c] = (probs - hot).astype(jnp.bfloat16)
        mine = resid.at[t, c]
        copies = [
            send(mine, mine, res_sem.at[t, r], "centre", peer) for r, peer in enumerate(c_peers)
        ]
        for copy in copies:
            copy.wait_recv()

    def gradient(t):
        if share % 128 == 0:
            whole = jnp.concatenate([resid[t, k] for k in range(n_c)], axis=1)

            def grad(j):
                return jnp.dot(whole, kern[t, j], preferred_element_type=jnp.float32)
        else:
            def grad(j):
                return sum(
                    jnp.dot(resid[t, k], kern[t, j, k * share:(k + 1) * share, :],
                            preferred_element_type=jnp.float32)
                    for k in range(n_c)
                )
        def put(i, value, peer):
            gsend[t, i] = value.astype(GRAD_WIRE)
            return send(gsend.at[t, i], grecv.at[t, i], grad_sem.at[t, i], "sample", peer)

        far = [lax.rem(start + 2 * q, n_s) for q in order for start in (s, pair)]
        copies = [put(i, grad(peer), peer) for i, peer in enumerate(far)]
        psend[t] = grad(pair)
        last = send(psend.at[t], precv.at[t], grad_sem.at[t, n_s - 2], "sample", pair)
        return grad(s), last, copies

    forward_coefs(0, coef_near, coef_direct[:2])
    forward_feats(0, *moves[0])
    forward_coefs(0, coef_near, coef_direct[2:])
    laplace(0)
    for t in range(steps):
        for copy in coef_near:
            copy.wait_recv()
        residual(t)
        total, last, copies = gradient(t)
        if t + 1 < steps:
            laplace(t + 1)
        last.wait_recv()
        total = total + precv[t]
        for r, copy in enumerate(copies):
            copy.wait_recv()
            total = total + grecv[t, r].astype(jnp.float32)
        fresh = cur[...] - rate * total
        if t + 1 < steps:
            cur[...] = fresh
            coefb[t + 1, s] = fresh.astype(jnp.bfloat16)
            coef_near, coef_direct = send_coefs(t + 1)
            forward_coefs(t + 1, coef_near, coef_direct)
        else:
            out_ref[...] = fresh
    for copy in started:
        copy.wait_send()


CHUNKS = 2
PIECES = 3
LOG_STEPS = 520.0
LOG_LOW = 50.0
LEVELS = 64.0
FIXED = 32000.0


def encode(value):
    size = jnp.maximum(jnp.abs(value), 2.0 ** -LOG_LOW)
    code = jnp.round((jnp.log(size) * (1.0 / math.log(2.0)) + LOG_LOW) * LOG_STEPS)
    return jnp.where(value < 0.0, -code, code).astype(jnp.int16)


def decode(code):
    number = code.astype(jnp.float32)
    size = jnp.exp2(jnp.abs(number) * (1.0 / LOG_STEPS) - LOG_LOW)
    return jnp.where(number < 0.0, -size, jnp.where(number > 0.0, size, 0.0))


def line_kernel(
    logit_scale, rate,
    cen_hbm, pool_hbm, labels_hbm, picks_hbm, coefs_hbm, out_ref,
    cen, pool_ref, labels_ref, picks_ref, cur,
    csq, part, feats, kern, labs, coefb, lacc, lpart, lrecv, lsum, ysend, ysum, resid, gown,
    near_out, near_in, cross_out, cross_in,
    load_sem, send_sem, feat_sem, log_sem, near_sem, cross_sem, mine_sem, over_sem, pass_sem,
):
    steps, batch = picks_ref.shape
    fd, pool_dev = pool_ref.shape
    classes, own = cur.shape
    width, cen_dev = cen.shape
    rows_n = batch // CHUNKS
    half = rows_n // 2
    piece = classes // PIECES
    tile = 2 * own
    tiles = cen_dev // tile
    blocks = cen_dev // own

    c = lax.axis_index("centre")
    s = lax.axis_index("sample")
    y, k = lax.div(c, 2), lax.rem(c, 2)
    z, x = lax.div(s, 2), lax.rem(s, 2)
    z_near = z + 1 - 2 * lax.rem(z, 2)
    z_over = lax.rem(z + 2, 4)
    z_both = lax.rem(z_near + 2, 4)
    far_c = (1 - y) * 2 + k
    sib = {"centre": c + 1 - 2 * k}
    far = {"centre": far_c}
    over = {"sample": z_over * 2 + x}
    quad = [z * 2 + 1 - x, z_near * 2 + x, z_near * 2 + 1 - x]
    across = [z_over * 2 + 1 - x, z_both * 2 + x, z_both * 2 + 1 - x]
    near = [{"sample": q} for q in quad]

    barrier = pltpu.get_barrier_semaphore()
    for peer in [sib, far, over] + near:
        pl.semaphore_signal(barrier, inc=1, device_id=peer, device_id_type=MESH)

    loads = [
        pltpu.make_async_copy(src, dst, load_sem.at[i])
        for i, (src, dst) in enumerate(
            [(picks_hbm, picks_ref), (pool_hbm, pool_ref), (labels_hbm, labels_ref), (coefs_hbm, cur), (cen_hbm, cen)]
        )
    ]
    for i in (0, 1, 3, 2, 4):
        loads[i].start()

    def make(kind, t, src, dst, recv, peer):
        return pltpu.make_async_remote_copy(
            src_ref=src, dst_ref=dst, send_sem=send_sem.at[kind], recv_sem=recv,
            device_id=peer, device_id_type=MESH,
        )

    def rows_of(i):
        return slice(i * rows_n, (i + 1) * rows_n)

    def piece_of(h):
        return slice(h * piece, (h + 1) * piece)

    def feat_copy(t, i, owner, n, peer):
        slot = feats.at[t, owner, rows_of(i)]
        return make(0, t, slot, slot, feat_sem.at[t, n, i], peer)

    def feat_far(t, i):
        return feat_copy(t, i, c, 0, far)

    def feat_sib(t, i):
        return feat_copy(t, i, c, 1, sib)

    def feat_fwd(t, i):
        return feat_copy(t, i, far_c, 2, sib)

    def log_sib(t, i):
        return make(1, t, lpart.at[t, i, 1 - k], lrecv.at[t, i], log_sem.at[0, t, i], sib)

    def log_far(t, i):
        return make(6, t, ysend.at[t, i], ysum.at[t, i], log_sem.at[1, t, i], far)

    def res_sib(t, i):
        return make(2, t, resid.at[t, i, k], resid.at[t, i, k], log_sem.at[2, t, i], sib)

    def sum_near(t, n, q, h):
        rows = piece_of(h)
        return make(3, t, near_out.at[t, n, q, rows], near_in.at[t, n, q, rows], near_sem.at[n, q, h], near[q])

    def sum_over(t, h):
        rows = piece_of(h)
        return make(4, t, cross_out.at[t, rows], cross_in.at[t, rows], cross_sem.at[h], over)

    def coef_mine(t, q, h=None):
        slot = coefb.at[t, s] if h is None else coefb.at[t, s, piece_of(h)]
        return make(5, t, slot, slot, mine_sem.at[q], near[q])

    def coef_over(t, h):
        slot = coefb.at[t, s, piece_of(h)]
        return make(5, t, slot, slot, over_sem.at[h], over)

    def coef_pass(t, q, h):
        slot = coefb.at[t, z_over * 2 + x, piece_of(h)]
        return make(5, t, slot, slot, pass_sem.at[q, h], near[q])

    def pick(t, i):
        chosen = picks_ref[t:t + 1, rows_of(i)] - s * pool_dev
        rows = lax.broadcasted_iota(jnp.int32, (pool_dev, rows_n), 0)
        hot = jnp.where(rows == chosen, -2.0, 0.0).astype(jnp.bfloat16)
        got = jnp.dot(pool_ref[...], hot, preferred_element_type=jnp.float32)
        feats[t, c, rows_of(i)] = got.T.astype(jnp.bfloat16)
        return hot

    def pick_labels(t, i, hot):
        label_rows = jnp.broadcast_to(labels_ref[...].astype(jnp.float32), (16, pool_dev)).astype(jnp.bfloat16)
        lab = -0.5 * jnp.dot(label_rows, hot, preferred_element_type=jnp.float32)
        for h in range(2):
            labs[t, 2 * i + h] = lab[0:8, h * half:(h + 1) * half]

    bend = (1.0 / (LENGTH_SCALE * math.log(2.0))) ** 2

    def laplace(t, i, first, last):
        rows = rows_of(i)
        ssq = sum(
            jnp.sum(jnp.square(feats[t, q, rows].astype(jnp.float32)), axis=1, keepdims=True) for q in range(4)
        ) * 0.25

        def body(j, _):
            cols = pl.ds(pl.multiple_of(j * tile, tile), tile)
            lhs = jnp.concatenate([feats[t, q, rows] for q in range(4)], axis=1)
            cross = jnp.dot(lhs, cen[:, cols], preferred_element_type=jnp.float32)
            arg = ((ssq + csq[:, cols]) + cross) * (bend / width) + bend * EPS
            arg = jnp.maximum(arg, 1e-30)
            value = jnp.exp2(-(arg * lax.rsqrt(arg)))
            for q in range(2):
                kern[t, j * 2 + q, rows] = value[:, q * own:(q + 1) * own].astype(jnp.bfloat16)
            return 0

        lax.fori_loop(first, last, body, 0, unroll=min(2, last - first))

    def near_part(i):
        rows = rows_of(i)
        slots = (2 * y, 2 * y + 1)
        ssq = sum(
            jnp.sum(jnp.square(feats[0, q, rows].astype(jnp.float32)), axis=1, keepdims=True) for q in slots
        ) * 0.25

        def body(j, _):
            cols = pl.ds(pl.multiple_of(j * tile, tile), tile)
            lhs = jnp.concatenate([feats[0, q, rows] for q in slots], axis=1)
            deep = pl.ds(pl.multiple_of(2 * y * fd, 2 * fd), 2 * fd)
            cross = jnp.dot(lhs, cen[deep, cols], preferred_element_type=jnp.float32)
            part[rows, cols] = (ssq + csq[:, cols]) + cross
            return 0

        lax.fori_loop(0, tiles, body, 0, unroll=2)

    def laplace_far(i, first, last):
        rows = rows_of(i)
        slots = (2 * (1 - y), 2 * (1 - y) + 1)
        ssq = sum(
            jnp.sum(jnp.square(feats[0, q, rows].astype(jnp.float32)), axis=1, keepdims=True) for q in slots
        ) * 0.25

        def body(j, _):
            cols = pl.ds(pl.multiple_of(j * tile, tile), tile)
            lhs = jnp.concatenate([feats[0, q, rows] for q in slots], axis=1)
            deep = pl.ds(pl.multiple_of(2 * (1 - y) * fd, 2 * fd), 2 * fd)
            cross = jnp.dot(lhs, cen[deep, cols], preferred_element_type=jnp.float32)
            arg = ((part[rows, cols] + ssq) + cross) * (bend / width) + bend * EPS
            arg = jnp.maximum(arg, 1e-30)
            value = jnp.exp2(-(arg * lax.rsqrt(arg)))
            for q in range(2):
                kern[0, j * 2 + q, rows] = value[:, q * own:(q + 1) * own].astype(jnp.bfloat16)
            return 0

        lax.fori_loop(first, last, body, 0, unroll=min(2, last - first))

    def logits(t, i, group, first, last):
        total = sum(
            lax.dot_general(coefb[t, j], kern[t, j, rows_of(i)], NT, preferred_element_type=jnp.float32)
            for j in group
        )
        if not first:
            total = total + lacc[i]
        if not last:
            lacc[i] = total
            return
        for h in range(2):
            lpart[t, i, h] = total[:, h * half:(h + 1) * half]
        log_sib(t, i).start()

    def chip_sum(t, i):
        log_sib(t, i).wait_recv()
        value = lpart[t, i, k] + lrecv[t, i]
        lsum[t, i] = value
        top = jnp.maximum(jnp.max(jnp.abs(value), axis=0, keepdims=True), 2.0 ** -100)
        level = jnp.ceil(jnp.log(top) * (LEVELS / math.log(2.0)))
        code = jnp.round(value * (FIXED * jnp.exp2(level * (-1.0 / LEVELS))))
        ysend[t, i, 0:classes] = code.astype(jnp.int16)
        ysend[t, i, classes:] = jnp.broadcast_to(level, (16, half)).astype(jnp.int16)
        log_far(t, i).start()

    def residual(t, i):
        log_far(t, i).wait_recv()
        level = ysum[t, i, classes:].astype(jnp.float32)[0:1]
        other = ysum[t, i, 0:classes].astype(jnp.float32) * (jnp.exp2(level * (1.0 / LEVELS)) * (1.0 / FIXED))
        value = (lsum[t, i] + other) * logit_scale
        expo = jnp.exp(value - jnp.max(value, axis=0, keepdims=True))
        probs = expo / jnp.sum(expo, axis=0, keepdims=True)
        ids = lax.broadcasted_iota(jnp.int32, (classes, half), 0).astype(jnp.float32)
        hot = jnp.where(ids == labs[t, 2 * i + k][0:1, :], 1.0, 0.0)
        resid[t, i, k] = (probs - hot).astype(jnp.bfloat16)
        res_sib(t, i).start()

    def gradient(t):
        for i in range(CHUNKS):
            res_sib(t, i).wait_recv()
        whole = jnp.concatenate([resid[t, i, h] for i in range(CHUNKS) for h in range(2)], axis=1)

        def grad(block):
            return jnp.dot(whole, kern[t, block], preferred_element_type=jnp.float32)

        parts = [grad(block) for block in across]
        for h in range(PIECES):
            for q in (2, 1, 0):
                near_out[t, 0, q, piece_of(h)] = encode(parts[q][piece_of(h)])
                sum_near(t, 0, q, h).start()
        parts = [grad(block) for block in quad]
        for h in range(PIECES):
            for q in (2, 1, 0):
                near_out[t, 1, q, piece_of(h)] = encode(parts[q][piece_of(h)])
                sum_near(t, 1, q, h).start()
        gown[0] = grad(z_over * 2 + x)
        gown[1] = grad(s)

    def reduce_near(t, n, h):
        total = gown[n, piece_of(h)]
        for q in range(3):
            sum_near(t, n, q, h).wait_recv()
            total = total + decode(near_in[t, n, q, piece_of(h)])
        return total

    def reduce_across(t, h):
        cross_out[t, piece_of(h)] = encode(reduce_near(t, 0, h))
        sum_over(t, h).start()

    def reduce_end(t, h):
        total = reduce_near(t, 1, h)
        sum_over(t, h).wait_recv()
        return total + decode(cross_in[t, piece_of(h)])

    def share_mine(t):
        for h in range(PIECES):
            coef_over(t, h).start()
        for q in range(3):
            coef_mine(t, q).start()

    def share_pass(t, h):
        coef_over(t, h).wait_recv()
        for q in (2, 1, 0):
            coef_pass(t, q, h).start()

    def share_near(t):
        for q in range(3):
            coef_mine(t, q).wait_recv()

    def share_end(t, q):
        for h in range(PIECES):
            coef_pass(t, q, h).wait_recv()

    first_group = [s] + quad + [z_over * 2 + x]

    pl.semaphore_wait(barrier, 6)
    loads[3].wait()
    coefb[0, s] = cur[...].astype(jnp.bfloat16)
    share_mine(0)
    loads[0].wait()
    loads[1].wait()
    hots = []
    for i in range(CHUNKS):
        hots.append(pick(0, i))
        feat_far(0, i).start()
        feat_sib(0, i).start()
    loads[2].wait()
    for i in range(CHUNKS):
        pick_labels(0, i, hots[i])
    for i in range(CHUNKS):
        pick_labels(1, i, pick(1, i))
    loads[4].wait()

    def square(j, _):
        cols = pl.ds(pl.multiple_of(j * own, own), own)
        block = cen[:, cols].astype(jnp.float32)
        csq[:, cols] = jnp.sum(block * block, axis=0, keepdims=True)
        return 0

    lax.fori_loop(0, cen_dev // own, square, 0)

    feat_sib(0, 0).wait_recv()
    near_part(0)
    share_pass(0, 0)
    feat_sib(0, 1).wait_recv()
    near_part(1)
    for h in range(1, PIECES):
        share_pass(0, h)
    feat_far(0, 0).wait_recv()
    feat_fwd(0, 0).start()
    feat_fwd(0, 0).wait_recv()
    laplace_far(0, 0, tiles // 2)
    feat_far(0, 1).wait_recv()
    feat_fwd(0, 1).start()
    laplace_far(0, tiles // 2, tiles)
    feat_fwd(0, 1).wait_recv()
    laplace_far(1, 0, tiles)
    share_near(0)
    for q in range(3):
        share_end(0, q)
    for i in range(CHUNKS):
        logits(0, i, range(blocks), True, True)
    for i in range(CHUNKS):
        chip_sum(0, i)
    residual(0, 0)
    for i in range(CHUNKS):
        feat_far(1, i).start()
        feat_sib(1, i).start()
    residual(0, 1)

    gradient(0)
    feat_far(1, 0).wait_recv()
    feat_fwd(1, 0).start()
    feat_sib(1, 0).wait_recv()
    reduce_across(0, 0)
    feat_fwd(1, 0).wait_recv()
    reduce_across(0, 1)
    laplace(1, 0, 0, 1)
    reduce_across(0, 2)
    feat_far(1, 1).wait_recv()
    feat_fwd(1, 1).start()
    laplace(1, 0, 1, tiles)
    for h in range(PIECES):
        rows = piece_of(h)
        fresh = cur[rows] - rate * reduce_end(0, h)
        cur[rows] = fresh
        coefb[1, s, rows] = fresh.astype(jnp.bfloat16)
        coef_over(1, h).start()
        for q in (2, 1, 0):
            coef_mine(1, q, h).start()
    feat_sib(1, 1).wait_recv()
    feat_fwd(1, 1).wait_recv()
    laplace(1, 1, 0, tiles)
    for h in range(PIECES):
        share_pass(1, h)
    share_near(1)
    for i in range(CHUNKS):
        logits(1, i, first_group, True, False)
    for q in range(3):
        share_end(1, q)
        for i in range(CHUNKS):
            logits(1, i, across[q:q + 1], False, q == 2)
    for i in range(CHUNKS):
        chip_sum(1, i)
    for i in range(CHUNKS):
        residual(1, i)
    gradient(1)
    for h in range(PIECES):
        reduce_across(1, h)
    for h in range(PIECES):
        out_ref[piece_of(h)] = cur[piece_of(h)] - rate * reduce_end(1, h)

    def drain(kind, ref):
        make(kind, 0, ref, ref, cross_sem.at[0], over).wait_send()

    drain(0, feats.at[:, 0:3])
    drain(1, lpart.at[:, 0])
    drain(2, resid.at[:, 0])
    drain(3, near_out)
    drain(4, cross_out)
    drain(5, coefb.at[:, 0:7])
    drain(6, ysend)


def line_device(n_c, n_s, centres, pool, labels, picks, coefs):
    width, cen_dev = centres.shape
    fd, pool_dev = pool.shape
    steps, batch = picks.shape
    classes, own = coefs.shape
    half = batch // CHUNKS // 2
    bf16, f32, i16 = jnp.bfloat16, jnp.float32, jnp.int16
    dma = pltpu.SemaphoreType.DMA
    return pl.pallas_call(
        functools.partial(
            line_kernel, LOGIT_GAIN / (cen_dev * n_c), STEP_GAIN * LOGIT_GAIN / (batch * n_s)
        ),
        out_shape=pltpu.VMEM((classes, own), f32),
        in_specs=[pl.BlockSpec(memory_space=pltpu.HBM)] * 5,
        out_specs=pl.BlockSpec(memory_space=pltpu.VMEM),
        scratch_shapes=[
            pltpu.VMEM((width, cen_dev), bf16),
            pltpu.VMEM((fd, pool_dev), bf16),
            pltpu.VMEM((1, pool_dev), jnp.int32),
            pltpu.VMEM((steps, batch), jnp.int32),
            pltpu.VMEM((classes, own), f32),
            pltpu.VMEM((1, cen_dev), f32),
            pltpu.VMEM((batch, cen_dev), f32),
            pltpu.VMEM((steps, n_c, batch, fd), bf16),
            pltpu.VMEM((steps, n_s, batch, own), bf16),
            pltpu.VMEM((steps, 2 * CHUNKS, 8, half), f32),
            pltpu.VMEM((steps, n_s, classes, own), bf16),
            pltpu.VMEM((CHUNKS, classes, 2 * half), f32),
            pltpu.VMEM((steps, CHUNKS, 2, classes, half), f32),
            pltpu.VMEM((steps, CHUNKS, classes, half), f32),
            pltpu.VMEM((steps, CHUNKS, classes, half), f32),
            pltpu.VMEM((steps, CHUNKS, classes + 16, half), i16),
            pltpu.VMEM((steps, CHUNKS, classes + 16, half), i16),
            pltpu.VMEM((steps, CHUNKS, 2, classes, half), bf16),
            pltpu.VMEM((2, classes, own), f32),
            pltpu.VMEM((steps, 2, 3, classes, own), i16),
            pltpu.VMEM((steps, 2, 3, classes, own), i16),
            pltpu.VMEM((steps, classes, own), i16),
            pltpu.VMEM((steps, classes, own), i16),
            dma((5,)),
            dma((7,)),
            dma((steps, 3, CHUNKS)),
            dma((3, steps, CHUNKS)),
            dma((2, 3, PIECES)),
            dma((PIECES,)),
            dma((3,)),
            dma((PIECES,)),
            dma((3, PIECES)),
        ],
        compiler_params=pltpu.CompilerParams(
            collective_id=0, has_side_effects=True, vmem_limit_bytes=60 * 1024 * 1024
        ),
    )(centres, pool, labels.reshape(1, pool_dev), picks, coefs)


def suits_line(mesh, centres, pool, picks, coefs):
    n_c, n_s = mesh.shape["centre"], mesh.shape["sample"]
    own, batch, fd = coefs.shape[1], picks.shape[1], pool.shape[0]
    return (
        n_c == 4 and n_s == 8 and own % 128 == 0 and fd % 128 == 0 and picks.shape[0] == 2
        and batch % (256 * CHUNKS) == 0 and coefs.shape[0] % (16 * PIECES) == 0 and batch * n_s <= 4096
    )


def on_device(mesh, centres, pool, labels, picks, coefs):
    n_c, n_s = mesh.shape["centre"], mesh.shape["sample"]
    if suits_line(mesh, centres, pool, picks, coefs):
        return line_device(n_c, n_s, centres, pool, labels, picks, coefs)
    width, cen_dev = centres.shape
    fd, pool_dev = pool.shape
    steps, batch = picks.shape
    classes, own = coefs.shape
    share = batch // n_c
    bf16, f32 = jnp.bfloat16, jnp.float32
    body = functools.partial(
        kernel, n_c, n_s, LOGIT_GAIN / (cen_dev * n_c), STEP_GAIN * LOGIT_GAIN / (batch * n_s)
    )
    vmem = pl.BlockSpec(memory_space=pltpu.VMEM)
    return pl.pallas_call(
        body,
        out_shape=jax.ShapeDtypeStruct((classes, own), f32),
        in_specs=[pl.BlockSpec(memory_space=pl.ANY)] + [vmem] * 4,
        out_specs=vmem,
        scratch_shapes=[
            pltpu.VMEM((width, cen_dev), bf16),
            pltpu.VMEM((1, cen_dev), f32),
            pltpu.VMEM((steps, n_c, batch, fd), bf16),
            pltpu.VMEM((steps, n_s, batch, own), bf16),
            pltpu.VMEM((steps, n_c, 8, share), f32),
            pltpu.VMEM((steps, n_s, classes, own), bf16),
            pltpu.VMEM((steps, n_c, classes, share), LOGIT_WIRE),
            pltpu.VMEM((steps, n_c - 1, classes, share), LOGIT_WIRE),
            pltpu.VMEM((steps, n_c, classes, share), bf16),
            pltpu.VMEM((steps, n_s - 2, classes, own), GRAD_WIRE),
            pltpu.VMEM((steps, n_s - 2, classes, own), GRAD_WIRE),
            pltpu.VMEM((steps, classes, own), f32),
            pltpu.VMEM((steps, classes, own), f32),
            pltpu.VMEM((classes, own), f32),
            pltpu.SemaphoreType.DMA,
            pltpu.SemaphoreType.DMA((steps * (3 * (n_c - 1) + 2 * (n_s - 1)),)),
            pltpu.SemaphoreType.DMA((steps, n_c - 1)),
            pltpu.SemaphoreType.DMA((steps, n_c - 1)),
            pltpu.SemaphoreType.DMA((steps, n_c - 1)),
            pltpu.SemaphoreType.DMA((steps, n_s - 1)),
            pltpu.SemaphoreType.DMA((steps, n_s - 1)),
        ],
        compiler_params=pltpu.CompilerParams(
            collective_id=0, has_side_effects=True, vmem_limit_bytes=60 * 1024 * 1024
        ),
    )(centres, pool, labels.reshape(1, pool_dev), picks, coefs)


def solution(mesh):
    placed = (
        P(None, "centre"),
        P("centre", "sample"),
        P("sample"),
        P(None, "sample"),
        P(None, ("centre", "sample")),
    )
    return jax.shard_map(
        functools.partial(on_device, mesh),
        mesh=mesh,
        in_specs=placed,
        out_specs=P(None, ("centre", "sample")),
        check_vma=False,
    )
```

```python
import functools
import math

import jax
import jax.numpy as jnp
from jax import lax
from jax.experimental import pallas as pl
from jax.experimental.pallas import tpu as pltpu
from jax.sharding import PartitionSpec as P

LOGIT_GAIN = 16.0
LENGTH_SCALE = 0.5
STEP_GAIN = 2048.0
EPS = 1e-06

GRAD_WIRE = jnp.bfloat16
LOGIT_WIRE = jnp.float32
MESH = pl.DeviceIdType.MESH
NT = (((1,), (1,)), ((), ()))


def kernel(
    n_c, n_s, logit_scale, rate,
    cen_hbm, pool_ref, labels_ref, picks_ref, coefs_ref, out_ref,
    cen, csq, feats, kern, labs, coefb, lsend, lrecv, resid, gsend, grecv, psend, precv, cur,
    cen_sem, send_sem, feat_sem, log_sem, res_sem, coef_sem, grad_sem,
):
    steps, batch = picks_ref.shape
    fd, pool_dev = pool_ref.shape
    classes, own = coefs_ref.shape
    width, cen_dev = cen.shape
    share = batch // n_c
    ny = n_c // 2
    tile = max(own, min(256, cen_dev))
    pieces = tile // own

    c = lax.axis_index("centre")
    s = lax.axis_index("sample")
    sib = c + 1 - 2 * lax.rem(c, 2)
    c_peers = [lax.rem(c + r, n_c) for r in range(1, n_c)]
    s_peers = [lax.rem(s + r, n_s) for r in range(1, n_s)]
    pair = s + 1 - 2 * lax.rem(s, 2)
    nz = n_s // 2
    order = sorted(range(1, nz), key=lambda q: -min(q, nz - q))

    barrier = pltpu.get_barrier_semaphore()
    for peer in c_peers:
        pl.semaphore_signal(barrier, inc=1, device_id={"centre": peer}, device_id_type=MESH)
    for peer in s_peers:
        pl.semaphore_signal(barrier, inc=1, device_id={"sample": peer}, device_id_type=MESH)

    load = pltpu.make_async_copy(cen_hbm, cen, cen_sem)
    load.start()
    started = []

    def send(src, dst, recv, axis, peer):
        copy = pltpu.make_async_remote_copy(
            src_ref=src, dst_ref=dst, send_sem=send_sem.at[len(started)], recv_sem=recv,
            device_id={axis: peer}, device_id_type=MESH,
        )
        copy.start()
        started.append(copy)
        return copy

    label_rows = jnp.broadcast_to(labels_ref[...].astype(jnp.float32), (16, pool_dev)).astype(jnp.bfloat16)

    def pick(t):
        chosen = picks_ref[t:t + 1, :] - s * pool_dev
        rows = lax.broadcasted_iota(jnp.int32, (pool_dev, batch), 0)
        hot = jnp.where(rows == chosen, -2.0, 0.0).astype(jnp.bfloat16)
        got = jnp.dot(pool_ref[...], hot, preferred_element_type=jnp.float32)
        feats[t, c] = got.T.astype(jnp.bfloat16)
        lab = -0.5 * jnp.dot(label_rows, hot, preferred_element_type=jnp.float32)
        for k in range(n_c):
            labs[t, k] = lab[0:8, k * share:(k + 1) * share]

    def send_feats(t):
        mine = feats.at[t, c]
        direct = []
        for q in range(1, ny):
            direct.append(send(mine, mine, feat_sem.at[t, q], "centre", lax.rem(c + 2 * q, n_c)))
        return [send(mine, mine, feat_sem.at[t, 0], "centre", sib)], direct

    def forward_feats(t, near, direct):
        for q, copy in enumerate(direct, 1):
            copy.wait_recv()
            slot = feats.at[t, lax.rem(c - 2 * q + n_c, n_c)]
            near.append(send(slot, slot, feat_sem.at[t, ny - 1 + q], "centre", sib))
        for copy in near:
            copy.wait_recv()

    def send_coefs(t):
        mine = coefb.at[t, s]
        direct = [
            (q, send(mine, mine, coef_sem.at[t, q], "sample", lax.rem(s + 2 * q, n_s)))
            for q in order
        ]
        return [send(mine, mine, coef_sem.at[t, 0], "sample", pair)], direct

    def forward_coefs(t, near, direct):
        for q, copy in direct:
            copy.wait_recv()
            slot = coefb.at[t, lax.rem(s - 2 * q + n_s, n_s)]
            near.append(send(slot, slot, coef_sem.at[t, nz - 1 + q], "sample", pair))

    cur[...] = coefs_ref[...]
    coefb[0, s] = coefs_ref[...].astype(jnp.bfloat16)
    pl.semaphore_wait(barrier, n_c - 1 + n_s - 1)
    coef_near, coef_direct = send_coefs(0)
    pick(0)
    moves = [send_feats(0)]
    pick(1)
    moves.append(send_feats(1))

    load.wait()

    def square(j, _):
        cols = pl.ds(pl.multiple_of(j * tile, tile), tile)
        block = cen[:, cols].astype(jnp.float32)
        csq[:, cols] = jnp.sum(block * block, axis=0, keepdims=True)
        return 0

    lax.fori_loop(0, cen_dev // tile, square, 0)

    bend = (1.0 / (LENGTH_SCALE * math.log(2.0))) ** 2

    def laplace(t):
        parts = [feats[t, k] for k in range(n_c)]
        ssq = sum(
            jnp.sum(jnp.square(p.astype(jnp.float32)), axis=1, keepdims=True) for p in parts
        ) * 0.25
        if fd % 128 == 0:
            parts = [jnp.concatenate(parts, axis=1)]
        deep = width // len(parts)

        def body(j, _):
            cols = pl.ds(pl.multiple_of(j * tile, tile), tile)
            cross = sum(
                jnp.dot(p, cen[k * deep:(k + 1) * deep, cols], preferred_element_type=jnp.float32)
                for k, p in enumerate(parts)
            )
            arg = ((ssq + csq[:, cols]) + cross) * (bend / width) + bend * EPS
            arg = jnp.maximum(arg, 1e-30)
            value = jnp.exp2(-(arg * lax.rsqrt(arg)))
            for k in range(pieces):
                kern[t, j * pieces + k] = value[:, k * own:(k + 1) * own].astype(jnp.bfloat16)
            return 0

        lax.fori_loop(0, cen_dev // tile, body, 0)

    def residual(t):
        part = sum(
            lax.dot_general(coefb[t, j], kern[t, j], NT, preferred_element_type=jnp.float32)
            for j in range(n_s)
        )
        for k in range(n_c):
            lsend[t, k] = part[:, k * share:(k + 1) * share].astype(LOGIT_WIRE)
        copies = [
            send(lsend.at[t, peer], lrecv.at[t, r], log_sem.at[t, r], "centre", peer)
            for r, peer in enumerate(c_peers)
        ]
        if t + 1 < steps:
            forward_feats(t + 1, *moves[t + 1])
        total = lsend[t, c].astype(jnp.float32)
        for r, copy in enumerate(copies):
            copy.wait_recv()
            total = total + lrecv[t, r].astype(jnp.float32)
        logits = total * logit_scale
        expo = jnp.exp(logits - jnp.max(logits, axis=0, keepdims=True))
        probs = expo / jnp.sum(expo, axis=0, keepdims=True)
        ids = lax.broadcasted_iota(jnp.int32, (classes, share), 0).astype(jnp.float32)
        hot = jnp.where(ids == labs[t, c][0:1, :], 1.0, 0.0)
        resid[t, c] = (probs - hot).astype(jnp.bfloat16)
        mine = resid.at[t, c]
        copies = [
            send(mine, mine, res_sem.at[t, r], "centre", peer) for r, peer in enumerate(c_peers)
        ]
        for copy in copies:
            copy.wait_recv()

    def gradient(t):
        if share % 128 == 0:
            whole = jnp.concatenate([resid[t, k] for k in range(n_c)], axis=1)

            def grad(j):
                return jnp.dot(whole, kern[t, j], preferred_element_type=jnp.float32)
        else:
            def grad(j):
                return sum(
                    jnp.dot(resid[t, k], kern[t, j, k * share:(k + 1) * share, :],
                            preferred_element_type=jnp.float32)
                    for k in range(n_c)
                )
        def put(i, value, peer):
            gsend[t, i] = value.astype(GRAD_WIRE)
            return send(gsend.at[t, i], grecv.at[t, i], grad_sem.at[t, i], "sample", peer)

        far = [lax.rem(start + 2 * q, n_s) for q in order for start in (s, pair)]
        copies = [put(i, grad(peer), peer) for i, peer in enumerate(far)]
        psend[t] = grad(pair)
        last = send(psend.at[t], precv.at[t], grad_sem.at[t, n_s - 2], "sample", pair)
        return grad(s), last, copies

    forward_coefs(0, coef_near, coef_direct[:2])
    forward_feats(0, *moves[0])
    forward_coefs(0, coef_near, coef_direct[2:])
    laplace(0)
    for t in range(steps):
        for copy in coef_near:
            copy.wait_recv()
        residual(t)
        total, last, copies = gradient(t)
        if t + 1 < steps:
            laplace(t + 1)
        last.wait_recv()
        total = total + precv[t]
        for r, copy in enumerate(copies):
            copy.wait_recv()
            total = total + grecv[t, r].astype(jnp.float32)
        fresh = cur[...] - rate * total
        if t + 1 < steps:
            cur[...] = fresh
            coefb[t + 1, s] = fresh.astype(jnp.bfloat16)
            coef_near, coef_direct = send_coefs(t + 1)
            forward_coefs(t + 1, coef_near, coef_direct)
        else:
            out_ref[...] = fresh
    for copy in started:
        copy.wait_send()


CHUNKS = 2
PIECES = 3
LOG_STEPS = 520.0
LOG_LOW = 50.0
LEVELS = 64.0
FIXED = 32000.0


def encode(value):
    size = jnp.maximum(jnp.abs(value), 2.0 ** -LOG_LOW)
    code = jnp.round((jnp.log(size) * (1.0 / math.log(2.0)) + LOG_LOW) * LOG_STEPS)
    return jnp.where(value < 0.0, -code, code).astype(jnp.int16)


def decode(code):
    number = code.astype(jnp.float32)
    size = jnp.exp2(jnp.abs(number) * (1.0 / LOG_STEPS) - LOG_LOW)
    return jnp.where(number < 0.0, -size, jnp.where(number > 0.0, size, 0.0))


def line_kernel(
    logit_scale, rate,
    cen_hbm, pool_hbm, labels_hbm, picks_hbm, coefs_hbm, out_ref,
    cen, pool_ref, labels_ref, picks_ref, cur,
    csq, part, feats, kern, labs, coefb, lacc, lpart, lrecv, lsum, ysend, ysum, resid, gown,
    near_out, near_in, cross_out, cross_in,
    load_sem, send_sem, feat_sem, log_sem, near_sem, cross_sem, mine_sem, over_sem, pass_sem,
):
    steps, batch = picks_ref.shape
    fd, pool_dev = pool_ref.shape
    classes, own = cur.shape
    width, cen_dev = cen.shape
    rows_n = batch // CHUNKS
    half = rows_n // 2
    piece = classes // PIECES
    tile = 2 * own
    tiles = cen_dev // tile
    blocks = cen_dev // own

    c = lax.axis_index("centre")
    s = lax.axis_index("sample")
    y, k = lax.div(c, 2), lax.rem(c, 2)
    z, x = lax.div(s, 2), lax.rem(s, 2)
    z_near = z + 1 - 2 * lax.rem(z, 2)
    z_over = lax.rem(z + 2, 4)
    z_both = lax.rem(z_near + 2, 4)
    far_c = (1 - y) * 2 + k
    sib = {"centre": c + 1 - 2 * k}
    far = {"centre": far_c}
    over = {"sample": z_over * 2 + x}
    quad = [z * 2 + 1 - x, z_near * 2 + x, z_near * 2 + 1 - x]
    across = [z_over * 2 + 1 - x, z_both * 2 + x, z_both * 2 + 1 - x]
    near = [{"sample": q} for q in quad]

    barrier = pltpu.get_barrier_semaphore()
    for peer in [sib, far, over] + near:
        pl.semaphore_signal(barrier, inc=1, device_id=peer, device_id_type=MESH)

    loads = [
        pltpu.make_async_copy(src, dst, load_sem.at[i])
        for i, (src, dst) in enumerate(
            [(picks_hbm, picks_ref), (pool_hbm, pool_ref), (labels_hbm, labels_ref), (coefs_hbm, cur), (cen_hbm, cen)]
        )
    ]
    for i in (0, 1, 3, 2, 4):
        loads[i].start()

    def make(kind, t, src, dst, recv, peer):
        return pltpu.make_async_remote_copy(
            src_ref=src, dst_ref=dst, send_sem=send_sem.at[kind], recv_sem=recv,
            device_id=peer, device_id_type=MESH,
        )

    def rows_of(i):
        return slice(i * rows_n, (i + 1) * rows_n)

    def piece_of(h):
        return slice(h * piece, (h + 1) * piece)

    def feat_copy(t, i, owner, n, peer):
        slot = feats.at[t, owner, rows_of(i)]
        return make(0, t, slot, slot, feat_sem.at[t, n, i], peer)

    def feat_far(t, i):
        return feat_copy(t, i, c, 0, far)

    def feat_sib(t, i):
        return feat_copy(t, i, c, 1, sib)

    def feat_fwd(t, i):
        return feat_copy(t, i, far_c, 2, sib)

    def log_sib(t, i):
        return make(1, t, lpart.at[t, i, 1 - k], lrecv.at[t, i], log_sem.at[0, t, i], sib)

    def log_far(t, i):
        return make(6, t, ysend.at[t, i], ysum.at[t, i], log_sem.at[1, t, i], far)

    def res_sib(t, i):
        return make(2, t, resid.at[t, i, k], resid.at[t, i, k], log_sem.at[2, t, i], sib)

    def sum_near(t, n, q, h):
        rows = piece_of(h)
        return make(3, t, near_out.at[t, n, q, rows], near_in.at[t, n, q, rows], near_sem.at[n, q, h], near[q])

    def sum_over(t, h):
        rows = piece_of(h)
        return make(4, t, cross_out.at[t, rows], cross_in.at[t, rows], cross_sem.at[h], over)

    def coef_mine(t, q, h=None):
        slot = coefb.at[t, s] if h is None else coefb.at[t, s, piece_of(h)]
        return make(5, t, slot, slot, mine_sem.at[q], near[q])

    def coef_over(t, h):
        slot = coefb.at[t, s, piece_of(h)]
        return make(5, t, slot, slot, over_sem.at[h], over)

    def coef_pass(t, q, h):
        slot = coefb.at[t, z_over * 2 + x, piece_of(h)]
        return make(5, t, slot, slot, pass_sem.at[q, h], near[q])

    def pick(t, i):
        chosen = picks_ref[t:t + 1, rows_of(i)] - s * pool_dev
        rows = lax.broadcasted_iota(jnp.int32, (pool_dev, rows_n), 0)
        hot = jnp.where(rows == chosen, -2.0, 0.0).astype(jnp.bfloat16)
        got = jnp.dot(pool_ref[...], hot, preferred_element_type=jnp.float32)
        feats[t, c, rows_of(i)] = got.T.astype(jnp.bfloat16)
        return hot

    def pick_labels(t, i, hot):
        label_rows = jnp.broadcast_to(labels_ref[...].astype(jnp.float32), (16, pool_dev)).astype(jnp.bfloat16)
        lab = -0.5 * jnp.dot(label_rows, hot, preferred_element_type=jnp.float32)
        for h in range(2):
            labs[t, 2 * i + h] = lab[0:8, h * half:(h + 1) * half]

    bend = (1.0 / (LENGTH_SCALE * math.log(2.0))) ** 2

    def laplace(t, i, first, last):
        rows = rows_of(i)
        ssq = sum(
            jnp.sum(jnp.square(feats[t, q, rows].astype(jnp.float32)), axis=1, keepdims=True) for q in range(4)
        ) * 0.25

        def body(j, _):
            cols = pl.ds(pl.multiple_of(j * tile, tile), tile)
            lhs = jnp.concatenate([feats[t, q, rows] for q in range(4)], axis=1)
            cross = jnp.dot(lhs, cen[:, cols], preferred_element_type=jnp.float32)
            arg = ((ssq + csq[:, cols]) + cross) * (bend / width) + bend * EPS
            arg = jnp.maximum(arg, 1e-30)
            value = jnp.exp2(-(arg * lax.rsqrt(arg)))
            for q in range(2):
                kern[t, j * 2 + q, rows] = value[:, q * own:(q + 1) * own].astype(jnp.bfloat16)
            return 0

        lax.fori_loop(first, last, body, 0, unroll=last - first)

    def near_part(i):
        rows = rows_of(i)
        slots = (2 * y, 2 * y + 1)
        ssq = sum(
            jnp.sum(jnp.square(feats[0, q, rows].astype(jnp.float32)), axis=1, keepdims=True) for q in slots
        ) * 0.25

        def body(j, _):
            cols = pl.ds(pl.multiple_of(j * tile, tile), tile)
            lhs = jnp.concatenate([feats[0, q, rows] for q in slots], axis=1)
            deep = pl.ds(pl.multiple_of(2 * y * fd, 2 * fd), 2 * fd)
            cross = jnp.dot(lhs, cen[deep, cols], preferred_element_type=jnp.float32)
            part[rows, cols] = (ssq + csq[:, cols]) + cross
            return 0

        lax.fori_loop(0, tiles, body, 0, unroll=tiles)

    def laplace_far(i, first, last):
        rows = rows_of(i)
        slots = (2 * (1 - y), 2 * (1 - y) + 1)
        ssq = sum(
            jnp.sum(jnp.square(feats[0, q, rows].astype(jnp.float32)), axis=1, keepdims=True) for q in slots
        ) * 0.25

        def body(j, _):
            cols = pl.ds(pl.multiple_of(j * tile, tile), tile)
            lhs = jnp.concatenate([feats[0, q, rows] for q in slots], axis=1)
            deep = pl.ds(pl.multiple_of(2 * (1 - y) * fd, 2 * fd), 2 * fd)
            cross = jnp.dot(lhs, cen[deep, cols], preferred_element_type=jnp.float32)
            arg = ((part[rows, cols] + ssq) + cross) * (bend / width) + bend * EPS
            arg = jnp.maximum(arg, 1e-30)
            value = jnp.exp2(-(arg * lax.rsqrt(arg)))
            for q in range(2):
                kern[0, j * 2 + q, rows] = value[:, q * own:(q + 1) * own].astype(jnp.bfloat16)
            return 0

        lax.fori_loop(first, last, body, 0, unroll=last - first)

    def logits(t, i, group, first, last):
        total = sum(
            lax.dot_general(coefb[t, j], kern[t, j, rows_of(i)], NT, preferred_element_type=jnp.float32)
            for j in group
        )
        if not first:
            total = total + lacc[i]
        if not last:
            lacc[i] = total
            return
        for h in range(2):
            lpart[t, i, h] = total[:, h * half:(h + 1) * half]
        log_sib(t, i).start()

    def chip_sum(t, i):
        log_sib(t, i).wait_recv()
        value = lpart[t, i, k] + lrecv[t, i]
        lsum[t, i] = value
        top = jnp.maximum(jnp.max(jnp.abs(value), axis=0, keepdims=True), 2.0 ** -100)
        level = jnp.ceil(jnp.log(top) * (LEVELS / math.log(2.0)))
        code = jnp.round(value * (FIXED * jnp.exp2(level * (-1.0 / LEVELS))))
        ysend[t, i, 0:classes] = code.astype(jnp.int16)
        ysend[t, i, classes:] = jnp.broadcast_to(level, (16, half)).astype(jnp.int16)
        log_far(t, i).start()

    def residual(t, i):
        log_far(t, i).wait_recv()
        level = ysum[t, i, classes:].astype(jnp.float32)[0:1]
        other = ysum[t, i, 0:classes].astype(jnp.float32) * (jnp.exp2(level * (1.0 / LEVELS)) * (1.0 / FIXED))
        value = (lsum[t, i] + other) * logit_scale
        expo = jnp.exp(value - jnp.max(value, axis=0, keepdims=True))
        probs = expo / jnp.sum(expo, axis=0, keepdims=True)
        ids = lax.broadcasted_iota(jnp.int32, (classes, half), 0).astype(jnp.float32)
        hot = jnp.where(ids == labs[t, 2 * i + k][0:1, :], 1.0, 0.0)
        resid[t, i, k] = (probs - hot).astype(jnp.bfloat16)
        res_sib(t, i).start()

    def gradient(t):
        for i in range(CHUNKS):
            res_sib(t, i).wait_recv()
        whole = jnp.concatenate([resid[t, i, h] for i in range(CHUNKS) for h in range(2)], axis=1)

        def grad(block):
            return jnp.dot(whole, kern[t, block], preferred_element_type=jnp.float32)

        parts = [grad(block) for block in across]
        for h in range(PIECES):
            for q in (2, 1, 0):
                near_out[t, 0, q, piece_of(h)] = encode(parts[q][piece_of(h)])
                sum_near(t, 0, q, h).start()
        parts = [grad(block) for block in quad]
        for h in range(PIECES):
            for q in (2, 1, 0):
                near_out[t, 1, q, piece_of(h)] = encode(parts[q][piece_of(h)])
                sum_near(t, 1, q, h).start()
        gown[0] = grad(z_over * 2 + x)
        gown[1] = grad(s)

    def reduce_near(t, n, h):
        total = gown[n, piece_of(h)]
        for q in range(3):
            sum_near(t, n, q, h).wait_recv()
            total = total + decode(near_in[t, n, q, piece_of(h)])
        return total

    def reduce_across(t, h):
        cross_out[t, piece_of(h)] = encode(reduce_near(t, 0, h))
        sum_over(t, h).start()

    def reduce_end(t, h):
        total = reduce_near(t, 1, h)
        sum_over(t, h).wait_recv()
        return total + decode(cross_in[t, piece_of(h)])

    def share_mine(t):
        for h in range(PIECES):
            coef_over(t, h).start()
        for q in range(3):
            coef_mine(t, q).start()

    def share_pass(t, h):
        coef_over(t, h).wait_recv()
        for q in (2, 1, 0):
            coef_pass(t, q, h).start()

    def share_near(t):
        for q in range(3):
            coef_mine(t, q).wait_recv()

    def share_end(t, q):
        for h in range(PIECES):
            coef_pass(t, q, h).wait_recv()

    first_group = [s] + quad + [z_over * 2 + x]

    pl.semaphore_wait(barrier, 6)
    loads[3].wait()
    coefb[0, s] = cur[...].astype(jnp.bfloat16)
    share_mine(0)
    loads[0].wait()
    loads[1].wait()
    hots = []
    for i in range(CHUNKS):
        hots.append(pick(0, i))
        feat_far(0, i).start()
        feat_sib(0, i).start()
    loads[2].wait()
    for i in range(CHUNKS):
        pick_labels(0, i, hots[i])
    for i in range(CHUNKS):
        pick_labels(1, i, pick(1, i))
    loads[4].wait()

    def square(j, _):
        cols = pl.ds(pl.multiple_of(j * own, own), own)
        block = cen[:, cols].astype(jnp.float32)
        csq[:, cols] = jnp.sum(block * block, axis=0, keepdims=True)
        return 0

    lax.fori_loop(0, cen_dev // own, square, 0)

    feat_sib(0, 0).wait_recv()
    near_part(0)
    share_pass(0, 0)
    feat_sib(0, 1).wait_recv()
    near_part(1)
    for h in range(1, PIECES):
        share_pass(0, h)
    feat_far(0, 0).wait_recv()
    feat_fwd(0, 0).start()
    feat_fwd(0, 0).wait_recv()
    laplace_far(0, 0, tiles // 2)
    feat_far(0, 1).wait_recv()
    feat_fwd(0, 1).start()
    laplace_far(0, tiles // 2, tiles)
    feat_fwd(0, 1).wait_recv()
    laplace_far(1, 0, tiles)
    share_near(0)
    for q in range(3):
        share_end(0, q)
    for i in range(CHUNKS):
        logits(0, i, range(blocks), True, True)
    for i in range(CHUNKS):
        chip_sum(0, i)
    residual(0, 0)
    for i in range(CHUNKS):
        feat_far(1, i).start()
        feat_sib(1, i).start()
    residual(0, 1)

    gradient(0)
    feat_far(1, 0).wait_recv()
    feat_fwd(1, 0).start()
    feat_sib(1, 0).wait_recv()
    reduce_across(0, 0)
    feat_fwd(1, 0).wait_recv()
    reduce_across(0, 1)
    laplace(1, 0, 0, 1)
    reduce_across(0, 2)
    feat_far(1, 1).wait_recv()
    feat_fwd(1, 1).start()
    laplace(1, 0, 1, tiles)
    for h in range(PIECES):
        rows = piece_of(h)
        fresh = cur[rows] - rate * reduce_end(0, h)
        cur[rows] = fresh
        coefb[1, s, rows] = fresh.astype(jnp.bfloat16)
        coef_over(1, h).start()
        for q in (2, 1, 0):
            coef_mine(1, q, h).start()
    feat_sib(1, 1).wait_recv()
    feat_fwd(1, 1).wait_recv()
    laplace(1, 1, 0, tiles)
    for h in range(PIECES):
        share_pass(1, h)
    share_near(1)
    for i in range(CHUNKS):
        logits(1, i, first_group, True, False)
    for q in range(3):
        share_end(1, q)
        for i in range(CHUNKS):
            logits(1, i, across[q:q + 1], False, q == 2)
    for i in range(CHUNKS):
        chip_sum(1, i)
    for i in range(CHUNKS):
        residual(1, i)
    gradient(1)
    for h in range(PIECES):
        reduce_across(1, h)
    for h in range(PIECES):
        out_ref[piece_of(h)] = cur[piece_of(h)] - rate * reduce_end(1, h)

    def drain(kind, ref):
        make(kind, 0, ref, ref, cross_sem.at[0], over).wait_send()

    drain(0, feats.at[:, 0:3])
    drain(1, lpart.at[:, 0])
    drain(2, resid.at[:, 0])
    drain(3, near_out)
    drain(4, cross_out)
    drain(5, coefb.at[:, 0:7])
    drain(6, ysend)


def line_device(n_c, n_s, centres, pool, labels, picks, coefs):
    width, cen_dev = centres.shape
    fd, pool_dev = pool.shape
    steps, batch = picks.shape
    classes, own = coefs.shape
    half = batch // CHUNKS // 2
    bf16, f32, i16 = jnp.bfloat16, jnp.float32, jnp.int16
    dma = pltpu.SemaphoreType.DMA
    return pl.pallas_call(
        functools.partial(
            line_kernel, LOGIT_GAIN / (cen_dev * n_c), STEP_GAIN * LOGIT_GAIN / (batch * n_s)
        ),
        out_shape=pltpu.VMEM((classes, own), f32),
        in_specs=[pl.BlockSpec(memory_space=pltpu.HBM)] * 5,
        out_specs=pl.BlockSpec(memory_space=pltpu.VMEM),
        scratch_shapes=[
            pltpu.VMEM((width, cen_dev), bf16),
            pltpu.VMEM((fd, pool_dev), bf16),
            pltpu.VMEM((1, pool_dev), jnp.int32),
            pltpu.VMEM((steps, batch), jnp.int32),
            pltpu.VMEM((classes, own), f32),
            pltpu.VMEM((1, cen_dev), f32),
            pltpu.VMEM((batch, cen_dev), f32),
            pltpu.VMEM((steps, n_c, batch, fd), bf16),
            pltpu.VMEM((steps, n_s, batch, own), bf16),
            pltpu.VMEM((steps, 2 * CHUNKS, 8, half), f32),
            pltpu.VMEM((steps, n_s, classes, own), bf16),
            pltpu.VMEM((CHUNKS, classes, 2 * half), f32),
            pltpu.VMEM((steps, CHUNKS, 2, classes, half), f32),
            pltpu.VMEM((steps, CHUNKS, classes, half), f32),
            pltpu.VMEM((steps, CHUNKS, classes, half), f32),
            pltpu.VMEM((steps, CHUNKS, classes + 16, half), i16),
            pltpu.VMEM((steps, CHUNKS, classes + 16, half), i16),
            pltpu.VMEM((steps, CHUNKS, 2, classes, half), bf16),
            pltpu.VMEM((2, classes, own), f32),
            pltpu.VMEM((steps, 2, 3, classes, own), i16),
            pltpu.VMEM((steps, 2, 3, classes, own), i16),
            pltpu.VMEM((steps, classes, own), i16),
            pltpu.VMEM((steps, classes, own), i16),
            dma((5,)),
            dma((7,)),
            dma((steps, 3, CHUNKS)),
            dma((3, steps, CHUNKS)),
            dma((2, 3, PIECES)),
            dma((PIECES,)),
            dma((3,)),
            dma((PIECES,)),
            dma((3, PIECES)),
        ],
        compiler_params=pltpu.CompilerParams(
            collective_id=0, has_side_effects=True, vmem_limit_bytes=60 * 1024 * 1024
        ),
    )(centres, pool, labels.reshape(1, pool_dev), picks, coefs)


def suits_line(mesh, centres, pool, picks, coefs):
    n_c, n_s = mesh.shape["centre"], mesh.shape["sample"]
    own, batch, fd = coefs.shape[1], picks.shape[1], pool.shape[0]
    return (
        n_c == 4 and n_s == 8 and own % 128 == 0 and fd % 128 == 0 and picks.shape[0] == 2
        and batch % (256 * CHUNKS) == 0 and coefs.shape[0] % (16 * PIECES) == 0 and batch * n_s <= 4096
    )


def on_device(mesh, centres, pool, labels, picks, coefs):
    n_c, n_s = mesh.shape["centre"], mesh.shape["sample"]
    if suits_line(mesh, centres, pool, picks, coefs):
        return line_device(n_c, n_s, centres, pool, labels, picks, coefs)
    width, cen_dev = centres.shape
    fd, pool_dev = pool.shape
    steps, batch = picks.shape
    classes, own = coefs.shape
    share = batch // n_c
    bf16, f32 = jnp.bfloat16, jnp.float32
    body = functools.partial(
        kernel, n_c, n_s, LOGIT_GAIN / (cen_dev * n_c), STEP_GAIN * LOGIT_GAIN / (batch * n_s)
    )
    vmem = pl.BlockSpec(memory_space=pltpu.VMEM)
    return pl.pallas_call(
        body,
        out_shape=jax.ShapeDtypeStruct((classes, own), f32),
        in_specs=[pl.BlockSpec(memory_space=pl.ANY)] + [vmem] * 4,
        out_specs=vmem,
        scratch_shapes=[
            pltpu.VMEM((width, cen_dev), bf16),
            pltpu.VMEM((1, cen_dev), f32),
            pltpu.VMEM((steps, n_c, batch, fd), bf16),
            pltpu.VMEM((steps, n_s, batch, own), bf16),
            pltpu.VMEM((steps, n_c, 8, share), f32),
            pltpu.VMEM((steps, n_s, classes, own), bf16),
            pltpu.VMEM((steps, n_c, classes, share), LOGIT_WIRE),
            pltpu.VMEM((steps, n_c - 1, classes, share), LOGIT_WIRE),
            pltpu.VMEM((steps, n_c, classes, share), bf16),
            pltpu.VMEM((steps, n_s - 2, classes, own), GRAD_WIRE),
            pltpu.VMEM((steps, n_s - 2, classes, own), GRAD_WIRE),
            pltpu.VMEM((steps, classes, own), f32),
            pltpu.VMEM((steps, classes, own), f32),
            pltpu.VMEM((classes, own), f32),
            pltpu.SemaphoreType.DMA,
            pltpu.SemaphoreType.DMA((steps * (3 * (n_c - 1) + 2 * (n_s - 1)),)),
            pltpu.SemaphoreType.DMA((steps, n_c - 1)),
            pltpu.SemaphoreType.DMA((steps, n_c - 1)),
            pltpu.SemaphoreType.DMA((steps, n_c - 1)),
            pltpu.SemaphoreType.DMA((steps, n_s - 1)),
            pltpu.SemaphoreType.DMA((steps, n_s - 1)),
        ],
        compiler_params=pltpu.CompilerParams(
            collective_id=0, has_side_effects=True, vmem_limit_bytes=60 * 1024 * 1024
        ),
    )(centres, pool, labels.reshape(1, pool_dev), picks, coefs)


def solution(mesh):
    placed = (
        P(None, "centre"),
        P("centre", "sample"),
        P("sample"),
        P(None, "sample"),
        P(None, ("centre", "sample")),
    )
    return jax.shard_map(
        functools.partial(on_device, mesh),
        mesh=mesh,
        in_specs=placed,
        out_specs=P(None, ("centre", "sample")),
        check_vma=False,
    )
```

```python
import functools
import math

import jax
import jax.numpy as jnp
from jax import lax
from jax.experimental import pallas as pl
from jax.experimental.pallas import tpu as pltpu
from jax.sharding import PartitionSpec as P

LOGIT_GAIN = 16.0
LENGTH_SCALE = 0.5
STEP_GAIN = 2048.0
EPS = 1e-06

GRAD_WIRE = jnp.bfloat16
LOGIT_WIRE = jnp.float32
MESH = pl.DeviceIdType.MESH
NT = (((1,), (1,)), ((), ()))


def kernel(
    n_c, n_s, logit_scale, rate,
    cen_hbm, pool_ref, labels_ref, picks_ref, coefs_ref, out_ref,
    cen, csq, feats, kern, labs, coefb, lsend, lrecv, resid, gsend, grecv, psend, precv, cur,
    cen_sem, send_sem, feat_sem, log_sem, res_sem, coef_sem, grad_sem,
):
    steps, batch = picks_ref.shape
    fd, pool_dev = pool_ref.shape
    classes, own = coefs_ref.shape
    width, cen_dev = cen.shape
    share = batch // n_c
    ny = n_c // 2
    tile = max(own, min(256, cen_dev))
    pieces = tile // own

    c = lax.axis_index("centre")
    s = lax.axis_index("sample")
    sib = c + 1 - 2 * lax.rem(c, 2)
    c_peers = [lax.rem(c + r, n_c) for r in range(1, n_c)]
    s_peers = [lax.rem(s + r, n_s) for r in range(1, n_s)]
    pair = s + 1 - 2 * lax.rem(s, 2)
    nz = n_s // 2
    order = sorted(range(1, nz), key=lambda q: -min(q, nz - q))

    barrier = pltpu.get_barrier_semaphore()
    for peer in c_peers:
        pl.semaphore_signal(barrier, inc=1, device_id={"centre": peer}, device_id_type=MESH)
    for peer in s_peers:
        pl.semaphore_signal(barrier, inc=1, device_id={"sample": peer}, device_id_type=MESH)

    load = pltpu.make_async_copy(cen_hbm, cen, cen_sem)
    load.start()
    started = []

    def send(src, dst, recv, axis, peer):
        copy = pltpu.make_async_remote_copy(
            src_ref=src, dst_ref=dst, send_sem=send_sem.at[len(started)], recv_sem=recv,
            device_id={axis: peer}, device_id_type=MESH,
        )
        copy.start()
        started.append(copy)
        return copy

    label_rows = jnp.broadcast_to(labels_ref[...].astype(jnp.float32), (16, pool_dev)).astype(jnp.bfloat16)

    def pick(t):
        chosen = picks_ref[t:t + 1, :] - s * pool_dev
        rows = lax.broadcasted_iota(jnp.int32, (pool_dev, batch), 0)
        hot = jnp.where(rows == chosen, -2.0, 0.0).astype(jnp.bfloat16)
        got = jnp.dot(pool_ref[...], hot, preferred_element_type=jnp.float32)
        feats[t, c] = got.T.astype(jnp.bfloat16)
        lab = -0.5 * jnp.dot(label_rows, hot, preferred_element_type=jnp.float32)
        for k in range(n_c):
            labs[t, k] = lab[0:8, k * share:(k + 1) * share]

    def send_feats(t):
        mine = feats.at[t, c]
        direct = []
        for q in range(1, ny):
            direct.append(send(mine, mine, feat_sem.at[t, q], "centre", lax.rem(c + 2 * q, n_c)))
        return [send(mine, mine, feat_sem.at[t, 0], "centre", sib)], direct

    def forward_feats(t, near, direct):
        for q, copy in enumerate(direct, 1):
            copy.wait_recv()
            slot = feats.at[t, lax.rem(c - 2 * q + n_c, n_c)]
            near.append(send(slot, slot, feat_sem.at[t, ny - 1 + q], "centre", sib))
        for copy in near:
            copy.wait_recv()

    def send_coefs(t):
        mine = coefb.at[t, s]
        direct = [
            (q, send(mine, mine, coef_sem.at[t, q], "sample", lax.rem(s + 2 * q, n_s)))
            for q in order
        ]
        return [send(mine, mine, coef_sem.at[t, 0], "sample", pair)], direct

    def forward_coefs(t, near, direct):
        for q, copy in direct:
            copy.wait_recv()
            slot = coefb.at[t, lax.rem(s - 2 * q + n_s, n_s)]
            near.append(send(slot, slot, coef_sem.at[t, nz - 1 + q], "sample", pair))

    cur[...] = coefs_ref[...]
    coefb[0, s] = coefs_ref[...].astype(jnp.bfloat16)
    pl.semaphore_wait(barrier, n_c - 1 + n_s - 1)
    coef_near, coef_direct = send_coefs(0)
    pick(0)
    moves = [send_feats(0)]
    pick(1)
    moves.append(send_feats(1))

    load.wait()

    def square(j, _):
        cols = pl.ds(pl.multiple_of(j * tile, tile), tile)
        block = cen[:, cols].astype(jnp.float32)
        csq[:, cols] = jnp.sum(block * block, axis=0, keepdims=True)
        return 0

    lax.fori_loop(0, cen_dev // tile, square, 0)

    bend = (1.0 / (LENGTH_SCALE * math.log(2.0))) ** 2

    def laplace(t):
        parts = [feats[t, k] for k in range(n_c)]
        ssq = sum(
            jnp.sum(jnp.square(p.astype(jnp.float32)), axis=1, keepdims=True) for p in parts
        ) * 0.25
        if fd % 128 == 0:
            parts = [jnp.concatenate(parts, axis=1)]
        deep = width // len(parts)

        def body(j, _):
            cols = pl.ds(pl.multiple_of(j * tile, tile), tile)
            cross = sum(
                jnp.dot(p, cen[k * deep:(k + 1) * deep, cols], preferred_element_type=jnp.float32)
                for k, p in enumerate(parts)
            )
            arg = ((ssq + csq[:, cols]) + cross) * (bend / width) + bend * EPS
            arg = jnp.maximum(arg, 1e-30)
            value = jnp.exp2(-(arg * lax.rsqrt(arg)))
            for k in range(pieces):
                kern[t, j * pieces + k] = value[:, k * own:(k + 1) * own].astype(jnp.bfloat16)
            return 0

        lax.fori_loop(0, cen_dev // tile, body, 0)

    def residual(t):
        part = sum(
            lax.dot_general(coefb[t, j], kern[t, j], NT, preferred_element_type=jnp.float32)
            for j in range(n_s)
        )
        for k in range(n_c):
            lsend[t, k] = part[:, k * share:(k + 1) * share].astype(LOGIT_WIRE)
        copies = [
            send(lsend.at[t, peer], lrecv.at[t, r], log_sem.at[t, r], "centre", peer)
            for r, peer in enumerate(c_peers)
        ]
        if t + 1 < steps:
            forward_feats(t + 1, *moves[t + 1])
        total = lsend[t, c].astype(jnp.float32)
        for r, copy in enumerate(copies):
            copy.wait_recv()
            total = total + lrecv[t, r].astype(jnp.float32)
        logits = total * logit_scale
        expo = jnp.exp(logits - jnp.max(logits, axis=0, keepdims=True))
        probs = expo / jnp.sum(expo, axis=0, keepdims=True)
        ids = lax.broadcasted_iota(jnp.int32, (classes, share), 0).astype(jnp.float32)
        hot = jnp.where(ids == labs[t, c][0:1, :], 1.0, 0.0)
        resid[t, c] = (probs - hot).astype(jnp.bfloat16)
        mine = resid.at[t, c]
        copies = [
            send(mine, mine, res_sem.at[t, r], "centre", peer) for r, peer in enumerate(c_peers)
        ]
        for copy in copies:
            copy.wait_recv()

    def gradient(t):
        if share % 128 == 0:
            whole = jnp.concatenate([resid[t, k] for k in range(n_c)], axis=1)

            def grad(j):
                return jnp.dot(whole, kern[t, j], preferred_element_type=jnp.float32)
        else:
            def grad(j):
                return sum(
                    jnp.dot(resid[t, k], kern[t, j, k * share:(k + 1) * share, :],
                            preferred_element_type=jnp.float32)
                    for k in range(n_c)
                )
        def put(i, value, peer):
            gsend[t, i] = value.astype(GRAD_WIRE)
            return send(gsend.at[t, i], grecv.at[t, i], grad_sem.at[t, i], "sample", peer)

        far = [lax.rem(start + 2 * q, n_s) for q in order for start in (s, pair)]
        copies = [put(i, grad(peer), peer) for i, peer in enumerate(far)]
        psend[t] = grad(pair)
        last = send(psend.at[t], precv.at[t], grad_sem.at[t, n_s - 2], "sample", pair)
        return grad(s), last, copies

    forward_coefs(0, coef_near, coef_direct[:2])
    forward_feats(0, *moves[0])
    forward_coefs(0, coef_near, coef_direct[2:])
    laplace(0)
    for t in range(steps):
        for copy in coef_near:
            copy.wait_recv()
        residual(t)
        total, last, copies = gradient(t)
        if t + 1 < steps:
            laplace(t + 1)
        last.wait_recv()
        total = total + precv[t]
        for r, copy in enumerate(copies):
            copy.wait_recv()
            total = total + grecv[t, r].astype(jnp.float32)
        fresh = cur[...] - rate * total
        if t + 1 < steps:
            cur[...] = fresh
            coefb[t + 1, s] = fresh.astype(jnp.bfloat16)
            coef_near, coef_direct = send_coefs(t + 1)
            forward_coefs(t + 1, coef_near, coef_direct)
        else:
            out_ref[...] = fresh
    for copy in started:
        copy.wait_send()


CHUNKS = 2
PIECES = 3
LOG_STEPS = 520.0
LOG_LOW = 50.0
LEVELS = 64.0
FIXED = 32000.0


def encode(value):
    size = jnp.maximum(jnp.abs(value), 2.0 ** -LOG_LOW)
    code = jnp.round((jnp.log(size) * (1.0 / math.log(2.0)) + LOG_LOW) * LOG_STEPS)
    return jnp.where(value < 0.0, -code, code).astype(jnp.int16)


def decode(code):
    number = code.astype(jnp.float32)
    size = jnp.exp2(jnp.abs(number) * (1.0 / LOG_STEPS) - LOG_LOW)
    return jnp.where(number < 0.0, -size, jnp.where(number > 0.0, size, 0.0))


def line_kernel(
    logit_scale, rate,
    cen_hbm, pool_hbm, labels_hbm, picks_hbm, coefs_hbm, out_ref,
    cen, pool_ref, labels_ref, picks_ref, cur,
    csq, part, feats, kern, labs, coefb, lacc, lpart, lrecv, lsum, ysend, ysum, resid, gown,
    near_out, near_in, cross_out, cross_in,
    load_sem, send_sem, feat_sem, log_sem, near_sem, cross_sem, mine_sem, over_sem, pass_sem,
):
    steps, batch = picks_ref.shape
    fd, pool_dev = pool_ref.shape
    classes, own = cur.shape
    width, cen_dev = cen.shape
    rows_n = batch // CHUNKS
    half = rows_n // 2
    piece = classes // PIECES
    tile = 2 * own
    tiles = cen_dev // tile
    blocks = cen_dev // own

    c = lax.axis_index("centre")
    s = lax.axis_index("sample")
    y, k = lax.div(c, 2), lax.rem(c, 2)
    z, x = lax.div(s, 2), lax.rem(s, 2)
    z_near = z + 1 - 2 * lax.rem(z, 2)
    z_over = lax.rem(z + 2, 4)
    z_both = lax.rem(z_near + 2, 4)
    far_c = (1 - y) * 2 + k
    sib = {"centre": c + 1 - 2 * k}
    far = {"centre": far_c}
    over = {"sample": z_over * 2 + x}
    quad = [z * 2 + 1 - x, z_near * 2 + x, z_near * 2 + 1 - x]
    across = [z_over * 2 + 1 - x, z_both * 2 + x, z_both * 2 + 1 - x]
    near = [{"sample": q} for q in quad]

    barrier = pltpu.get_barrier_semaphore()
    for peer in [sib, far, over] + near:
        pl.semaphore_signal(barrier, inc=1, device_id=peer, device_id_type=MESH)

    loads = [
        pltpu.make_async_copy(src, dst, load_sem.at[i])
        for i, (src, dst) in enumerate(
            [(picks_hbm, picks_ref), (pool_hbm, pool_ref), (labels_hbm, labels_ref), (coefs_hbm, cur), (cen_hbm, cen)]
        )
    ]
    for i in (1, 3, 0, 2):
        loads[i].start()

    def make(kind, t, src, dst, recv, peer):
        return pltpu.make_async_remote_copy(
            src_ref=src, dst_ref=dst, send_sem=send_sem.at[kind], recv_sem=recv,
            device_id=peer, device_id_type=MESH,
        )

    def rows_of(i):
        return slice(i * rows_n, (i + 1) * rows_n)

    def piece_of(h):
        return slice(h * piece, (h + 1) * piece)

    def feat_copy(t, i, owner, n, peer):
        slot = feats.at[t, owner, rows_of(i)]
        return make(0, t, slot, slot, feat_sem.at[t, n, i], peer)

    def feat_far(t, i):
        return feat_copy(t, i, c, 0, far)

    def feat_sib(t, i):
        return feat_copy(t, i, c, 1, sib)

    def feat_fwd(t, i):
        return feat_copy(t, i, far_c, 2, sib)

    def log_sib(t, i):
        return make(1, t, lpart.at[t, i, 1 - k], lrecv.at[t, i], log_sem.at[0, t, i], sib)

    def log_far(t, i):
        return make(6, t, ysend.at[t, i], ysum.at[t, i], log_sem.at[1, t, i], far)

    def res_sib(t, i):
        return make(2, t, resid.at[t, i, k], resid.at[t, i, k], log_sem.at[2, t, i], sib)

    def sum_near(t, n, q, h):
        rows = piece_of(h)
        return make(3, t, near_out.at[t, n, q, rows], near_in.at[t, n, q, rows], near_sem.at[n, q, h], near[q])

    def sum_over(t, h):
        rows = piece_of(h)
        return make(4, t, cross_out.at[t, rows], cross_in.at[t, rows], cross_sem.at[h], over)

    def coef_mine(t, q, h=None):
        slot = coefb.at[t, s] if h is None else coefb.at[t, s, piece_of(h)]
        return make(5, t, slot, slot, mine_sem.at[q], near[q])

    def coef_over(t, h):
        slot = coefb.at[t, s, piece_of(h)]
        return make(5, t, slot, slot, over_sem.at[h], over)

    def coef_pass(t, q, h):
        slot = coefb.at[t, z_over * 2 + x, piece_of(h)]
        return make(5, t, slot, slot, pass_sem.at[q, h], near[q])

    def pick(t, i):
        chosen = picks_ref[t:t + 1, rows_of(i)] - s * pool_dev
        rows = lax.broadcasted_iota(jnp.int32, (pool_dev, rows_n), 0)
        hot = jnp.where(rows == chosen, -2.0, 0.0).astype(jnp.bfloat16)
        got = jnp.dot(pool_ref[...], hot, preferred_element_type=jnp.float32)
        feats[t, c, rows_of(i)] = got.T.astype(jnp.bfloat16)
        return hot

    def pick_labels(t, i, hot):
        label_rows = jnp.broadcast_to(labels_ref[...].astype(jnp.float32), (16, pool_dev)).astype(jnp.bfloat16)
        lab = -0.5 * jnp.dot(label_rows, hot, preferred_element_type=jnp.float32)
        for h in range(2):
            labs[t, 2 * i + h] = lab[0:8, h * half:(h + 1) * half]

    bend = (1.0 / (LENGTH_SCALE * math.log(2.0))) ** 2

    def laplace(t, i, first, last):
        rows = rows_of(i)
        ssq = sum(
            jnp.sum(jnp.square(feats[t, q, rows].astype(jnp.float32)), axis=1, keepdims=True) for q in range(4)
        ) * 0.25

        def body(j, _):
            cols = pl.ds(pl.multiple_of(j * tile, tile), tile)
            lhs = jnp.concatenate([feats[t, q, rows] for q in range(4)], axis=1)
            cross = jnp.dot(lhs, cen[:, cols], preferred_element_type=jnp.float32)
            arg = ((ssq + csq[:, cols]) + cross) * (bend / width) + bend * EPS
            arg = jnp.maximum(arg, 1e-30)
            value = jnp.exp2(-(arg * lax.rsqrt(arg)))
            for q in range(2):
                kern[t, j * 2 + q, rows] = value[:, q * own:(q + 1) * own].astype(jnp.bfloat16)
            return 0

        lax.fori_loop(first, last, body, 0, unroll=last - first)

    def near_part(i):
        rows = rows_of(i)
        slots = (2 * y, 2 * y + 1)
        ssq = sum(
            jnp.sum(jnp.square(feats[0, q, rows].astype(jnp.float32)), axis=1, keepdims=True) for q in slots
        ) * 0.25

        def body(j, _):
            cols = pl.ds(pl.multiple_of(j * tile, tile), tile)
            lhs = jnp.concatenate([feats[0, q, rows] for q in slots], axis=1)
            deep = pl.ds(pl.multiple_of(2 * y * fd, 2 * fd), 2 * fd)
            cross = jnp.dot(lhs, cen[deep, cols], preferred_element_type=jnp.float32)
            part[rows, cols] = (ssq + csq[:, cols]) + cross
            return 0

        lax.fori_loop(0, tiles, body, 0, unroll=tiles)

    def laplace_far(i, first, last):
        rows = rows_of(i)
        slots = (2 * (1 - y), 2 * (1 - y) + 1)
        ssq = sum(
            jnp.sum(jnp.square(feats[0, q, rows].astype(jnp.float32)), axis=1, keepdims=True) for q in slots
        ) * 0.25

        def body(j, _):
            cols = pl.ds(pl.multiple_of(j * tile, tile), tile)
            lhs = jnp.concatenate([feats[0, q, rows] for q in slots], axis=1)
            deep = pl.ds(pl.multiple_of(2 * (1 - y) * fd, 2 * fd), 2 * fd)
            cross = jnp.dot(lhs, cen[deep, cols], preferred_element_type=jnp.float32)
            arg = ((part[rows, cols] + ssq) + cross) * (bend / width) + bend * EPS
            arg = jnp.maximum(arg, 1e-30)
            value = jnp.exp2(-(arg * lax.rsqrt(arg)))
            for q in range(2):
                kern[0, j * 2 + q, rows] = value[:, q * own:(q + 1) * own].astype(jnp.bfloat16)
            return 0

        lax.fori_loop(first, last, body, 0, unroll=last - first)

    def logits(t, i, group, first, last):
        total = sum(
            lax.dot_general(coefb[t, j], kern[t, j, rows_of(i)], NT, preferred_element_type=jnp.float32)
            for j in group
        )
        if not first:
            total = total + lacc[i]
        if not last:
            lacc[i] = total
            return
        for h in range(2):
            lpart[t, i, h] = total[:, h * half:(h + 1) * half]
        log_sib(t, i).start()

    def chip_sum(t, i):
        log_sib(t, i).wait_recv()
        value = lpart[t, i, k] + lrecv[t, i]
        lsum[t, i] = value
        top = jnp.maximum(jnp.max(jnp.abs(value), axis=0, keepdims=True), 2.0 ** -100)
        level = jnp.ceil(jnp.log(top) * (LEVELS / math.log(2.0)))
        code = jnp.round(value * (FIXED * jnp.exp2(level * (-1.0 / LEVELS))))
        ysend[t, i, 0:classes] = code.astype(jnp.int16)
        ysend[t, i, classes:] = jnp.broadcast_to(level, (16, half)).astype(jnp.int16)
        log_far(t, i).start()

    def residual(t, i):
        log_far(t, i).wait_recv()
        level = ysum[t, i, classes:].astype(jnp.float32)[0:1]
        other = ysum[t, i, 0:classes].astype(jnp.float32) * (jnp.exp2(level * (1.0 / LEVELS)) * (1.0 / FIXED))
        value = (lsum[t, i] + other) * logit_scale
        expo = jnp.exp(value - jnp.max(value, axis=0, keepdims=True))
        probs = expo / jnp.sum(expo, axis=0, keepdims=True)
        ids = lax.broadcasted_iota(jnp.int32, (classes, half), 0).astype(jnp.float32)
        hot = jnp.where(ids == labs[t, 2 * i + k][0:1, :], 1.0, 0.0)
        resid[t, i, k] = (probs - hot).astype(jnp.bfloat16)
        res_sib(t, i).start()

    def gradient(t):
        def share(block, h):
            left = jnp.concatenate([resid[t, i, h] for i in range(CHUNKS)], axis=1)
            rows = [pl.ds(pl.multiple_of(i * rows_n + h * half, half), half) for i in range(CHUNKS)]
            right = jnp.concatenate([kern[t, block, r] for r in rows], axis=0)
            return jnp.dot(left, right, preferred_element_type=jnp.float32)

        parts = [share(block, k) for block in across]
        for i in range(CHUNKS):
            res_sib(t, i).wait_recv()
        whole = jnp.concatenate([resid[t, i, h] for i in range(CHUNKS) for h in range(2)], axis=1)

        def grad(block):
            return jnp.dot(whole, kern[t, block], preferred_element_type=jnp.float32)

        parts = [part + share(block, 1 - k) for part, block in zip(parts, across)]
        for h in range(PIECES):
            for q in (2, 1, 0):
                near_out[t, 0, q, piece_of(h)] = encode(parts[q][piece_of(h)])
                sum_near(t, 0, q, h).start()
        parts = [grad(block) for block in quad]
        for h in range(PIECES):
            for q in (2, 1, 0):
                near_out[t, 1, q, piece_of(h)] = encode(parts[q][piece_of(h)])
                sum_near(t, 1, q, h).start()
        gown[0] = grad(z_over * 2 + x)
        gown[1] = grad(s)

    def reduce_near(t, n, h):
        total = gown[n, piece_of(h)]
        for q in range(3):
            sum_near(t, n, q, h).wait_recv()
            total = total + decode(near_in[t, n, q, piece_of(h)])
        return total

    def reduce_across(t, h):
        cross_out[t, piece_of(h)] = encode(reduce_near(t, 0, h))
        sum_over(t, h).start()

    def reduce_end(t, h):
        total = reduce_near(t, 1, h)
        sum_over(t, h).wait_recv()
        return total + decode(cross_in[t, piece_of(h)])

    def share_mine(t):
        for h in range(PIECES):
            coef_over(t, h).start()
        for q in range(3):
            coef_mine(t, q).start()

    def share_pass(t, h):
        coef_over(t, h).wait_recv()
        for q in (2, 1, 0):
            coef_pass(t, q, h).start()

    def share_near(t):
        for q in range(3):
            coef_mine(t, q).wait_recv()

    def share_end(t, q):
        for h in range(PIECES):
            coef_pass(t, q, h).wait_recv()

    first_group = [s] + quad + [z_over * 2 + x]

    pl.semaphore_wait(barrier, 6)
    loads[3].wait()
    coefb[0, s] = cur[...].astype(jnp.bfloat16)
    share_mine(0)
    loads[0].wait()
    loads[1].wait()
    loads[4].start()
    hots = []
    for i in range(CHUNKS):
        hots.append(pick(0, i))
        feat_far(0, i).start()
        feat_sib(0, i).start()
    loads[2].wait()
    for i in range(CHUNKS):
        pick_labels(0, i, hots[i])
    for i in range(CHUNKS):
        pick_labels(1, i, pick(1, i))
    loads[4].wait()

    def square(j, _):
        cols = pl.ds(pl.multiple_of(j * own, own), own)
        block = cen[:, cols].astype(jnp.float32)
        csq[:, cols] = jnp.sum(block * block, axis=0, keepdims=True)
        return 0

    lax.fori_loop(0, cen_dev // own, square, 0)

    feat_sib(0, 0).wait_recv()
    near_part(0)
    share_pass(0, 0)
    feat_sib(0, 1).wait_recv()
    near_part(1)
    for h in range(1, PIECES):
        share_pass(0, h)
    feat_far(0, 0).wait_recv()
    feat_fwd(0, 0).start()
    feat_fwd(0, 0).wait_recv()
    laplace_far(0, 0, tiles // 2)
    feat_far(0, 1).wait_recv()
    feat_fwd(0, 1).start()
    laplace_far(0, tiles // 2, tiles)
    feat_fwd(0, 1).wait_recv()
    laplace_far(1, 0, tiles)
    share_near(0)
    for q in range(3):
        share_end(0, q)
    for i in range(CHUNKS):
        logits(0, i, range(blocks), True, True)
    for i in range(CHUNKS):
        chip_sum(0, i)
    residual(0, 0)
    for i in range(CHUNKS):
        feat_far(1, i).start()
        feat_sib(1, i).start()
    residual(0, 1)

    gradient(0)
    feat_far(1, 0).wait_recv()
    feat_fwd(1, 0).start()
    feat_sib(1, 0).wait_recv()
    reduce_across(0, 0)
    feat_fwd(1, 0).wait_recv()
    reduce_across(0, 1)
    reduce_across(0, 2)
    feat_far(1, 1).wait_recv()
    feat_fwd(1, 1).start()
    laplace(1, 0, 0, tiles)
    for h in range(PIECES):
        rows = piece_of(h)
        fresh = cur[rows] - rate * reduce_end(0, h)
        cur[rows] = fresh
        coefb[1, s, rows] = fresh.astype(jnp.bfloat16)
        coef_over(1, h).start()
        for q in (2, 1, 0):
            coef_mine(1, q, h).start()
    feat_sib(1, 1).wait_recv()
    feat_fwd(1, 1).wait_recv()
    laplace(1, 1, 0, tiles)
    for h in range(PIECES):
        share_pass(1, h)
    share_near(1)
    for i in range(CHUNKS):
        logits(1, i, first_group, True, False)
    for q in range(3):
        share_end(1, q)
        for i in range(CHUNKS):
            logits(1, i, across[q:q + 1], False, q == 2)
    for i in range(CHUNKS):
        chip_sum(1, i)
    for i in range(CHUNKS):
        residual(1, i)
    gradient(1)
    for h in range(PIECES):
        reduce_across(1, h)
    for h in range(PIECES):
        out_ref[piece_of(h)] = cur[piece_of(h)] - rate * reduce_end(1, h)

    def drain(kind, ref):
        make(kind, 0, ref, ref, cross_sem.at[0], over).wait_send()

    drain(0, feats.at[:, 0:3])
    drain(1, lpart.at[:, 0])
    drain(2, resid.at[:, 0])
    drain(3, near_out)
    drain(4, cross_out)
    drain(5, coefb.at[:, 0:7])
    drain(6, ysend)


def line_device(n_c, n_s, centres, pool, labels, picks, coefs):
    width, cen_dev = centres.shape
    fd, pool_dev = pool.shape
    steps, batch = picks.shape
    classes, own = coefs.shape
    half = batch // CHUNKS // 2
    bf16, f32, i16 = jnp.bfloat16, jnp.float32, jnp.int16
    dma = pltpu.SemaphoreType.DMA
    return pl.pallas_call(
        functools.partial(
            line_kernel, LOGIT_GAIN / (cen_dev * n_c), STEP_GAIN * LOGIT_GAIN / (batch * n_s)
        ),
        out_shape=pltpu.VMEM((classes, own), f32),
        in_specs=[pl.BlockSpec(memory_space=pltpu.HBM)] * 5,
        out_specs=pl.BlockSpec(memory_space=pltpu.VMEM),
        scratch_shapes=[
            pltpu.VMEM((width, cen_dev), bf16),
            pltpu.VMEM((fd, pool_dev), bf16),
            pltpu.VMEM((1, pool_dev), jnp.int32),
            pltpu.VMEM((steps, batch), jnp.int32),
            pltpu.VMEM((classes, own), f32),
            pltpu.VMEM((1, cen_dev), f32),
            pltpu.VMEM((batch, cen_dev), f32),
            pltpu.VMEM((steps, n_c, batch, fd), bf16),
            pltpu.VMEM((steps, n_s, batch, own), bf16),
            pltpu.VMEM((steps, 2 * CHUNKS, 8, half), f32),
            pltpu.VMEM((steps, n_s, classes, own), bf16),
            pltpu.VMEM((CHUNKS, classes, 2 * half), f32),
            pltpu.VMEM((steps, CHUNKS, 2, classes, half), f32),
            pltpu.VMEM((steps, CHUNKS, classes, half), f32),
            pltpu.VMEM((steps, CHUNKS, classes, half), f32),
            pltpu.VMEM((steps, CHUNKS, classes + 16, half), i16),
            pltpu.VMEM((steps, CHUNKS, classes + 16, half), i16),
            pltpu.VMEM((steps, CHUNKS, 2, classes, half), bf16),
            pltpu.VMEM((2, classes, own), f32),
            pltpu.VMEM((steps, 2, 3, classes, own), i16),
            pltpu.VMEM((steps, 2, 3, classes, own), i16),
            pltpu.VMEM((steps, classes, own), i16),
            pltpu.VMEM((steps, classes, own), i16),
            dma((5,)),
            dma((7,)),
            dma((steps, 3, CHUNKS)),
            dma((3, steps, CHUNKS)),
            dma((2, 3, PIECES)),
            dma((PIECES,)),
            dma((3,)),
            dma((PIECES,)),
            dma((3, PIECES)),
        ],
        compiler_params=pltpu.CompilerParams(
            collective_id=0, has_side_effects=True, vmem_limit_bytes=60 * 1024 * 1024
        ),
    )(centres, pool, labels.reshape(1, pool_dev), picks, coefs)


def suits_line(mesh, centres, pool, picks, coefs):
    n_c, n_s = mesh.shape["centre"], mesh.shape["sample"]
    own, batch, fd = coefs.shape[1], picks.shape[1], pool.shape[0]
    return (
        n_c == 4 and n_s == 8 and own % 128 == 0 and fd % 128 == 0 and picks.shape[0] == 2
        and batch % (256 * CHUNKS) == 0 and coefs.shape[0] % (16 * PIECES) == 0 and batch * n_s <= 4096
    )


def on_device(mesh, centres, pool, labels, picks, coefs):
    n_c, n_s = mesh.shape["centre"], mesh.shape["sample"]
    if suits_line(mesh, centres, pool, picks, coefs):
        return line_device(n_c, n_s, centres, pool, labels, picks, coefs)
    width, cen_dev = centres.shape
    fd, pool_dev = pool.shape
    steps, batch = picks.shape
    classes, own = coefs.shape
    share = batch // n_c
    bf16, f32 = jnp.bfloat16, jnp.float32
    body = functools.partial(
        kernel, n_c, n_s, LOGIT_GAIN / (cen_dev * n_c), STEP_GAIN * LOGIT_GAIN / (batch * n_s)
    )
    vmem = pl.BlockSpec(memory_space=pltpu.VMEM)
    return pl.pallas_call(
        body,
        out_shape=jax.ShapeDtypeStruct((classes, own), f32),
        in_specs=[pl.BlockSpec(memory_space=pl.ANY)] + [vmem] * 4,
        out_specs=vmem,
        scratch_shapes=[
            pltpu.VMEM((width, cen_dev), bf16),
            pltpu.VMEM((1, cen_dev), f32),
            pltpu.VMEM((steps, n_c, batch, fd), bf16),
            pltpu.VMEM((steps, n_s, batch, own), bf16),
            pltpu.VMEM((steps, n_c, 8, share), f32),
            pltpu.VMEM((steps, n_s, classes, own), bf16),
            pltpu.VMEM((steps, n_c, classes, share), LOGIT_WIRE),
            pltpu.VMEM((steps, n_c - 1, classes, share), LOGIT_WIRE),
            pltpu.VMEM((steps, n_c, classes, share), bf16),
            pltpu.VMEM((steps, n_s - 2, classes, own), GRAD_WIRE),
            pltpu.VMEM((steps, n_s - 2, classes, own), GRAD_WIRE),
            pltpu.VMEM((steps, classes, own), f32),
            pltpu.VMEM((steps, classes, own), f32),
            pltpu.VMEM((classes, own), f32),
            pltpu.SemaphoreType.DMA,
            pltpu.SemaphoreType.DMA((steps * (3 * (n_c - 1) + 2 * (n_s - 1)),)),
            pltpu.SemaphoreType.DMA((steps, n_c - 1)),
            pltpu.SemaphoreType.DMA((steps, n_c - 1)),
            pltpu.SemaphoreType.DMA((steps, n_c - 1)),
            pltpu.SemaphoreType.DMA((steps, n_s - 1)),
            pltpu.SemaphoreType.DMA((steps, n_s - 1)),
        ],
        compiler_params=pltpu.CompilerParams(
            collective_id=0, has_side_effects=True, vmem_limit_bytes=60 * 1024 * 1024
        ),
    )(centres, pool, labels.reshape(1, pool_dev), picks, coefs)


def solution(mesh):
    placed = (
        P(None, "centre"),
        P("centre", "sample"),
        P("sample"),
        P(None, "sample"),
        P(None, ("centre", "sample")),
    )
    return jax.shard_map(
        functools.partial(on_device, mesh),
        mesh=mesh,
        in_specs=placed,
        out_specs=P(None, ("centre", "sample")),
        check_vma=False,
    )
```
